32 devices in a mesh: dp: 4 (over z), mp: 8 (over y, x, core).
Axes of the slice: x: 2, y: 2, z: 4, core: 2. Of those that a mesh axis runs over, the one named last changes fastest.
Arguments:
- patches: bfloat16 [4096, 1280], P(('dp', 'mp')), may hold values from -6 to 6
- window_ids: int32 [32, 128], P(('dp', 'mp')), may hold values from 0 to 7, never falling along the last dimension, each value on 1 to 64 neighbouring positions
- owner: int32 [1024, 1], P(('dp', 'mp')), may hold values from 0 to 3; in each aligned block of 32 rows (0 to 31, 32 to 63, ...) at most 16 rows name the same one
- slot_of_row: int32 [32, 64], P(('dp', 'mp')), may hold values from 0 to 63, each once within a row
- text_embeds: bfloat16 [2048, 8192], P(('dp', 'mp')), may hold values from -6 to 6
- vit_norm: float32 [1280], replicated, may hold values from 0.3 to 3
- vit_qkv_w: bfloat16 [1280, 1920], replicated, may hold values from -0.15625 to 0.15625
- vit_qkv_b: float32 [1920], replicated, may hold values from -12 to 12
- vit_out_w: bfloat16 [640, 1280], replicated, may hold values from -0.25 to 0.25
- merge_norm: float32 [1280], replicated, may hold values from 0.3 to 3
- merge_w1: bfloat16 [5120, 5120], P(None, 'mp'), may hold values from -0.078125 to 0.078125
- merge_b1: float32 [5120], P('mp'), may hold values from -3 to 3
- merge_w2: bfloat16 [5120, 8192], P('mp'), may hold values from -0.078125 to 0.078125
- merge_b2: float32 [8192], replicated, may hold values from -3 to 3
- llm_norm: float32 [8192], replicated, may hold values from 0.5 to 1.5
- q_w: bfloat16 [8192, 4096], P(None, 'mp'), may hold values from -0.0625 to 0.0625
- q_b: float32 [4096], P('mp'), may hold values from -12 to 12
- kv_w: bfloat16 [2, 8192, 512], P(None, None, 'mp'), may hold values from -0.0625 to 0.0625
- kv_b: float32 [2, 512], P(None, 'mp'), may hold values from -12 to 12
Outputs:
- attended: bfloat16 [2048, 4096], P('dp', 'mp')
The draws below stay inside these ranges and needn't reach their ends.
Inputs may be any that keep to these rules, and one draw needn't show every extreme that they name: `window_ids`: within each block, window numbers never fall and each window has at most 64 patches. Among the 32 merged rows of one device, no owner is named by more than 16 rows, a bound that some block reaches. `slot_of_row`: each row is a permutation of the 64 slots.
All inputs are finite; a program needn't handle non-finite values.
Results may differ from the reference program's by a relative error of at most 0.04.
Values may be sent and summed in bfloat16 or wider, within the bound.
A program may use at most 128 MiB of HBM per device.

```python
import math
import jax
import jax.numpy as jnp
import numpy as np
from jax import lax

VW = 1280
VHD = 80
VH = 8
D = 8192
HD = 128
QH = 32
KVH = 4
BLOCK = 128
ROWS_DEV = 64
MW = 5120
MR = 32
CAP = 16
SEQ = 512
PATCHES = 4096
MERGED = 1024
TOTAL_ROWS = 2048
N_DP = 4
N_MP = 8
DEVICES = 32


def drawn_bias(key, bias_shape):
    return jnp.clip(0.5 * jax.random.normal(key, bias_shape, jnp.float32), -3.0, 3.0)


def draw_vit_qkv_b(key, part):
    noise_part = drawn_bias(jax.random.fold_in(key, 7201), (3, VH, VHD))
    return noise_part.reshape(3 * VH * VHD)


def draw_q_b(key, part):
    noise_part = drawn_bias(jax.random.fold_in(key, 7501), (QH, HD))
    return noise_part.reshape(QH * HD)


def draw_kv_b(key, part):
    noise_part = drawn_bias(jax.random.fold_in(key, 7601), (2, KVH, HD))
    return jnp.swapaxes(noise_part, 1, 2).reshape(2, KVH * HD)


def levels(key, shape, shards, least, high):
    factor_of, own = 1.0, jax.random.fold_in(key, 6)
    for axis_at, shards_of in shards:
        draws = jnp.exp(jax.random.uniform(jax.random.fold_in(own, axis_at), (shards_of,), jnp.float32, least / len(shards), high / len(shards)))
        factor_of = factor_of * jnp.repeat(draws, shape[axis_at] // shards_of).reshape([-1 if axis == axis_at else 1 for axis in range(len(shape))])
    return factor_of


def length_profile(number_of, total, limit, skew):
    loads = [(1 << 20) // math.isqrt(standing ** skew) + 1 for standing in range(2, number_of + 1)]
    spare, counts = total - limit - (number_of - 1), [1] * (number_of - 1)
    while spare > 0:
        movable = [i for i in range(number_of - 1) if counts[i] < limit]
        pool, budget = sum([loads[i] for i in movable]), spare
        for i in movable:
            extra = min(limit - counts[i], max(1, budget * loads[i] // pool), spare)
            counts[i] = counts[i] + extra
            spare = spare - extra
    return np.array([limit] + counts)


def uneven_parts(own_key, count, total, reach, skew):
    if count == 2:
        one = jax.random.randint(own_key, (), max(1, total - reach), min(reach, total - 1) + 1)
        return jnp.stack([one, total - one])
    tallies = jnp.asarray(length_profile(count, total, reach, skew), jnp.int32)
    couples = (count - 1) // 2
    donor, taker = tallies[1:1 + 2 * couples:2], tallies[2:2 + 2 * couples:2]
    room = jnp.minimum(donor - 1, reach - taker)
    passed = jax.random.randint(jax.random.fold_in(own_key, 1), (couples,), 0, 1 << 20) % (room + 1)
    tallies = tallies.at[1:1 + 2 * couples:2].set(donor - passed).at[2:2 + 2 * couples:2].set(taker + passed)
    return tallies[jax.random.permutation(jax.random.fold_in(own_key, 2), count)]


def shared_out(stream_key, own, number, rows, amount, top, limit, slope):
    ranking = jax.random.permutation(stream_key, amount)
    heavy_load, ordinary = shares(amount, rows * top, limit, slope, True), shares(amount, rows * top, limit, slope, False)
    places = jnp.arange(amount)

    def named(lengths, turn):
        used = int((lengths > 0).sum())
        fixed = max(1, used // 4)
        shifted = fixed + (places - fixed + turn * (used - fixed)) % max(1, amount - fixed)
        return jnp.zeros((amount,), jnp.int32).at[ranking[jnp.where(places < fixed, places, shifted)]].set(jnp.asarray(lengths, jnp.int32))

    lengths = jnp.where(number % 4 == 0, named(heavy_load, number // 4), named(ordinary, number - number // 4 - 1))
    mixed = jax.random.permutation(jax.random.fold_in(own, 3), amount)
    source_of, receiver = mixed[0:amount // 2 * 2:2], mixed[1:amount // 2 * 2:2]
    slack = jnp.minimum(lengths[source_of] - 1, limit - lengths[receiver]) // 2
    slack = jnp.where((source_of == ranking[0]) | (receiver == ranking[0]) | (lengths[receiver] == 0), 0, jnp.maximum(slack, 0))
    shifted = jax.random.randint(jax.random.fold_in(own, 4), (amount // 2,), 0, 1 << 20) % (slack + 1)
    lengths = lengths.at[source_of].add(-shifted).at[receiver].add(shifted)
    labels = jnp.searchsorted(jnp.cumsum(lengths), jnp.arange(rows * top), side="right").astype(jnp.int32)
    listing = labels.reshape(top, rows).T
    listing = listing[jax.random.permutation(jax.random.fold_in(own, 1), rows)]
    turn = jax.random.randint(jax.random.fold_in(own, 2), (rows, 1), 0, top)
    return jnp.take_along_axis(listing, (jnp.arange(top)[None, :] + turn) % top, axis=1)


def shares(count, total, limit, slope, full):
    portions = [(1 << 20) // math.isqrt(grade ** slope) + 1 for grade in range(1, count + 1)]
    largest = limit if full else min(limit, max(-(-total // count), total * portions[0] // sum(portions)))
    least = 1 if total - largest >= count - 1 else 0
    counts, rest = [largest] + [least] * (count - 1), total - largest - least * (count - 1)
    while rest > 0:
        candidates = [i for i in range(1, count) if counts[i] < largest] or [i for i in range(1, count) if counts[i] < limit]
        mass, left = sum([portions[i] for i in candidates]), rest
        for i in candidates:
            extra = min(limit - counts[i], max(1, left * portions[i] // mass), rest)
            counts[i] = counts[i] + extra
            rest = rest - extra
    return np.array(counts)


def centred(rng, shape, deviation, reach, cuts=(), kind=jnp.bfloat16):
    factor_of = levels(rng, shape, cuts, -0.22, 0.18) if cuts else 1.0
    array = jax.random.normal(rng, shape, jnp.float32) * deviation * factor_of
    return jnp.minimum(jnp.maximum(array, -reach), reach).astype(kind)


def setup_inputs(seed: int = 0) -> dict:
    keys = jax.random.split(jax.random.key(seed), 20)
    patches = centred(keys[0], (PATCHES, VW), 1.0, 6.0, ((0, 32),))
    window_ids = jax.vmap(lambda own: jnp.searchsorted(jnp.cumsum(uneven_parts(own, 8, BLOCK, BLOCK // 2, 2)), jnp.arange(BLOCK), side="right"))(jax.random.split(keys[1], (PATCHES // BLOCK))).reshape((PATCHES // BLOCK, BLOCK)).astype(jnp.int32)
    owner_keys = jax.random.split(jax.random.fold_in(keys[2], 1), MERGED // MR)
    owner_turns = jax.random.permutation(jax.random.fold_in(keys[2], 3), MERGED // MR)
    owner = jax.vmap(lambda own, number: shared_out(jax.random.fold_in(keys[2], 2), own, number, MR, N_DP, 1, CAP, 2))(owner_keys, owner_turns).reshape((MERGED, 1))
    slot_of_row = jax.vmap(lambda own: jax.random.permutation(own, ROWS_DEV))(jax.random.split(keys[3], DEVICES)).reshape((DEVICES, ROWS_DEV)).astype(jnp.int32)
    text_embeds = centred(keys[4], (TOTAL_ROWS, D), 1.0, 6.0, ((0, 32),))
    vit_norm = jnp.clip(jnp.exp(jax.random.uniform(keys[5], (VW,), jnp.float32, math.log(0.3), math.log(3.0))), 0.3, 3.0)
    vit_qkv_w = centred(keys[6], (VW, 3 * VH * VHD), VW ** -0.5, 0.15625)
    vit_qkv_b = draw_vit_qkv_b(jax.random.fold_in(keys[19], 71), 0)
    vit_out_w = centred(keys[8], (VH * VHD, VW), (VH * VHD) ** -0.5, 0.25)
    merge_norm = jnp.clip(jnp.exp(jax.random.uniform(keys[9], (VW,), jnp.float32, math.log(0.3), math.log(3.0))), 0.3, 3.0)
    merge_w1 = centred(keys[10], (MW, MW), MW ** -0.5, 0.078125, ((1, 8),))
    merge_b1 = centred(keys[11], (MW,), 0.5, 3.0, ((0, 8),), jnp.float32)
    merge_w2 = centred(keys[12], (MW, D), MW ** -0.5, 0.078125, ((0, 8),))
    merge_b2 = centred(keys[13], (D,), 0.5, 3.0, (), jnp.float32)
    llm_norm = jnp.clip(1.0 + 0.1 * jax.random.normal(keys[14], (D,), jnp.float32), 0.5, 1.5)
    q_w = centred(keys[15], (D, QH * HD), D ** -0.5, 0.0625, ((1, 8),))
    q_b = draw_q_b(jax.random.fold_in(keys[19], 71), 0)
    kv_w = centred(keys[17], (2, D, KVH * HD), D ** -0.5, 0.0625, ((2, 8),))
    kv_b = draw_kv_b(jax.random.fold_in(keys[19], 71), 0)
    return dict(patches=patches, window_ids=window_ids, owner=owner, slot_of_row=slot_of_row, text_embeds=text_embeds, vit_norm=vit_norm, vit_qkv_w=vit_qkv_w, vit_qkv_b=vit_qkv_b, vit_out_w=vit_out_w, merge_norm=merge_norm, merge_w1=merge_w1, merge_b1=merge_b1, merge_w2=merge_w2, merge_b2=merge_b2, llm_norm=llm_norm, q_w=q_w, q_b=q_b, kv_w=kv_w, kv_b=kv_b)


epsilon = 1e-06

def rms_norm(inputs, gain):
    inputs = inputs.astype(jnp.float32)
    return inputs * lax.rsqrt(lax.optimization_barrier(jnp.mean(inputs * inputs, axis=-1, keepdims=True)) + epsilon) * gain

def vision_block(patches, window_ids, vit_norm, vit_qkv_w, vit_qkv_b, vit_out_w, merge_norm):
    normed = rms_norm(patches, vit_norm).astype(jnp.bfloat16)
    projected = (jnp.dot(normed, vit_qkv_w, preferred_element_type=jnp.float32) + vit_qkv_b).astype(jnp.bfloat16)
    blocks = window_ids.shape[0]
    width = window_ids.shape[1]
    inner_width = vit_out_w.shape[0]
    heads = inner_width // VHD
    shaped = projected.reshape(blocks, width, 3, heads, VHD).astype(jnp.float32)
    scores = jnp.einsum('bqhd,bkhd->bhqk', shaped[:, :, 0], shaped[:, :, 1]) * VHD ** (-0.5)
    in_window = window_ids[:, None, :, None] == window_ids[:, None, None, :]
    scores = jnp.where(in_window, scores, -1e+30)
    peak = lax.optimization_barrier(jnp.max(scores, axis=-1, keepdims=True))
    weights = jnp.exp(scores - peak)
    weights = (weights / lax.optimization_barrier(jnp.sum(weights, axis=-1, keepdims=True))).astype(jnp.bfloat16)
    mixture = jnp.einsum('bhqk,bkhd->bqhd', weights.astype(jnp.float32), shaped[:, :, 2])
    mixture = mixture.astype(jnp.bfloat16).reshape(blocks * width, inner_width)
    residual = (patches.astype(jnp.float32) + jnp.dot(mixture, vit_out_w, preferred_element_type=jnp.float32)).astype(jnp.bfloat16)
    merged = rms_norm(residual, merge_norm).astype(jnp.bfloat16)
    return merged.reshape(blocks * width // 4, 4 * patches.shape[1])

def causal_heads(queries, key_heads, value_heads):
    length = queries.shape[0]
    scores = jnp.einsum('qhd,khd->hqk', queries.astype(jnp.float32), key_heads.astype(jnp.float32)) * HD ** (-0.5)
    allowed = jnp.arange(length)[:, None] >= jnp.arange(length)[None, :]
    scores = jnp.where(allowed[None], scores, -1e+30)
    peak = lax.optimization_barrier(jnp.max(scores, axis=-1, keepdims=True))
    weights = jnp.exp(scores - peak)
    weights = (weights / lax.optimization_barrier(jnp.sum(weights, axis=-1, keepdims=True))).astype(jnp.bfloat16)
    mixture = jnp.einsum('hqk,khd->qhd', weights.astype(jnp.float32), value_heads.astype(jnp.float32))
    return mixture.astype(jnp.bfloat16).reshape(length, -1)

def reference(patches, window_ids, owner, slot_of_row, text_embeds, vit_norm, vit_qkv_w, vit_qkv_b, vit_out_w, merge_norm, merge_w1, merge_b1, merge_w2, merge_b2, llm_norm, q_w, q_b, kv_w, kv_b):
    merged = vision_block(patches, window_ids, vit_norm, vit_qkv_w, vit_qkv_b, vit_out_w, merge_norm)
    hidden = jax.nn.gelu(jnp.dot(merged, merge_w1, preferred_element_type=jnp.float32) + merge_b1, approximate=False).astype(jnp.bfloat16)
    shard_width = MW // N_MP

    def add_shard(running, shard_index):
        first = shard_index * shard_width
        part_hidden = lax.dynamic_slice_in_dim(hidden, first, shard_width, 1)
        part_weight = lax.dynamic_slice_in_dim(merge_w2, first, shard_width, 0)
        partial_value = jnp.dot(part_hidden, part_weight, preferred_element_type=jnp.float32)
        rounded = lax.optimization_barrier(partial_value.astype(jnp.bfloat16))
        return (running + rounded.astype(jnp.float32), 0)
    start_sum = jnp.zeros((merged.shape[0], D), jnp.float32)
    running, unused = lax.scan(add_shard, start_sum, jnp.arange(N_MP, dtype=jnp.int32))
    embedded = (running + merge_b2).astype(jnp.bfloat16)
    devices = DEVICES
    row_ids = jnp.arange(MERGED, dtype=jnp.int32)
    sender = row_ids // MR
    sender_dp = sender // N_MP
    sender_mp = sender % N_MP
    target_group = owner[:, 0]
    onehot = (target_group[:, None] == jnp.arange(N_DP, dtype=jnp.int32)[None, :]).astype(jnp.int32)
    per_device = onehot.reshape(devices, MR, N_DP)
    earlier = (jnp.cumsum(per_device, axis=1) - per_device).reshape(MERGED, N_DP)
    rank_in = lax.optimization_barrier(jnp.sum(earlier * onehot, axis=1))
    target_device = target_group * N_MP + sender_mp
    global_slot = (target_device * ROWS_DEV + sender_dp * CAP + rank_in).astype(jnp.int32)
    buffer = jnp.zeros((TOTAL_ROWS, D), jnp.bfloat16).at[global_slot].set(embedded)
    filled = jnp.zeros((TOTAL_ROWS,), jnp.int32).at[global_slot].set(1)
    source_rows = (jnp.arange(devices, dtype=jnp.int32)[:, None] * ROWS_DEV + slot_of_row).reshape(-1).astype(jnp.int32)
    sequence = jnp.where(filled[source_rows][:, None] > 0, buffer[source_rows], text_embeds)
    llm_normed = rms_norm(sequence, llm_norm).astype(jnp.bfloat16)
    queries = (jnp.dot(llm_normed, q_w, preferred_element_type=jnp.float32) + q_b).astype(jnp.bfloat16)
    key_rows = (jnp.dot(llm_normed, kv_w[0], preferred_element_type=jnp.float32) + kv_b[0]).astype(jnp.bfloat16)
    value_rows = (jnp.dot(llm_normed, kv_w[1], preferred_element_type=jnp.float32) + kv_b[1]).astype(jnp.bfloat16)
    group_size = QH // KVH

    def one_group(inputs):
        group_queries, group_keys, group_values = inputs
        key_heads = jnp.repeat(jnp.swapaxes(group_keys, 1, 2), group_size, axis=1)
        value_heads = jnp.repeat(jnp.swapaxes(group_values, 1, 2), group_size, axis=1)
        return causal_heads(group_queries, key_heads, value_heads)
    attended = lax.map(one_group, (queries.reshape(N_DP, SEQ, QH, HD), key_rows.reshape(N_DP, SEQ, HD, KVH), value_rows.reshape(N_DP, SEQ, HD, KVH)))
    return attended.reshape(N_DP * SEQ, QH * HD)
```

```python
import functools
import jax
import jax.numpy as jnp
from jax import lax
from jax.experimental import pallas as pl
from jax.experimental.pallas import tpu as pltpu
from jax.sharding import PartitionSpec as P

VHD = 80
HD = 128
QH = 32
KVH = 4

MESH = pl.DeviceIdType.MESH
LIMIT = 60 * 1024 * 1024


def corners():
    me = lax.axis_index("mp")
    core, first, second = me % 2, (me // 2) % 2, me // 4
    partner = 1 - 2 * core
    across = 2 - 4 * first
    up = 4 - 8 * second
    return me, partner, across, up


def greet(axis, others):
    barrier = pltpu.get_barrier_semaphore()
    for other in others:
        pl.semaphore_signal(barrier, inc=1, device_id={axis: other}, device_id_type=MESH)
    pl.semaphore_wait(barrier, len(others))


def gather_kernel(rows, in_ref, out_ref, local_sem, send_sem, recv_sem):
    me, partner, across, up = corners()
    greet("mp", (me + partner, me + across, me + up))
    half = rows // 2

    def piece(device, part):
        if part is None:
            return out_ref.at[pl.ds(pl.multiple_of(device * rows, rows), rows)]
        return out_ref.at[pl.ds(pl.multiple_of(device * rows + part * half, half), half)]

    def own(part):
        return in_ref if part is None else in_ref.at[pl.ds(part * half, half)]

    def copy(index, device, part, target, mine=False):
        return pltpu.make_async_remote_copy(
            src_ref=own(part) if mine else piece(device, part),
            dst_ref=piece(device, part),
            send_sem=send_sem.at[index],
            recv_sem=recv_sem.at[index],
            device_id={"mp": target},
            device_id_type=MESH,
        )

    x0 = copy(0, me, 0, me + across, True)
    y1 = copy(4, me, 1, me + up, True)
    x1 = copy(1, me, 1, me + across, True)
    y0 = copy(3, me, 0, me + up, True)
    mate = copy(6, me, None, me + partner, True)
    for item in (x0, y1, x1, y0, mate):
        item.start()
    keep = pltpu.make_async_copy(in_ref, piece(me, None), local_sem)
    keep.start()
    x0.wait_recv()
    far0 = copy(5, me + across, 0, me + up)
    far0.start()
    y1.wait_recv()
    far1 = copy(2, me + up, 1, me + across)
    far1.start()
    x1.wait_recv()
    mate_x = copy(7, me + across, None, me + partner)
    mate_x.start()
    y0.wait_recv()
    mate_y = copy(8, me + up, None, me + partner)
    mate_y.start()
    far0.wait_recv()
    mate_f0 = copy(9, me + across + up, 0, me + partner)
    mate_f0.start()
    far1.wait_recv()
    mate_f1 = copy(10, me + across + up, 1, me + partner)
    mate_f1.start()
    for item in (mate, mate_x, mate_y, mate_f0, mate_f1):
        item.wait_recv()
    for item in (x0, x1, y0, y1, far0, far1, mate, mate_x, mate_y, mate_f0, mate_f1):
        item.wait_send()
    keep.wait()


def gather_mp(block, collective_id):
    ranks = lax.axis_size("mp")
    if ranks != 8:
        return lax.all_gather(block, "mp", axis=0, tiled=True)
    rows, columns = block.shape
    return pl.pallas_call(
        functools.partial(gather_kernel, rows),
        out_shape=jax.ShapeDtypeStruct((ranks * rows, columns), block.dtype),
        in_specs=[pl.BlockSpec(memory_space=pltpu.VMEM)],
        out_specs=pl.BlockSpec(memory_space=pl.ANY),
        scratch_shapes=[
            pltpu.SemaphoreType.DMA,
            pltpu.SemaphoreType.DMA((11,)),
            pltpu.SemaphoreType.DMA((11,)),
        ],
        compiler_params=pltpu.CompilerParams(collective_id=collective_id, has_side_effects=True),
        cost_estimate=pl.CostEstimate(flops=0, bytes_accessed=ranks * block.size * 2, transcendentals=0),
    )(block)


def scatter_kernel(in_ref, out_ref, mate_ref, sum_ref, in_x, in_y, via_ref, last_ref, send_sem, recv_sem):
    me, partner, across, up = corners()
    greet("mp", (me + partner, me + across, me + up))
    columns = in_ref.shape[2]
    half = columns // 2
    step = min(half, 1024)
    devices = (me + across + up, me + across, me + up, me)

    def copy(index, src, dst, target):
        return pltpu.make_async_remote_copy(
            src_ref=src, dst_ref=dst, send_sem=send_sem.at[index], recv_sem=recv_sem.at[index],
            device_id={"mp": target}, device_id_type=MESH,
        )

    def tiles(body):
        def run(i, carry):
            body(pl.multiple_of(i * step, step))
            return carry
        lax.fori_loop(0, half // step, run, 0)

    mates = []
    for slot in range(4):
        item = copy(slot, in_ref.at[devices[slot] + partner], mate_ref.at[slot], me + partner)
        item.start()
        mates.append(item)

    def add_mate(slot):
        mates[slot].wait_recv()
        for part in range(2):
            def body(at):
                cut = pl.ds(part * half + at, step)
                sum_ref[slot, :, cut] = (
                    in_ref[devices[slot], :, cut].astype(jnp.float32) + mate_ref[slot, :, cut].astype(jnp.float32)
                ).astype(jnp.bfloat16)
            tiles(body)

    low, high = pl.ds(0, half), pl.ds(half, half)
    add_mate(0)
    far_x = copy(4, sum_ref.at[0, :, low], in_x.at[0], me + across)
    far_x.start()
    far_y = copy(5, sum_ref.at[0, :, high], in_y.at[0], me + up)
    far_y.start()
    add_mate(1)
    near_x = copy(6, sum_ref.at[1, :, low], in_x.at[1], me + across)
    near_x.start()
    add_mate(2)
    near_y = copy(7, sum_ref.at[2, :, high], in_y.at[1], me + up)
    near_y.start()
    add_mate(3)
    far_x.wait_recv()

    def via_low(at):
        cut = pl.ds(at, step)
        via_ref[0, :, cut] = (
            sum_ref[2, :, cut].astype(jnp.float32) + in_x[0, :, cut].astype(jnp.float32)
        ).astype(jnp.bfloat16)
    tiles(via_low)
    last_y = copy(8, via_ref.at[0], last_ref.at[0], me + up)
    last_y.start()
    far_y.wait_recv()

    def via_high(at):
        cut = pl.ds(at, step)
        via_ref[1, :, cut] = (
            sum_ref[1, :, pl.ds(half + at, step)].astype(jnp.float32) + in_y[0, :, cut].astype(jnp.float32)
        ).astype(jnp.bfloat16)
    tiles(via_high)
    last_x = copy(9, via_ref.at[1], last_ref.at[1], me + across)
    last_x.start()
    near_x.wait_recv()
    last_y.wait_recv()

    def own_low(at):
        cut = pl.ds(at, step)
        out_ref[:, cut] = (
            sum_ref[3, :, cut].astype(jnp.float32)
            + in_x[1, :, cut].astype(jnp.float32) + last_ref[0, :, cut].astype(jnp.float32)
        )
    tiles(own_low)
    near_y.wait_recv()
    last_x.wait_recv()

    def own_high(at):
        cut, wide = pl.ds(at, step), pl.ds(half + at, step)
        out_ref[:, wide] = (
            sum_ref[3, :, wide].astype(jnp.float32)
            + in_y[1, :, cut].astype(jnp.float32) + last_ref[1, :, cut].astype(jnp.float32)
        )
    tiles(own_high)
    for item in mates + [far_x, far_y, near_x, near_y, last_x, last_y]:
        item.wait_send()


def scatter_mp(partial, collective_id):
    ranks = lax.axis_size("mp")
    if ranks != 8:
        return lax.psum_scatter(partial, "mp", scatter_dimension=0, tiled=True).astype(jnp.float32)
    rows, columns = partial.shape[0] // ranks, partial.shape[1]
    half = columns // 2
    return pl.pallas_call(
        scatter_kernel,
        out_shape=jax.ShapeDtypeStruct((rows, columns), jnp.float32),
        in_specs=[pl.BlockSpec(memory_space=pltpu.VMEM)],
        out_specs=pl.BlockSpec(memory_space=pltpu.VMEM),
        scratch_shapes=[
            pltpu.VMEM((4, rows, columns), jnp.bfloat16),
            pltpu.VMEM((4, rows, columns), jnp.bfloat16),
            pltpu.VMEM((2, rows, half), jnp.bfloat16),
            pltpu.VMEM((2, rows, half), jnp.bfloat16),
            pltpu.VMEM((2, rows, half), jnp.bfloat16),
            pltpu.VMEM((2, rows, half), jnp.bfloat16),
            pltpu.SemaphoreType.DMA((10,)),
            pltpu.SemaphoreType.DMA((10,)),
        ],
        compiler_params=pltpu.CompilerParams(collective_id=collective_id, has_side_effects=True),
        cost_estimate=pl.CostEstimate(flops=0, bytes_accessed=partial.size * 4, transcendentals=0),
    )(partial.reshape(ranks, rows, columns))


def exchange_kernel(axis, ranks, pick, count, *refs):
    ins, outs = refs[:count], refs[count:2 * count]
    local_sem, send_sem, recv_sem = refs[2 * count:]
    me = lax.axis_index(axis)
    targets = [lax.rem(me + step, ranks) for step in range(1, ranks)]
    greet(axis, targets)
    copies = []
    for index in range(count):
        for place, target in enumerate(targets):
            item = pltpu.make_async_remote_copy(
                src_ref=ins[index].at[pick(target)], dst_ref=outs[index].at[me],
                send_sem=send_sem.at[index, place], recv_sem=recv_sem.at[index, place],
                device_id={axis: target}, device_id_type=MESH,
            )
            item.start()
            copies.append(item)
        item = pltpu.make_async_copy(ins[index].at[pick(me)], outs[index].at[me], local_sem.at[index])
        item.start()
        copies.append(item)
    for item in copies:
        item.wait()


def exchange(arrays, axis, pick, collective_id):
    ranks = lax.axis_size(axis)
    return pl.pallas_call(
        functools.partial(exchange_kernel, axis, ranks, pick, len(arrays)),
        out_shape=[jax.ShapeDtypeStruct((ranks,) + a.shape[1:], a.dtype) for a in arrays],
        in_specs=[pl.BlockSpec(memory_space=pltpu.VMEM)] * len(arrays),
        out_specs=[pl.BlockSpec(memory_space=pltpu.VMEM)] * len(arrays),
        scratch_shapes=[
            pltpu.SemaphoreType.DMA((len(arrays),)),
            pltpu.SemaphoreType.DMA((len(arrays), ranks - 1)),
            pltpu.SemaphoreType.DMA((len(arrays), ranks - 1)),
        ],
        compiler_params=pltpu.CompilerParams(collective_id=collective_id, has_side_effects=True),
        cost_estimate=pl.CostEstimate(flops=0, bytes_accessed=4 * sum(a.size for a in arrays), transcendentals=0),
    )(*arrays)


CHUNKS = 4


def handover_kernel(
    groups, ranks, emb_ref, selector_ref, marks_ref, picker_ref, text_ref, gain_ref, q_ref, kv_ref,
    out_ref, square_ref,
    send_ref, arrived_ref, arrived_marks, rows_ref, q_here, kv_here, own_square,
    load_sem, z_send, z_recv, send_sem, recv_sem, s_send, s_recv,
):
    me, partner, across, up = corners()
    group = lax.axis_index("dp")
    peers = [lax.rem(group + step, groups) for step in range(1, groups)]
    others = [lax.rem(me + step, ranks) for step in range(1, ranks)]
    loads = [pltpu.make_async_copy(q_ref, q_here, load_sem.at[0]), pltpu.make_async_copy(kv_ref, kv_here, load_sem.at[1])]
    for item in loads:
        item.start()
    barrier = pltpu.get_barrier_semaphore()
    for peer in peers:
        pl.semaphore_signal(barrier, inc=1, device_id={"dp": peer}, device_id_type=MESH)
    for other in others:
        pl.semaphore_signal(barrier, inc=1, device_id={"mp": other}, device_id_type=MESH)
    pl.semaphore_wait(barrier, groups + ranks - 2)

    slots, width = text_ref.shape
    room = slots // groups
    wide = width // CHUNKS
    half = slots // 2

    def block_of(index):
        return pl.ds(pl.multiple_of(index * room, room), room)

    own_block = block_of(group)
    pending = []

    def z_copy(index, place, src, dst):
        item = pltpu.make_async_remote_copy(
            src_ref=src, dst_ref=dst, send_sem=z_send.at[index, place], recv_sem=z_recv.at[index, place],
            device_id={"dp": peers[place]}, device_id_type=MESH,
        )
        item.start()
        pending.append(item)
        return item

    mark_copies = [
        z_copy(CHUNKS, place, marks_ref.at[block_of(peers[place])], arrived_marks.at[own_block])
        for place in range(groups - 1)
    ]
    arrived_marks[own_block, :] = marks_ref[own_block, :]
    z_copies = []
    for chunk in range(CHUNKS):
        cut = pl.ds(chunk * wide, wide)
        send_ref[:, cut] = jnp.dot(
            selector_ref[...], emb_ref[:, cut], preferred_element_type=jnp.float32
        ).astype(jnp.bfloat16)
        z_copies.append([
            z_copy(chunk, place, send_ref.at[block_of(peers[place]), cut], arrived_ref.at[own_block, cut])
            for place in range(groups - 1)
        ])
        arrived_ref[own_block, cut] = send_ref[own_block, cut]

    def piece(device, part, cut):
        if part is None:
            return rows_ref.at[pl.ds(pl.multiple_of(device * slots, slots), slots), cut]
        return rows_ref.at[pl.ds(pl.multiple_of(device * slots + part * half, half), half), cut]

    def copy(chunk, index, device, part, target):
        ref = piece(device, part, pl.ds(chunk * wide, wide))
        item = pltpu.make_async_remote_copy(
            src_ref=ref, dst_ref=ref, send_sem=send_sem.at[chunk, index], recv_sem=recv_sem.at[chunk, index],
            device_id={"mp": target}, device_id_type=MESH,
        )
        item.start()
        pending.append(item)
        return item

    for item in mark_copies:
        item.wait_recv()
    image_here = jnp.dot(picker_ref[...], arrived_marks[...], preferred_element_type=jnp.float32)[:, :1] > 0.5
    own_square[...] = jnp.zeros_like(own_square)
    firsts, mates = [], []

    def choose(chunk):
        cut = pl.ds(chunk * wide, wide)
        for item in z_copies[chunk]:
            item.wait_recv()
        picked = jnp.dot(picker_ref[...], arrived_ref[:, cut], preferred_element_type=jnp.float32)
        sequence = jnp.where(image_here, picked, text_ref[:, cut].astype(jnp.float32))
        squares = sequence * sequence
        total = squares[:, :128]
        for at in range(128, wide, 128):
            total = total + squares[:, at:at + 128]
        own_square[pl.ds(0, slots), :] += total
        rows_ref[pl.ds(pl.multiple_of(me * slots, slots), slots), cut] = (
            sequence * gain_ref[:, cut]
        ).astype(jnp.bfloat16)
        x0 = copy(chunk, 0, me, 0, me + across)
        y1 = copy(chunk, 4, me, 1, me + up)
        x1 = copy(chunk, 1, me, 1, me + across)
        y0 = copy(chunk, 3, me, 0, me + up)
        mate = copy(chunk, 6, me, None, me + partner)
        firsts.append((x0, y1, x1, y0))
        mates.append([mate])

    def forward(chunk):
        x0, y1, x1, y0 = firsts[chunk]
        x0.wait_recv()
        far0 = copy(chunk, 5, me + across, 0, me + up)
        y1.wait_recv()
        far1 = copy(chunk, 2, me + up, 1, me + across)
        x1.wait_recv()
        mates[chunk].append(copy(chunk, 7, me + across, None, me + partner))
        y0.wait_recv()
        mates[chunk].append(copy(chunk, 8, me + up, None, me + partner))
        firsts[chunk] = (far0, far1)

    def corner(chunk):
        far0, far1 = firsts[chunk]
        far0.wait_recv()
        mates[chunk].append(copy(chunk, 9, me + across + up, 0, me + partner))
        far1.wait_recv()
        mates[chunk].append(copy(chunk, 10, me + across + up, 1, me + partner))

    queries = q_here.shape[1]
    height = 256

    def project(chunk):
        cut = pl.ds(chunk * wide, wide)
        for item in mates[chunk]:
            item.wait_recv()
        if chunk == 0:
            for item in loads:
                item.wait()

        def run(i, carry):
            some = pl.ds(pl.multiple_of(i * height, height), height)
            left = jnp.dot(rows_ref[some, cut], q_here[cut, :], preferred_element_type=jnp.float32)
            right = jnp.dot(rows_ref[some, cut], kv_here[cut, :], preferred_element_type=jnp.float32)
            if chunk:
                left = left + out_ref[some, pl.ds(0, queries)]
                right = right + out_ref[some, pl.ds(queries, kv_here.shape[1])]
            out_ref[some, pl.ds(0, queries)] = left
            out_ref[some, pl.ds(queries, kv_here.shape[1])] = right
            return carry
        lax.fori_loop(0, ranks * slots // height, run, 0)

    for chunk in range(CHUNKS):
        choose(chunk)
        if chunk > 0:
            forward(chunk - 1)
        if chunk > 1:
            corner(chunk - 2)
            project(chunk - 2)
    square_ref[me] = jnp.broadcast_to(jnp.sum(own_square[...].T, axis=0, keepdims=True), square_ref.shape[1:])
    forward(CHUNKS - 1)
    square_copies = []
    for place, other in enumerate(others):
        item = pltpu.make_async_remote_copy(
            src_ref=square_ref.at[me], dst_ref=square_ref.at[me], send_sem=s_send.at[place], recv_sem=s_recv.at[place],
            device_id={"mp": other}, device_id_type=MESH,
        )
        item.start()
        square_copies.append(item)
    corner(CHUNKS - 2)
    project(CHUNKS - 2)
    corner(CHUNKS - 1)
    project(CHUNKS - 1)
    for item in square_copies:
        item.wait()
    for item in pending:
        item.wait_send()


def handover(embedded, selector, picker, text, gain, q_w, kv_both, collective_id):
    groups, ranks = lax.axis_size("dp"), lax.axis_size("mp")
    slots, width = text.shape
    marks = jnp.broadcast_to(jnp.sum(selector, axis=1, keepdims=True), (slots, 128)).astype(jnp.bfloat16)
    columns = q_w.shape[1] + kv_both.shape[1]
    vmem = pl.BlockSpec(memory_space=pltpu.VMEM)
    hbm = pl.BlockSpec(memory_space=pl.ANY)
    return pl.pallas_call(
        functools.partial(handover_kernel, groups, ranks),
        out_shape=[
            jax.ShapeDtypeStruct((ranks * slots, columns), jnp.float32),
            jax.ShapeDtypeStruct((ranks, 8, 128), jnp.float32),
        ],
        in_specs=[vmem] * 6 + [hbm] * 2,
        out_specs=[vmem] * 2,
        scratch_shapes=[
            pltpu.VMEM((slots, width), jnp.bfloat16),
            pltpu.VMEM((slots, width), jnp.bfloat16),
            pltpu.VMEM((slots, 128), jnp.bfloat16),
            pltpu.VMEM((ranks * slots, width), jnp.bfloat16),
            pltpu.VMEM(q_w.shape, q_w.dtype),
            pltpu.VMEM(kv_both.shape, kv_both.dtype),
            pltpu.VMEM((128, 128), jnp.float32),
            pltpu.SemaphoreType.DMA((2,)),
            pltpu.SemaphoreType.DMA((CHUNKS + 1, groups - 1)),
            pltpu.SemaphoreType.DMA((CHUNKS + 1, groups - 1)),
            pltpu.SemaphoreType.DMA((CHUNKS, 11)),
            pltpu.SemaphoreType.DMA((CHUNKS, 11)),
            pltpu.SemaphoreType.DMA((ranks - 1,)),
            pltpu.SemaphoreType.DMA((ranks - 1,)),
        ],
        compiler_params=pltpu.CompilerParams(collective_id=collective_id, has_side_effects=True, vmem_limit_bytes=LIMIT),
        cost_estimate=pl.CostEstimate(flops=2 * ranks * slots * width * columns, bytes_accessed=12 * ranks * slots * width, transcendentals=0),
    )(embedded, selector.astype(jnp.bfloat16), marks, picker.astype(jnp.bfloat16), text, gain.reshape(1, -1), q_w, kv_both)


epsilon = 1e-06

STEPS = 8
WIDE = 256
TOP = 63 * 1024 * 1024


def tiles_of(width):
    return [(at, min(WIDE, width - at)) for at in range(0, width, WIDE)]


def fused_kernel(
    groups, ranks, steps, parts,
    merged_ref, owner_ref, slots_ref, b1_ref, b2_ref, gain_ref, qb_ref, kvb_ref,
    w1_hbm, w2_hbm, q_hbm, kv_hbm, text_hbm,
    out_ref,
    w1_ref, w2_ref, q_ref, kv_raw, kv_ref, text_ref,
    all_ref, hidden_acc, hidden_ref, partial_ref, mate_ref, in_x, in_y, last_ref,
    send_ref, arrived_ref, marks_ref, arrived_marks, rows_ref, acc_ref, own_square, square_ref,
    turned_ref, heads_ref, query_ref,
    load_sem, g_send, g_recv, r_send, r_recv, z_send, z_recv, a_send, a_recv, s_send, s_recv, k_send, k_recv,
):
    me, partner, across, up = corners()
    group = lax.axis_index("dp")
    peers = [lax.rem(group + step, groups) for step in range(1, groups)]
    others = [lax.rem(me + step, ranks) for step in range(1, ranks)]
    loads = [
        pltpu.make_async_copy(src, dst, load_sem.at[at])
        for at, (src, dst) in enumerate((
            (w1_hbm, w1_ref), (kv_hbm, kv_raw), (w2_hbm, w2_ref), (text_hbm, text_ref), (q_hbm, q_ref),
        ))
    ]
    for item in loads:
        item.start()
    barrier = pltpu.get_barrier_semaphore()
    for peer in peers:
        pl.semaphore_signal(barrier, inc=1, device_id={"dp": peer}, device_id_type=MESH)
    for other in others:
        pl.semaphore_signal(barrier, inc=1, device_id={"mp": other}, device_id_type=MESH)
    pl.semaphore_wait(barrier, groups + ranks - 2)
    pending = []

    def remote(src, dst, send, recv, where):
        item = pltpu.make_async_remote_copy(
            src_ref=src, dst_ref=dst, send_sem=send, recv_sem=recv, device_id=where, device_id_type=MESH,
        )
        item.start()
        pending.append(item)
        return item

    class Gather:
        def __init__(self, ref, count, width, send, recv, own=None):
            self.ref, self.count, self.width, self.send, self.recv, self.own = ref, count, width, send, recv, own
            self.firsts, self.mates = {}, {}

        def cut(self, chunk):
            return pl.ds(chunk * self.width, self.width)

        def copy(self, chunk, index, device, part, target, mine=False):
            size = self.count if part is None else self.count // 2
            shift = 0 if part is None else part * size
            dst = self.ref.at[pl.ds(pl.multiple_of(device * self.count + shift, size), size), self.cut(chunk)]
            src = self.own.at[pl.ds(shift, size), self.cut(chunk)] if mine and self.own is not None else dst
            return remote(src, dst, self.send.at[chunk, index], self.recv.at[chunk, index], {"mp": target})

        def begin(self, chunk):
            x0 = self.copy(chunk, 0, me, 0, me + across, True)
            y1 = self.copy(chunk, 4, me, 1, me + up, True)
            x1 = self.copy(chunk, 1, me, 1, me + across, True)
            y0 = self.copy(chunk, 3, me, 0, me + up, True)
            self.mates[chunk] = [self.copy(chunk, 6, me, None, me + partner, True)]
            self.firsts[chunk] = (x0, y1, x1, y0)

        def forward(self, chunk):
            x0, y1, x1, y0 = self.firsts[chunk]
            x0.wait_recv()
            far0 = self.copy(chunk, 5, me + across, 0, me + up)
            y1.wait_recv()
            far1 = self.copy(chunk, 2, me + up, 1, me + across)
            x1.wait_recv()
            self.mates[chunk].append(self.copy(chunk, 7, me + across, None, me + partner))
            y0.wait_recv()
            self.mates[chunk].append(self.copy(chunk, 8, me + up, None, me + partner))
            self.firsts[chunk] = (far0, far1)

        def corner(self, chunk):
            far0, far1 = self.firsts[chunk]
            far0.wait_recv()
            self.mates[chunk].append(self.copy(chunk, 9, me + across + up, 0, me + partner))
            far1.wait_recv()
            self.mates[chunk].append(self.copy(chunk, 10, me + across + up, 1, me + partner))

        def finish(self, chunk):
            for item in self.mates[chunk]:
                item.wait_recv()

    mine = merged_ref.shape[0]
    part_width = merged_ref.shape[1] // parts
    merged_all = Gather(all_ref, mine, part_width, g_send, g_recv, merged_ref)
    for part in range(parts):
        merged_all.begin(part)
    all_ref[pl.ds(pl.multiple_of(me * mine, mine), mine), :] = merged_ref[...]

    slots, width = text_ref.shape
    room = slots // groups
    wide = width // steps
    half = wide // 2

    def iota(shape, axis):
        return lax.broadcasted_iota(jnp.int32, shape, axis)

    own = owner_ref[...]
    eye = iota((mine, mine), 0) == iota((mine, mine), 1)
    own_row = jnp.sum(jnp.where(eye, own.astype(jnp.float32), 0.0), axis=0, keepdims=True)
    same = own.astype(jnp.float32) == own_row
    before = iota((mine, mine), 0) < iota((mine, mine), 1)
    rank_row = jnp.sum(jnp.where(same & before, 1.0, 0.0), axis=0, keepdims=True)
    slot_row = own_row * room + rank_row
    selected = jnp.where(iota((slots, mine), 0).astype(jnp.float32) == slot_row, 1.0, 0.0)
    selector = selected.astype(jnp.bfloat16)
    marks_ref[...] = jnp.broadcast_to(jnp.sum(selected, axis=1, keepdims=True), marks_ref.shape).astype(jnp.bfloat16)
    eye = iota((slots, slots), 0) == iota((slots, slots), 1)
    slot_col = jnp.sum(jnp.where(eye, slots_ref[...].astype(jnp.float32), 0.0), axis=1, keepdims=True)
    picker = jnp.where(slot_col == iota((slots, slots), 1).astype(jnp.float32), 1.0, 0.0).astype(jnp.bfloat16)

    def block_of(index):
        return pl.ds(pl.multiple_of(index * room, room), room)

    own_block = block_of(group)

    def z_copy(index, place, src, dst):
        return remote(src, dst, z_send.at[index, place], z_recv.at[index, place], {"dp": peers[place]})

    mark_copies = [
        z_copy(steps, place, marks_ref.at[block_of(peers[place])], arrived_marks.at[own_block])
        for place in range(groups - 1)
    ]
    arrived_marks[own_block, :] = marks_ref[own_block, :]

    def first(part):
        cut = merged_all.cut(part)
        for at, size in tiles_of(hidden_acc.shape[1]):
            value = jnp.dot(all_ref[:, cut], w1_ref[cut, pl.ds(at, size)], preferred_element_type=jnp.float32)
            if part:
                value = value + hidden_acc[:, pl.ds(at, size)]
            if part < parts - 1:
                hidden_acc[:, pl.ds(at, size)] = value
            else:
                value = value + b1_ref[:, pl.ds(at, size)]
                value = 0.5 * value * (1.0 + lax.erf(value * (2.0 ** -0.5)))
                hidden_ref[:, pl.ds(at, size)] = value.astype(jnp.bfloat16)

    for part in range(parts):
        merged_all.forward(part)
        if part == 0:
            loads[0].wait()
            loads[1].wait()
            height = 512
            def join(i, carry):
                some = pl.ds(pl.multiple_of(i * height, height), height)
                kv_ref[some, :] = jnp.concatenate([kv_raw[0, some, :], kv_raw[1, some, :]], axis=1)
                return carry
            lax.fori_loop(0, width // height, join, 0)
        else:
            merged_all.corner(part - 1)
            merged_all.finish(part - 1)
            first(part - 1)
    merged_all.corner(parts - 1)
    merged_all.finish(parts - 1)
    first(parts - 1)
    loads[2].wait()

    devices = (me + across + up, me + across, me + up, me)

    def rows_of(device):
        return pl.ds(pl.multiple_of(device * mine, mine), mine)

    reduce_mates, outward, lasts, z_copies = {}, {}, {}, {}

    def r_copy(chunk, index, src, dst, target):
        return remote(src, dst, r_send.at[chunk, index], r_recv.at[chunk, index], {"mp": target})

    def halves(chunk):
        return pl.ds(chunk * wide, half), pl.ds(chunk * wide + half, half), pl.ds(chunk * half, half)

    def second(chunk):
        for at, size in tiles_of(wide):
            cut = pl.ds(chunk * wide + at, size)
            partial_ref[:, cut] = jnp.dot(
                hidden_ref[...], w2_ref[:, cut], preferred_element_type=jnp.float32
            ).astype(jnp.bfloat16)
        cut = pl.ds(chunk * wide, wide)
        reduce_mates[chunk] = [
            r_copy(chunk, slot, partial_ref.at[rows_of(devices[slot] + partner), cut], mate_ref.at[slot, :, cut], me + partner)
            for slot in range(4)
        ]

    def add_mates(chunk):
        low, high, small = halves(chunk)
        cut = pl.ds(chunk * wide, wide)

        def add(slot):
            reduce_mates[chunk][slot].wait_recv()
            partial_ref[rows_of(devices[slot]), cut] = (
                partial_ref[rows_of(devices[slot]), cut].astype(jnp.float32) + mate_ref[slot, :, cut].astype(jnp.float32)
            ).astype(jnp.bfloat16)

        add(0)
        far_x = r_copy(chunk, 4, partial_ref.at[rows_of(devices[0]), low], in_x.at[0, :, small], me + across)
        far_y = r_copy(chunk, 5, partial_ref.at[rows_of(devices[0]), high], in_y.at[0, :, small], me + up)
        add(1)
        near_x = r_copy(chunk, 6, partial_ref.at[rows_of(devices[1]), low], in_x.at[1, :, small], me + across)
        add(2)
        near_y = r_copy(chunk, 7, partial_ref.at[rows_of(devices[2]), high], in_y.at[1, :, small], me + up)
        add(3)
        outward[chunk] = (far_x, far_y, near_x, near_y)

    def via(chunk):
        low, high, small = halves(chunk)
        far_x, far_y, near_x, near_y = outward[chunk]
        far_x.wait_recv()
        partial_ref[rows_of(devices[2]), low] = (
            partial_ref[rows_of(devices[2]), low].astype(jnp.float32) + in_x[0, :, small].astype(jnp.float32)
        ).astype(jnp.bfloat16)
        last_y = r_copy(chunk, 8, partial_ref.at[rows_of(devices[2]), low], last_ref.at[0, :, small], me + up)
        far_y.wait_recv()
        partial_ref[rows_of(devices[1]), high] = (
            partial_ref[rows_of(devices[1]), high].astype(jnp.float32) + in_y[0, :, small].astype(jnp.float32)
        ).astype(jnp.bfloat16)
        last_x = r_copy(chunk, 9, partial_ref.at[rows_of(devices[1]), high], last_ref.at[1, :, small], me + across)
        lasts[chunk] = (near_x, last_y, near_y, last_x)

    def embed(chunk):
        low, high, small = halves(chunk)
        near_x, last_y, near_y, last_x = lasts[chunk]
        pieces = []
        for at, (place, near, last, side) in enumerate(((low, near_x, last_y, in_x), (high, near_y, last_x, in_y))):
            near.wait_recv()
            last.wait_recv()
            total = (
                partial_ref[rows_of(me), place].astype(jnp.float32)
                + side[1, :, small].astype(jnp.float32) + last_ref[at, :, small].astype(jnp.float32)
            )
            rows = (total + b2_ref[:, place]).astype(jnp.bfloat16)
            send_ref[:, place] = jnp.dot(selector, rows, preferred_element_type=jnp.float32).astype(jnp.bfloat16)
        cut = pl.ds(chunk * wide, wide)
        z_copies[chunk] = [
            z_copy(chunk, place, send_ref.at[block_of(peers[place]), cut], arrived_ref.at[own_block, cut])
            for place in range(groups - 1)
        ]
        arrived_ref[own_block, cut] = send_ref[own_block, cut]

    sequence_all = Gather(rows_ref, slots, wide, a_send, a_recv)

    def choose(chunk):
        cut = pl.ds(chunk * wide, wide)
        if chunk == 0:
            loads[3].wait()
            for item in mark_copies:
                item.wait_recv()
            own_square[...] = jnp.zeros_like(own_square)
        image_here = jnp.dot(picker, arrived_marks[...], preferred_element_type=jnp.float32)[:, :1] > 0.5
        for item in z_copies[chunk]:
            item.wait_recv()
        picked = jnp.dot(picker, arrived_ref[:, cut], preferred_element_type=jnp.float32)
        sequence = jnp.where(image_here, picked, text_ref[:, cut].astype(jnp.float32))
        squares = sequence * sequence
        total = squares[:, :128]
        for at in range(128, wide, 128):
            total = total + squares[:, at:at + 128]
        own_square[pl.ds(0, slots), :] += total
        rows_ref[pl.ds(pl.multiple_of(me * slots, slots), slots), cut] = (
            sequence * gain_ref[:, cut]
        ).astype(jnp.bfloat16)
        sequence_all.begin(chunk)

    square_copies = []

    def share_squares():
        square_ref[me] = jnp.broadcast_to(jnp.sum(own_square[...].T, axis=0, keepdims=True), square_ref.shape[1:])
        for place, other in enumerate(others):
            square_copies.append(
                remote(square_ref.at[me], square_ref.at[me], s_send.at[place], s_recv.at[place], {"mp": other})
            )

    queries = q_ref.shape[1]
    columns = kv_ref.shape[1]

    def project_into(chunk, weight_ref, at, size, shift):
        cut = pl.ds(chunk * wide, wide)
        value = jnp.dot(rows_ref[:, cut], weight_ref[cut, pl.ds(at, size)], preferred_element_type=jnp.float32)
        place = pl.ds(shift + at, size)
        if chunk:
            value = value + acc_ref[:, place]
        acc_ref[:, place] = value

    def project_kv(chunk):
        sequence_all.finish(chunk)
        if chunk == 0:
            loads[4].wait()
        project_into(chunk, kv_ref, 0, columns, queries)

    def project_q(chunk):
        for at, size in tiles_of(queries):
            project_into(chunk, q_ref, at, size, 0)

    def stage(run, chunk):
        if 0 <= chunk < steps:
            run(chunk)

    for step in range(steps + 6):
        stage(second, step)
        stage(add_mates, step - 1)
        stage(via, step - 2)
        stage(embed, step - 3)
        stage(choose, step - 4)
        if step - 4 == steps - 1:
            share_squares()
        stage(sequence_all.forward, step - 5)
        stage(sequence_all.corner, step - 6)
        stage(project_kv, step - 7)
        stage(project_q, step - 7)
    for item in square_copies:
        item.wait_recv()
    project_kv(steps - 1)

    eye = iota((slots, slots), 0) == iota((slots, slots), 1)
    scales = [
        lax.rsqrt(
            jnp.sum(jnp.where(eye, square_ref[rank, pl.ds(0, 1), pl.ds(0, slots)], 0.0), axis=1, keepdims=True) / width
            + epsilon
        )
        for rank in range(ranks)
    ]
    length = ranks * slots
    scaled = jnp.concatenate(
        [acc_ref[pl.ds(rank * slots, slots), pl.ds(queries, columns)] * scales[rank] for rank in range(ranks)], axis=0
    )
    both = (scaled + kvb_ref[...]).astype(jnp.bfloat16)
    dims = columns // (2 * KVH)
    row = iota((columns, columns), 0)
    wanted = (row // dims) % 2 * (dims * KVH) + row % dims * KVH + row // (2 * dims)
    turn = jnp.where(iota((columns, columns), 1) == wanted, 1.0, 0.0).astype(jnp.bfloat16)
    turned_ref[...] = lax.dot_general(
        turn, both, (((1,), (1,)), ((), ())), preferred_element_type=jnp.float32
    ).astype(jnp.bfloat16)
    heads_here = queries // HD
    group_size = QH // KVH

    def head_rows(device):
        return pl.ds(pl.multiple_of(device * heads_here // group_size * (2 * dims), 2 * dims), 2 * dims)

    head_copies = [
        remote(turned_ref.at[head_rows(other)], heads_ref.at[me], k_send.at[place], k_recv.at[place], {"mp": other})
        for place, other in enumerate(others)
    ]
    heads_ref[me] = turned_ref[head_rows(me), :]
    project_q(steps - 1)
    for rank in range(ranks):
        some = pl.ds(rank * slots, slots)
        query_ref[some, :] = (acc_ref[some, pl.ds(0, queries)] * scales[rank] + qb_ref[...]).astype(jnp.bfloat16)
    for item in head_copies:
        item.wait_recv()
    tall = 256
    keys = heads_ref[:, pl.ds(0, dims), :].reshape(ranks * dims, length)
    values = heads_ref[:, pl.ds(dims, dims), :].reshape(ranks * dims, length)
    for block in range(length // tall):
        reach = (block + 1) * tall
        allowed = iota((tall, reach), 0) + block * tall >= iota((tall, reach), 1)
        for head in range(heads_here):
            place = pl.ds(head * HD, HD)
            scores = jnp.dot(
                query_ref[pl.ds(block * tall, tall), place], keys[:, :reach], preferred_element_type=jnp.float32
            ) * HD ** (-0.5)
            scores = jnp.where(allowed, scores, -1e30)
            weights = jnp.exp(scores - jnp.max(scores, axis=-1, keepdims=True))
            weights = (weights * (1.0 / jnp.sum(weights, axis=-1, keepdims=True))).astype(jnp.bfloat16)
            out_ref[pl.ds(block * tall, tall), place] = lax.dot_general(
                weights, values[:, :reach], (((1,), (1,)), ((), ())), preferred_element_type=jnp.float32
            ).astype(jnp.bfloat16)
    for item in pending:
        item.wait_send()


def fused(merged, owner, slot_of_row, text, gain, w1, b1, w2, b2, q_w, q_b, kv_w, kv_b, parts, collective_id):
    groups, ranks = lax.axis_size("dp"), lax.axis_size("mp")
    mine = merged.shape[0]
    slots, width = text.shape
    steps = STEPS
    half = width // 2
    queries, columns = q_w.shape[1], 2 * kv_w.shape[2]
    length = ranks * slots
    vmem = pl.BlockSpec(memory_space=pltpu.VMEM)
    hbm = pl.BlockSpec(memory_space=pl.ANY)
    dma = pltpu.SemaphoreType.DMA
    bf16, f32 = jnp.bfloat16, jnp.float32
    return pl.pallas_call(
        functools.partial(fused_kernel, groups, ranks, steps, parts),
        out_shape=jax.ShapeDtypeStruct((length, queries), bf16),
        in_specs=[vmem] * 8 + [hbm] * 5,
        out_specs=vmem,
        scratch_shapes=[
            pltpu.VMEM(w1.shape, bf16),
            pltpu.VMEM(w2.shape, bf16),
            pltpu.VMEM(q_w.shape, bf16),
            pltpu.VMEM(kv_w.shape, bf16),
            pltpu.VMEM((width, columns), bf16),
            pltpu.VMEM((slots, width), bf16),
            pltpu.VMEM((ranks * mine, merged.shape[1]), bf16),
            pltpu.VMEM((ranks * mine, w1.shape[1]), f32),
            pltpu.VMEM((ranks * mine, w1.shape[1]), bf16),
            pltpu.VMEM((ranks * mine, width), bf16),
            pltpu.VMEM((4, mine, width), bf16),
            pltpu.VMEM((2, mine, half), bf16),
            pltpu.VMEM((2, mine, half), bf16),
            pltpu.VMEM((2, mine, half), bf16),
            pltpu.VMEM((slots, width), bf16),
            pltpu.VMEM((slots, width), bf16),
            pltpu.VMEM((slots, 128), bf16),
            pltpu.VMEM((slots, 128), bf16),
            pltpu.VMEM((length, width), bf16),
            pltpu.VMEM((length, queries + columns), f32),
            pltpu.VMEM((128, 128), f32),
            pltpu.VMEM((ranks, 8, 128), f32),
            pltpu.VMEM((columns, length), bf16),
            pltpu.VMEM((ranks, columns // KVH, length), bf16),
            pltpu.VMEM((length, queries), bf16),
            dma((5,)),
            dma((parts, 11)), dma((parts, 11)),
            dma((steps, 10)), dma((steps, 10)),
            dma((steps + 1, groups - 1)), dma((steps + 1, groups - 1)),
            dma((steps, 11)), dma((steps, 11)),
            dma((ranks - 1,)), dma((ranks - 1,)),
            dma((ranks - 1,)), dma((ranks - 1,)),
        ],
        compiler_params=pltpu.CompilerParams(collective_id=collective_id, has_side_effects=True, vmem_limit_bytes=TOP),
        cost_estimate=pl.CostEstimate(flops=2 * length * width * (queries + columns), bytes_accessed=12 * length * width, transcendentals=0),
    )(
        merged, owner, slot_of_row, b1.reshape(1, -1), b2.reshape(1, -1), gain.reshape(1, -1), q_b.reshape(1, -1),
        kv_b.reshape(1, -1), w1, w2, q_w, kv_w, text,
    )


def rms_norm(inputs, gain):
    inputs = inputs.astype(jnp.float32)
    return inputs * lax.rsqrt(jnp.mean(inputs * inputs, axis=-1, keepdims=True) + epsilon) * gain


def vision_block(patches, window_ids, vit_norm, vit_qkv_w, vit_qkv_b, vit_out_w, merge_norm):
    normed = rms_norm(patches, vit_norm).astype(jnp.bfloat16)
    projected = (jnp.dot(normed, vit_qkv_w, preferred_element_type=jnp.float32) + vit_qkv_b).astype(
        jnp.bfloat16
    )
    blocks = window_ids.shape[0]
    width = window_ids.shape[1]
    inner_width = vit_out_w.shape[0]
    heads = inner_width // VHD
    shaped = projected.reshape(blocks, width, 3, heads, VHD)
    scores = jnp.einsum(
        "bqhd,bkhd->bhqk", shaped[:, :, 0], shaped[:, :, 1], preferred_element_type=jnp.float32
    ) * VHD ** (-0.5)
    in_window = window_ids[:, None, :, None] == window_ids[:, None, None, :]
    scores = jnp.where(in_window, scores, -1e30)
    peak = jnp.max(scores, axis=-1, keepdims=True)
    weights = jnp.exp(scores - peak)
    weights = (weights / jnp.sum(weights, axis=-1, keepdims=True)).astype(jnp.bfloat16)
    mixture = jnp.einsum(
        "bhqk,bkhd->bqhd", weights, shaped[:, :, 2], preferred_element_type=jnp.float32
    )
    mixture = mixture.astype(jnp.bfloat16).reshape(blocks * width, inner_width)
    residual = (
        patches.astype(jnp.float32)
        + jnp.dot(mixture, vit_out_w, preferred_element_type=jnp.float32)
    ).astype(jnp.bfloat16)
    merged = rms_norm(residual, merge_norm).astype(jnp.bfloat16)
    return merged.reshape(blocks * width // 4, 4 * patches.shape[1])


def shards(
    patches,
    window_ids,
    owner,
    slot_of_row,
    text_embeds,
    vit_norm,
    vit_qkv_w,
    vit_qkv_b,
    vit_out_w,
    merge_norm,
    merge_w1,
    merge_b1,
    merge_w2,
    merge_b2,
    llm_norm,
    q_w,
    q_b,
    kv_w,
    kv_b,
):
    merged = vision_block(
        patches, window_ids, vit_norm, vit_qkv_w, vit_qkv_b, vit_out_w, merge_norm
    )
    if lax.axis_size("mp") == 8:
        return fused(
            merged, owner, slot_of_row, text_embeds, llm_norm, merge_w1, merge_b1, merge_w2, merge_b2,
            q_w, q_b, kv_w, kv_b, merged.shape[1] // patches.shape[1], 2,
        )
    rows_all = gather_mp(merged, 0)
    hidden = jax.nn.gelu(
        jnp.dot(rows_all, merge_w1, preferred_element_type=jnp.float32) + merge_b1,
        approximate=False,
    ).astype(jnp.bfloat16)
    own_rows = scatter_mp(
        jnp.dot(hidden, merge_w2, preferred_element_type=jnp.float32).astype(jnp.bfloat16), 1
    )
    embedded = (own_rows + merge_b2).astype(jnp.bfloat16)
    seq_rows = text_embeds.shape[0]
    groups = lax.axis_size("dp")
    capacity = seq_rows // groups
    target_group = owner[:, 0]
    onehot = (target_group[:, None] == jnp.arange(groups, dtype=jnp.int32)[None, :]).astype(
        jnp.int32
    )
    rank_in = jnp.sum((jnp.cumsum(onehot, axis=0) - onehot) * onehot, axis=1)
    send_slot = target_group * capacity + rank_in
    selector = send_slot[None, :] == jnp.arange(seq_rows, dtype=jnp.int32)[:, None]
    query_cols = q_w.shape[1]
    kv_cols = kv_w.shape[2]
    if lax.axis_size("mp") == 8:
        picker = slot_of_row[0][:, None] == jnp.arange(seq_rows, dtype=jnp.int32)[None, :]
        kv_both = jnp.concatenate([kv_w[0], kv_w[1]], axis=1)
        projected, squares = handover(embedded, selector, picker, text_embeds, llm_norm, q_w, kv_both, 2)
        squares = squares[:, 0, :seq_rows].reshape(-1, 1)
        projected = projected * lax.rsqrt(squares / text_embeds.shape[1] + epsilon)
    else:
        buffer = jnp.dot(
            selector.astype(jnp.bfloat16), embedded, preferred_element_type=jnp.float32
        ).astype(jnp.bfloat16)
        buffer = buffer.reshape(groups, capacity, embedded.shape[1])
        counts = jnp.broadcast_to(jnp.sum(onehot, axis=0)[:, None, None], (groups, 8, 128))
        arrived, arrived_counts = exchange((buffer, counts), "dp", lambda target: target, 2)
        arrived = arrived.reshape(seq_rows, embedded.shape[1])
        chosen = slot_of_row[0]
        places = jnp.arange(seq_rows, dtype=jnp.int32)
        filled = places % capacity < jnp.repeat(arrived_counts[:, 0, 0], capacity)
        chooser = (chosen[:, None] == places[None, :]) & filled[None, :]
        picked = jnp.dot(chooser.astype(jnp.bfloat16), arrived, preferred_element_type=jnp.float32)
        image_here = jnp.any(chooser, axis=1)[:, None]
        sequence = jnp.where(image_here, picked, text_embeds.astype(jnp.float32))
        llm_normed = rms_norm(sequence, llm_norm).astype(jnp.bfloat16)
        shard_rows = gather_mp(llm_normed, 3)
        projected = jnp.concatenate(
            [
                jnp.dot(shard_rows, q_w, preferred_element_type=jnp.float32),
                jnp.dot(shard_rows, kv_w[0], preferred_element_type=jnp.float32),
                jnp.dot(shard_rows, kv_w[1], preferred_element_type=jnp.float32),
            ],
            axis=1,
        )
    length = projected.shape[0]
    queries = (projected[:, :query_cols] + q_b).astype(jnp.bfloat16)
    key_rows = (projected[:, query_cols : query_cols + kv_cols] + kv_b[0]).astype(jnp.bfloat16)
    value_rows = (projected[:, query_cols + kv_cols :] + kv_b[1]).astype(jnp.bfloat16)
    heads_here = query_cols // HD
    group_size = QH // KVH
    dims_here = kv_cols // KVH

    def head_major(columns):
        return columns.T.reshape(dims_here, KVH, length).swapaxes(0, 1)

    stacked = jnp.stack([head_major(key_rows), head_major(value_rows)], axis=1)
    (own_head,) = exchange((stacked,), "mp", lambda target: target * heads_here // group_size, 4)
    key_cols = own_head[:, 0].reshape(HD, length)
    value_cols = own_head[:, 1].reshape(HD, length)
    query_heads = queries.reshape(length, heads_here, HD)
    scores = jnp.einsum(
        "qhd,dk->hqk", query_heads, key_cols, preferred_element_type=jnp.float32
    ) * HD ** (-0.5)
    allowed = jnp.arange(length)[:, None] >= jnp.arange(length)[None, :]
    scores = jnp.where(allowed[None], scores, -1e30)
    peak = jnp.max(scores, axis=-1, keepdims=True)
    weights = jnp.exp(scores - peak)
    weights = (weights / jnp.sum(weights, axis=-1, keepdims=True)).astype(jnp.bfloat16)
    mixture = jnp.einsum("hqk,dk->qhd", weights, value_cols, preferred_element_type=jnp.float32)
    return mixture.astype(jnp.bfloat16).reshape(length, query_cols)


def solution(mesh):
    return jax.shard_map(
        shards,
        mesh=mesh,
        in_specs=(
            P(("dp", "mp"), None),
            P(("dp", "mp"), None),
            P(("dp", "mp"), None),
            P(("dp", "mp"), None),
            P(("dp", "mp"), None),
            P(),
            P(),
            P(),
            P(),
            P(),
            P(None, "mp"),
            P("mp"),
            P("mp", None),
            P(),
            P(),
            P(None, "mp"),
            P("mp"),
            P(None, None, "mp"),
            P(None, "mp"),
        ),
        out_specs=P("dp", "mp"),
        check_vma=False,
    )
```

```python
import functools
import jax
import jax.numpy as jnp
from jax import lax
from jax.experimental import pallas as pl
from jax.experimental.pallas import tpu as pltpu
from jax.sharding import PartitionSpec as P

VHD = 80
HD = 128
QH = 32
KVH = 4

MESH = pl.DeviceIdType.MESH
LIMIT = 60 * 1024 * 1024


def corners():
    me = lax.axis_index("mp")
    core, first, second = me % 2, (me // 2) % 2, me // 4
    partner = 1 - 2 * core
    across = 2 - 4 * first
    up = 4 - 8 * second
    return me, partner, across, up


def greet(axis, others):
    barrier = pltpu.get_barrier_semaphore()
    for other in others:
        pl.semaphore_signal(barrier, inc=1, device_id={axis: other}, device_id_type=MESH)
    pl.semaphore_wait(barrier, len(others))


def gather_kernel(rows, in_ref, out_ref, local_sem, send_sem, recv_sem):
    me, partner, across, up = corners()
    greet("mp", (me + partner, me + across, me + up))
    half = rows // 2

    def piece(device, part):
        if part is None:
            return out_ref.at[pl.ds(pl.multiple_of(device * rows, rows), rows)]
        return out_ref.at[pl.ds(pl.multiple_of(device * rows + part * half, half), half)]

    def own(part):
        return in_ref if part is None else in_ref.at[pl.ds(part * half, half)]

    def copy(index, device, part, target, mine=False):
        return pltpu.make_async_remote_copy(
            src_ref=own(part) if mine else piece(device, part),
            dst_ref=piece(device, part),
            send_sem=send_sem.at[index],
            recv_sem=recv_sem.at[index],
            device_id={"mp": target},
            device_id_type=MESH,
        )

    x0 = copy(0, me, 0, me + across, True)
    y1 = copy(4, me, 1, me + up, True)
    x1 = copy(1, me, 1, me + across, True)
    y0 = copy(3, me, 0, me + up, True)
    mate = copy(6, me, None, me + partner, True)
    for item in (x0, y1, x1, y0, mate):
        item.start()
    keep = pltpu.make_async_copy(in_ref, piece(me, None), local_sem)
    keep.start()
    x0.wait_recv()
    far0 = copy(5, me + across, 0, me + up)
    far0.start()
    y1.wait_recv()
    far1 = copy(2, me + up, 1, me + across)
    far1.start()
    x1.wait_recv()
    mate_x = copy(7, me + across, None, me + partner)
    mate_x.start()
    y0.wait_recv()
    mate_y = copy(8, me + up, None, me + partner)
    mate_y.start()
    far0.wait_recv()
    mate_f0 = copy(9, me + across + up, 0, me + partner)
    mate_f0.start()
    far1.wait_recv()
    mate_f1 = copy(10, me + across + up, 1, me + partner)
    mate_f1.start()
    for item in (mate, mate_x, mate_y, mate_f0, mate_f1):
        item.wait_recv()
    for item in (x0, x1, y0, y1, far0, far1, mate, mate_x, mate_y, mate_f0, mate_f1):
        item.wait_send()
    keep.wait()


def gather_mp(block, collective_id):
    ranks = lax.axis_size("mp")
    if ranks != 8:
        return lax.all_gather(block, "mp", axis=0, tiled=True)
    rows, columns = block.shape
    return pl.pallas_call(
        functools.partial(gather_kernel, rows),
        out_shape=jax.ShapeDtypeStruct((ranks * rows, columns), block.dtype),
        in_specs=[pl.BlockSpec(memory_space=pltpu.VMEM)],
        out_specs=pl.BlockSpec(memory_space=pl.ANY),
        scratch_shapes=[
            pltpu.SemaphoreType.DMA,
            pltpu.SemaphoreType.DMA((11,)),
            pltpu.SemaphoreType.DMA((11,)),
        ],
        compiler_params=pltpu.CompilerParams(collective_id=collective_id, has_side_effects=True),
        cost_estimate=pl.CostEstimate(flops=0, bytes_accessed=ranks * block.size * 2, transcendentals=0),
    )(block)


def scatter_kernel(in_ref, out_ref, mate_ref, sum_ref, in_x, in_y, via_ref, last_ref, send_sem, recv_sem):
    me, partner, across, up = corners()
    greet("mp", (me + partner, me + across, me + up))
    columns = in_ref.shape[2]
    half = columns // 2
    step = min(half, 1024)
    devices = (me + across + up, me + across, me + up, me)

    def copy(index, src, dst, target):
        return pltpu.make_async_remote_copy(
            src_ref=src, dst_ref=dst, send_sem=send_sem.at[index], recv_sem=recv_sem.at[index],
            device_id={"mp": target}, device_id_type=MESH,
        )

    def tiles(body):
        def run(i, carry):
            body(pl.multiple_of(i * step, step))
            return carry
        lax.fori_loop(0, half // step, run, 0)

    mates = []
    for slot in range(4):
        item = copy(slot, in_ref.at[devices[slot] + partner], mate_ref.at[slot], me + partner)
        item.start()
        mates.append(item)

    def add_mate(slot):
        mates[slot].wait_recv()
        for part in range(2):
            def body(at):
                cut = pl.ds(part * half + at, step)
                sum_ref[slot, :, cut] = (
                    in_ref[devices[slot], :, cut].astype(jnp.float32) + mate_ref[slot, :, cut].astype(jnp.float32)
                ).astype(jnp.bfloat16)
            tiles(body)

    low, high = pl.ds(0, half), pl.ds(half, half)
    add_mate(0)
    far_x = copy(4, sum_ref.at[0, :, low], in_x.at[0], me + across)
    far_x.start()
    far_y = copy(5, sum_ref.at[0, :, high], in_y.at[0], me + up)
    far_y.start()
    add_mate(1)
    near_x = copy(6, sum_ref.at[1, :, low], in_x.at[1], me + across)
    near_x.start()
    add_mate(2)
    near_y = copy(7, sum_ref.at[2, :, high], in_y.at[1], me + up)
    near_y.start()
    add_mate(3)
    far_x.wait_recv()

    def via_low(at):
        cut = pl.ds(at, step)
        via_ref[0, :, cut] = (
            sum_ref[2, :, cut].astype(jnp.float32) + in_x[0, :, cut].astype(jnp.float32)
        ).astype(jnp.bfloat16)
    tiles(via_low)
    last_y = copy(8, via_ref.at[0], last_ref.at[0], me + up)
    last_y.start()
    far_y.wait_recv()

    def via_high(at):
        cut = pl.ds(at, step)
        via_ref[1, :, cut] = (
            sum_ref[1, :, pl.ds(half + at, step)].astype(jnp.float32) + in_y[0, :, cut].astype(jnp.float32)
        ).astype(jnp.bfloat16)
    tiles(via_high)
    last_x = copy(9, via_ref.at[1], last_ref.at[1], me + across)
    last_x.start()
    near_x.wait_recv()
    last_y.wait_recv()

    def own_low(at):
        cut = pl.ds(at, step)
        out_ref[:, cut] = (
            sum_ref[3, :, cut].astype(jnp.float32)
            + in_x[1, :, cut].astype(jnp.float32) + last_ref[0, :, cut].astype(jnp.float32)
        )
    tiles(own_low)
    near_y.wait_recv()
    last_x.wait_recv()

    def own_high(at):
        cut, wide = pl.ds(at, step), pl.ds(half + at, step)
        out_ref[:, wide] = (
            sum_ref[3, :, wide].astype(jnp.float32)
            + in_y[1, :, cut].astype(jnp.float32) + last_ref[1, :, cut].astype(jnp.float32)
        )
    tiles(own_high)
    for item in mates + [far_x, far_y, near_x, near_y, last_x, last_y]:
        item.wait_send()


def scatter_mp(partial, collective_id):
    ranks = lax.axis_size("mp")
    if ranks != 8:
        return lax.psum_scatter(partial, "mp", scatter_dimension=0, tiled=True).astype(jnp.float32)
    rows, columns = partial.shape[0] // ranks, partial.shape[1]
    half = columns // 2
    return pl.pallas_call(
        scatter_kernel,
        out_shape=jax.ShapeDtypeStruct((rows, columns), jnp.float32),
        in_specs=[pl.BlockSpec(memory_space=pltpu.VMEM)],
        out_specs=pl.BlockSpec(memory_space=pltpu.VMEM),
        scratch_shapes=[
            pltpu.VMEM((4, rows, columns), jnp.bfloat16),
            pltpu.VMEM((4, rows, columns), jnp.bfloat16),
            pltpu.VMEM((2, rows, half), jnp.bfloat16),
            pltpu.VMEM((2, rows, half), jnp.bfloat16),
            pltpu.VMEM((2, rows, half), jnp.bfloat16),
            pltpu.VMEM((2, rows, half), jnp.bfloat16),
            pltpu.SemaphoreType.DMA((10,)),
            pltpu.SemaphoreType.DMA((10,)),
        ],
        compiler_params=pltpu.CompilerParams(collective_id=collective_id, has_side_effects=True),
        cost_estimate=pl.CostEstimate(flops=0, bytes_accessed=partial.size * 4, transcendentals=0),
    )(partial.reshape(ranks, rows, columns))


def exchange_kernel(axis, ranks, pick, count, *refs):
    ins, outs = refs[:count], refs[count:2 * count]
    local_sem, send_sem, recv_sem = refs[2 * count:]
    me = lax.axis_index(axis)
    targets = [lax.rem(me + step, ranks) for step in range(1, ranks)]
    greet(axis, targets)
    copies = []
    for index in range(count):
        for place, target in enumerate(targets):
            item = pltpu.make_async_remote_copy(
                src_ref=ins[index].at[pick(target)], dst_ref=outs[index].at[me],
                send_sem=send_sem.at[index, place], recv_sem=recv_sem.at[index, place],
                device_id={axis: target}, device_id_type=MESH,
            )
            item.start()
            copies.append(item)
        item = pltpu.make_async_copy(ins[index].at[pick(me)], outs[index].at[me], local_sem.at[index])
        item.start()
        copies.append(item)
    for item in copies:
        item.wait()


def exchange(arrays, axis, pick, collective_id):
    ranks = lax.axis_size(axis)
    return pl.pallas_call(
        functools.partial(exchange_kernel, axis, ranks, pick, len(arrays)),
        out_shape=[jax.ShapeDtypeStruct((ranks,) + a.shape[1:], a.dtype) for a in arrays],
        in_specs=[pl.BlockSpec(memory_space=pltpu.VMEM)] * len(arrays),
        out_specs=[pl.BlockSpec(memory_space=pltpu.VMEM)] * len(arrays),
        scratch_shapes=[
            pltpu.SemaphoreType.DMA((len(arrays),)),
            pltpu.SemaphoreType.DMA((len(arrays), ranks - 1)),
            pltpu.SemaphoreType.DMA((len(arrays), ranks - 1)),
        ],
        compiler_params=pltpu.CompilerParams(collective_id=collective_id, has_side_effects=True),
        cost_estimate=pl.CostEstimate(flops=0, bytes_accessed=4 * sum(a.size for a in arrays), transcendentals=0),
    )(*arrays)


CHUNKS = 4


def handover_kernel(
    groups, ranks, emb_ref, selector_ref, marks_ref, picker_ref, text_ref, gain_ref, q_ref, kv_ref,
    out_ref, square_ref,
    send_ref, arrived_ref, arrived_marks, rows_ref, q_here, kv_here, own_square,
    load_sem, z_send, z_recv, send_sem, recv_sem, s_send, s_recv,
):
    me, partner, across, up = corners()
    group = lax.axis_index("dp")
    peers = [lax.rem(group + step, groups) for step in range(1, groups)]
    others = [lax.rem(me + step, ranks) for step in range(1, ranks)]
    loads = [pltpu.make_async_copy(q_ref, q_here, load_sem.at[0]), pltpu.make_async_copy(kv_ref, kv_here, load_sem.at[1])]
    for item in loads:
        item.start()
    barrier = pltpu.get_barrier_semaphore()
    for peer in peers:
        pl.semaphore_signal(barrier, inc=1, device_id={"dp": peer}, device_id_type=MESH)
    for other in others:
        pl.semaphore_signal(barrier, inc=1, device_id={"mp": other}, device_id_type=MESH)
    pl.semaphore_wait(barrier, groups + ranks - 2)

    slots, width = text_ref.shape
    room = slots // groups
    wide = width // CHUNKS
    half = slots // 2

    def block_of(index):
        return pl.ds(pl.multiple_of(index * room, room), room)

    own_block = block_of(group)
    pending = []

    def z_copy(index, place, src, dst):
        item = pltpu.make_async_remote_copy(
            src_ref=src, dst_ref=dst, send_sem=z_send.at[index, place], recv_sem=z_recv.at[index, place],
            device_id={"dp": peers[place]}, device_id_type=MESH,
        )
        item.start()
        pending.append(item)
        return item

    mark_copies = [
        z_copy(CHUNKS, place, marks_ref.at[block_of(peers[place])], arrived_marks.at[own_block])
        for place in range(groups - 1)
    ]
    arrived_marks[own_block, :] = marks_ref[own_block, :]
    z_copies = []
    for chunk in range(CHUNKS):
        cut = pl.ds(chunk * wide, wide)
        send_ref[:, cut] = jnp.dot(
            selector_ref[...], emb_ref[:, cut], preferred_element_type=jnp.float32
        ).astype(jnp.bfloat16)
        z_copies.append([
            z_copy(chunk, place, send_ref.at[block_of(peers[place]), cut], arrived_ref.at[own_block, cut])
            for place in range(groups - 1)
        ])
        arrived_ref[own_block, cut] = send_ref[own_block, cut]

    def piece(device, part, cut):
        if part is None:
            return rows_ref.at[pl.ds(pl.multiple_of(device * slots, slots), slots), cut]
        return rows_ref.at[pl.ds(pl.multiple_of(device * slots + part * half, half), half), cut]

    def copy(chunk, index, device, part, target):
        ref = piece(device, part, pl.ds(chunk * wide, wide))
        item = pltpu.make_async_remote_copy(
            src_ref=ref, dst_ref=ref, send_sem=send_sem.at[chunk, index], recv_sem=recv_sem.at[chunk, index],
            device_id={"mp": target}, device_id_type=MESH,
        )
        item.start()
        pending.append(item)
        return item

    for item in mark_copies:
        item.wait_recv()
    image_here = jnp.dot(picker_ref[...], arrived_marks[...], preferred_element_type=jnp.float32)[:, :1] > 0.5
    own_square[...] = jnp.zeros_like(own_square)
    firsts, mates = [], []

    def choose(chunk):
        cut = pl.ds(chunk * wide, wide)
        for item in z_copies[chunk]:
            item.wait_recv()
        picked = jnp.dot(picker_ref[...], arrived_ref[:, cut], preferred_element_type=jnp.float32)
        sequence = jnp.where(image_here, picked, text_ref[:, cut].astype(jnp.float32))
        squares = sequence * sequence
        total = squares[:, :128]
        for at in range(128, wide, 128):
            total = total + squares[:, at:at + 128]
        own_square[pl.ds(0, slots), :] += total
        rows_ref[pl.ds(pl.multiple_of(me * slots, slots), slots), cut] = (
            sequence * gain_ref[:, cut]
        ).astype(jnp.bfloat16)
        x0 = copy(chunk, 0, me, 0, me + across)
        y1 = copy(chunk, 4, me, 1, me + up)
        x1 = copy(chunk, 1, me, 1, me + across)
        y0 = copy(chunk, 3, me, 0, me + up)
        mate = copy(chunk, 6, me, None, me + partner)
        firsts.append((x0, y1, x1, y0))
        mates.append([mate])

    def forward(chunk):
        x0, y1, x1, y0 = firsts[chunk]
        x0.wait_recv()
        far0 = copy(chunk, 5, me + across, 0, me + up)
        y1.wait_recv()
        far1 = copy(chunk, 2, me + up, 1, me + across)
        x1.wait_recv()
        mates[chunk].append(copy(chunk, 7, me + across, None, me + partner))
        y0.wait_recv()
        mates[chunk].append(copy(chunk, 8, me + up, None, me + partner))
        firsts[chunk] = (far0, far1)

    def corner(chunk):
        far0, far1 = firsts[chunk]
        far0.wait_recv()
        mates[chunk].append(copy(chunk, 9, me + across + up, 0, me + partner))
        far1.wait_recv()
        mates[chunk].append(copy(chunk, 10, me + across + up, 1, me + partner))

    queries = q_here.shape[1]
    height = 256

    def project(chunk):
        cut = pl.ds(chunk * wide, wide)
        for item in mates[chunk]:
            item.wait_recv()
        if chunk == 0:
            for item in loads:
                item.wait()

        def run(i, carry):
            some = pl.ds(pl.multiple_of(i * height, height), height)
            left = jnp.dot(rows_ref[some, cut], q_here[cut, :], preferred_element_type=jnp.float32)
            right = jnp.dot(rows_ref[some, cut], kv_here[cut, :], preferred_element_type=jnp.float32)
            if chunk:
                left = left + out_ref[some, pl.ds(0, queries)]
                right = right + out_ref[some, pl.ds(queries, kv_here.shape[1])]
            out_ref[some, pl.ds(0, queries)] = left
            out_ref[some, pl.ds(queries, kv_here.shape[1])] = right
            return carry
        lax.fori_loop(0, ranks * slots // height, run, 0)

    for chunk in range(CHUNKS):
        choose(chunk)
        if chunk > 0:
            forward(chunk - 1)
        if chunk > 1:
            corner(chunk - 2)
            project(chunk - 2)
    square_ref[me] = jnp.broadcast_to(jnp.sum(own_square[...].T, axis=0, keepdims=True), square_ref.shape[1:])
    forward(CHUNKS - 1)
    square_copies = []
    for place, other in enumerate(others):
        item = pltpu.make_async_remote_copy(
            src_ref=square_ref.at[me], dst_ref=square_ref.at[me], send_sem=s_send.at[place], recv_sem=s_recv.at[place],
            device_id={"mp": other}, device_id_type=MESH,
        )
        item.start()
        square_copies.append(item)
    corner(CHUNKS - 2)
    project(CHUNKS - 2)
    corner(CHUNKS - 1)
    project(CHUNKS - 1)
    for item in square_copies:
        item.wait()
    for item in pending:
        item.wait_send()


def handover(embedded, selector, picker, text, gain, q_w, kv_both, collective_id):
    groups, ranks = lax.axis_size("dp"), lax.axis_size("mp")
    slots, width = text.shape
    marks = jnp.broadcast_to(jnp.sum(selector, axis=1, keepdims=True), (slots, 128)).astype(jnp.bfloat16)
    columns = q_w.shape[1] + kv_both.shape[1]
    vmem = pl.BlockSpec(memory_space=pltpu.VMEM)
    hbm = pl.BlockSpec(memory_space=pl.ANY)
    return pl.pallas_call(
        functools.partial(handover_kernel, groups, ranks),
        out_shape=[
            jax.ShapeDtypeStruct((ranks * slots, columns), jnp.float32),
            jax.ShapeDtypeStruct((ranks, 8, 128), jnp.float32),
        ],
        in_specs=[vmem] * 6 + [hbm] * 2,
        out_specs=[vmem] * 2,
        scratch_shapes=[
            pltpu.VMEM((slots, width), jnp.bfloat16),
            pltpu.VMEM((slots, width), jnp.bfloat16),
            pltpu.VMEM((slots, 128), jnp.bfloat16),
            pltpu.VMEM((ranks * slots, width), jnp.bfloat16),
            pltpu.VMEM(q_w.shape, q_w.dtype),
            pltpu.VMEM(kv_both.shape, kv_both.dtype),
            pltpu.VMEM((128, 128), jnp.float32),
            pltpu.SemaphoreType.DMA((2,)),
            pltpu.SemaphoreType.DMA((CHUNKS + 1, groups - 1)),
            pltpu.SemaphoreType.DMA((CHUNKS + 1, groups - 1)),
            pltpu.SemaphoreType.DMA((CHUNKS, 11)),
            pltpu.SemaphoreType.DMA((CHUNKS, 11)),
            pltpu.SemaphoreType.DMA((ranks - 1,)),
            pltpu.SemaphoreType.DMA((ranks - 1,)),
        ],
        compiler_params=pltpu.CompilerParams(collective_id=collective_id, has_side_effects=True, vmem_limit_bytes=LIMIT),
        cost_estimate=pl.CostEstimate(flops=2 * ranks * slots * width * columns, bytes_accessed=12 * ranks * slots * width, transcendentals=0),
    )(embedded, selector.astype(jnp.bfloat16), marks, picker.astype(jnp.bfloat16), text, gain.reshape(1, -1), q_w, kv_both)


epsilon = 1e-06

def rms_norm(inputs, gain):
    inputs = inputs.astype(jnp.float32)
    return inputs * lax.rsqrt(jnp.mean(inputs * inputs, axis=-1, keepdims=True) + epsilon) * gain


STEPS = 8
WIDE = 256
TOP = 63 * 1024 * 1024


def tiles_of(width):
    return [(at, min(WIDE, width - at)) for at in range(0, width, WIDE)]


def fused_kernel(
    groups, ranks, steps, parts,
    ids_ref, owner_ref, slots_ref, vnorm_ref, vbias_ref, mnorm_ref, b1_ref, b2_ref, gain_ref, qb_ref, kvb_ref,
    patches_hbm, vqkv_hbm, vout_hbm, w1_hbm, w2_hbm, q_hbm, kv_hbm, text_hbm,
    out_ref,
    patches_ref, vqkv_ref, vout_ref, vturn_ref, vmix_ref, w1_ref, w2_ref, q_ref, kv_ref, text_ref,
    all_ref, hidden_acc, hidden_ref, partial_ref, mate_ref, in_x, in_y, last_ref,
    send_ref, arrived_ref, marks_ref, arrived_marks, rows_ref, acc_ref, own_square, square_ref,
    turned_ref, heads_ref, query_ref,
    load_sem, g_send, g_recv, r_send, r_recv, z_send, z_recv, a_send, a_recv, s_send, s_recv, k_send, k_recv,
):
    me, partner, across, up = corners()
    group = lax.axis_index("dp")
    peers = [lax.rem(group + step, groups) for step in range(1, groups)]
    others = [lax.rem(me + step, ranks) for step in range(1, ranks)]
    loads = [
        pltpu.make_async_copy(src, dst, load_sem.at[at])
        for at, (src, dst) in enumerate((
            (w1_hbm, w1_ref), (kv_hbm, kv_ref), (w2_hbm, w2_ref), (text_hbm, text_ref), (q_hbm, q_ref),
            (patches_hbm, patches_ref), (vqkv_hbm, vqkv_ref), (vout_hbm, vout_ref),
        ))
    ]
    for item in loads[5:]:
        item.start()
    barrier = pltpu.get_barrier_semaphore()
    for peer in peers:
        pl.semaphore_signal(barrier, inc=1, device_id={"dp": peer}, device_id_type=MESH)
    for other in others:
        pl.semaphore_signal(barrier, inc=1, device_id={"mp": other}, device_id_type=MESH)
    pending = []

    def iota(shape, axis):
        return lax.broadcasted_iota(jnp.int32, shape, axis)

    def column_of(row):
        size = row.shape[1]
        eye = iota((size, size), 0) == iota((size, size), 1)
        return jnp.sum(jnp.where(eye, row, 0.0), axis=1, keepdims=True)

    patch_rows, vision_width = patches_ref.shape
    mine = patch_rows // parts
    inner = vout_ref.shape[0]
    vision_heads = inner // VHD
    ids_row = ids_ref[...].astype(jnp.float32)
    in_window = column_of(ids_row) == ids_row
    loads[5].wait()
    normed = rms_norm(patches_ref[...], vnorm_ref[...].reshape(1, -1)).astype(jnp.bfloat16)
    loads[6].wait()
    for item in loads[:5]:
        item.start()
    for at, size in tiles_of(3 * inner):
        value = jnp.dot(normed, vqkv_ref[:, pl.ds(at, size)], preferred_element_type=jnp.float32)
        value = (value + vbias_ref[pl.ds(at, size)].reshape(1, -1)).astype(jnp.bfloat16).astype(jnp.float32)
        for low in range(0, size, 128):
            vturn_ref[pl.ds(at + low, 128), :] = value[:, low:low + 128].T.astype(jnp.bfloat16)
    for head in range(vision_heads):
        query, key, content = (vturn_ref[pl.ds(which * inner + head * VHD, VHD), :] for which in range(3))
        scores = lax.dot_general(
            key, query, (((0,), (0,)), ((), ())), preferred_element_type=jnp.float32
        ) * VHD ** (-0.5)
        scores = jnp.where(in_window, scores, -1e30)
        weights = jnp.exp(scores - jnp.max(scores, axis=0, keepdims=True))
        weights = (weights * (1.0 / jnp.sum(weights, axis=0, keepdims=True))).astype(jnp.bfloat16)
        vmix_ref[pl.ds(head * VHD, VHD), :] = jnp.dot(content, weights, preferred_element_type=jnp.float32)
    loads[7].wait()
    mixed = jnp.concatenate(
        [vmix_ref[pl.ds(at, 128), :].T.astype(jnp.bfloat16) for at in range(0, inner, 128)], axis=1
    )
    residual = (
        patches_ref[...].astype(jnp.float32) + jnp.dot(mixed, vout_ref[...], preferred_element_type=jnp.float32)
    ).astype(jnp.bfloat16)
    merged = rms_norm(residual, mnorm_ref[...].reshape(1, -1)).astype(jnp.bfloat16)
    row = iota((patch_rows, patch_rows), 0)
    regroup = jnp.where(
        iota((patch_rows, patch_rows), 1) == row % mine * parts + row // mine, 1.0, 0.0
    ).astype(jnp.bfloat16)
    regrouped = jnp.dot(regroup, merged, preferred_element_type=jnp.float32).astype(jnp.bfloat16)
    own_rows = pl.ds(pl.multiple_of(me * mine, mine), mine)
    for part in range(parts):
        all_ref[own_rows, pl.ds(part * vision_width, vision_width)] = regrouped[part * mine:(part + 1) * mine, :]
    pl.semaphore_wait(barrier, groups + ranks - 2)

    def remote(src, dst, send, recv, where):
        item = pltpu.make_async_remote_copy(
            src_ref=src, dst_ref=dst, send_sem=send, recv_sem=recv, device_id=where, device_id_type=MESH,
        )
        item.start()
        pending.append(item)
        return item

    class Gather:
        def __init__(self, ref, count, width, send, recv):
            self.ref, self.count, self.width, self.send, self.recv = ref, count, width, send, recv
            self.firsts, self.mates = {}, {}

        def cut(self, chunk):
            return pl.ds(chunk * self.width, self.width)

        def copy(self, chunk, index, device, part, target):
            size = self.count if part is None else self.count // 2
            shift = 0 if part is None else part * size
            ref = self.ref.at[pl.ds(pl.multiple_of(device * self.count + shift, size), size), self.cut(chunk)]
            return remote(ref, ref, self.send.at[chunk, index], self.recv.at[chunk, index], {"mp": target})

        def begin(self, chunk):
            x0 = self.copy(chunk, 0, me, 0, me + across)
            y1 = self.copy(chunk, 4, me, 1, me + up)
            x1 = self.copy(chunk, 1, me, 1, me + across)
            y0 = self.copy(chunk, 3, me, 0, me + up)
            self.mates[chunk] = [self.copy(chunk, 6, me, None, me + partner)]
            self.firsts[chunk] = (x0, y1, x1, y0)

        def forward(self, chunk):
            x0, y1, x1, y0 = self.firsts[chunk]
            x0.wait_recv()
            far0 = self.copy(chunk, 5, me + across, 0, me + up)
            y1.wait_recv()
            far1 = self.copy(chunk, 2, me + up, 1, me + across)
            x1.wait_recv()
            self.mates[chunk].append(self.copy(chunk, 7, me + across, None, me + partner))
            y0.wait_recv()
            self.mates[chunk].append(self.copy(chunk, 8, me + up, None, me + partner))
            self.firsts[chunk] = (far0, far1)

        def corner(self, chunk):
            far0, far1 = self.firsts[chunk]
            far0.wait_recv()
            self.mates[chunk].append(self.copy(chunk, 9, me + across + up, 0, me + partner))
            far1.wait_recv()
            self.mates[chunk].append(self.copy(chunk, 10, me + across + up, 1, me + partner))

        def finish(self, chunk):
            for item in self.mates[chunk]:
                item.wait_recv()

    merged_all = Gather(all_ref, mine, vision_width, g_send, g_recv)
    for part in range(parts):
        merged_all.begin(part)

    slots, width = text_ref.shape
    room = slots // groups
    wide = width // steps
    half = wide // 2

    own_row = owner_ref[...].astype(jnp.float32)
    same = column_of(own_row) == own_row
    before = iota((mine, mine), 0) < iota((mine, mine), 1)
    rank_row = jnp.sum(jnp.where(same & before, 1.0, 0.0), axis=0, keepdims=True)
    slot_row = own_row * room + rank_row
    selected = jnp.where(iota((slots, mine), 0).astype(jnp.float32) == slot_row, 1.0, 0.0)
    selector = selected.astype(jnp.bfloat16)
    marks_ref[...] = jnp.broadcast_to(jnp.sum(selected, axis=1, keepdims=True), marks_ref.shape).astype(jnp.bfloat16)
    slot_col = column_of(slots_ref[...].astype(jnp.float32))
    picker = jnp.where(slot_col == iota((slots, slots), 1).astype(jnp.float32), 1.0, 0.0).astype(jnp.bfloat16)

    def block_of(index):
        return pl.ds(pl.multiple_of(index * room, room), room)

    own_block = block_of(group)

    def z_copy(index, place, src, dst):
        return remote(src, dst, z_send.at[index, place], z_recv.at[index, place], {"dp": peers[place]})

    mark_copies = [
        z_copy(steps, place, marks_ref.at[block_of(peers[place])], arrived_marks.at[own_block])
        for place in range(groups - 1)
    ]
    arrived_marks[own_block, :] = marks_ref[own_block, :]

    def first(part):
        cut = merged_all.cut(part)
        for at, size in tiles_of(hidden_acc.shape[1]):
            value = jnp.dot(all_ref[:, cut], w1_ref[cut, pl.ds(at, size)], preferred_element_type=jnp.float32)
            if part:
                value = value + hidden_acc[:, pl.ds(at, size)]
            if part < parts - 1:
                hidden_acc[:, pl.ds(at, size)] = value
            else:
                value = value + b1_ref[pl.ds(at, size)].reshape(1, -1)
                value = 0.5 * value * (1.0 + lax.erf(value * (2.0 ** -0.5)))
                hidden_ref[:, pl.ds(at, size)] = value.astype(jnp.bfloat16)

    for part in range(parts):
        merged_all.forward(part)
        if part == 0:
            loads[0].wait()
        else:
            merged_all.corner(part - 1)
            merged_all.finish(part - 1)
            first(part - 1)
    merged_all.corner(parts - 1)
    merged_all.finish(parts - 1)
    first(parts - 1)
    loads[2].wait()

    devices = (me + across + up, me + across, me + up, me)

    def rows_of(device):
        return pl.ds(pl.multiple_of(device * mine, mine), mine)

    reduce_mates, outward, lasts, z_copies = {}, {}, {}, {}

    def r_copy(chunk, index, src, dst, target):
        return remote(src, dst, r_send.at[chunk, index], r_recv.at[chunk, index], {"mp": target})

    def halves(chunk):
        return pl.ds(chunk * wide, half), pl.ds(chunk * wide + half, half), pl.ds(chunk * half, half)

    def second(chunk):
        for at, size in tiles_of(wide):
            cut = pl.ds(chunk * wide + at, size)
            partial_ref[:, cut] = jnp.dot(
                hidden_ref[...], w2_ref[:, cut], preferred_element_type=jnp.float32
            ).astype(jnp.bfloat16)
        cut = pl.ds(chunk * wide, wide)
        reduce_mates[chunk] = [
            r_copy(chunk, slot, partial_ref.at[rows_of(devices[slot] + partner), cut], mate_ref.at[slot, :, cut], me + partner)
            for slot in range(4)
        ]

    def add_mates(chunk):
        low, high, small = halves(chunk)
        cut = pl.ds(chunk * wide, wide)

        def add(slot):
            reduce_mates[chunk][slot].wait_recv()
            partial_ref[rows_of(devices[slot]), cut] = (
                partial_ref[rows_of(devices[slot]), cut].astype(jnp.float32) + mate_ref[slot, :, cut].astype(jnp.float32)
            ).astype(jnp.bfloat16)

        add(0)
        far_x = r_copy(chunk, 4, partial_ref.at[rows_of(devices[0]), low], in_x.at[0, :, small], me + across)
        far_y = r_copy(chunk, 5, partial_ref.at[rows_of(devices[0]), high], in_y.at[0, :, small], me + up)
        add(1)
        near_x = r_copy(chunk, 6, partial_ref.at[rows_of(devices[1]), low], in_x.at[1, :, small], me + across)
        add(2)
        near_y = r_copy(chunk, 7, partial_ref.at[rows_of(devices[2]), high], in_y.at[1, :, small], me + up)
        add(3)
        outward[chunk] = (far_x, far_y, near_x, near_y)

    def via(chunk):
        low, high, small = halves(chunk)
        far_x, far_y, near_x, near_y = outward[chunk]
        far_x.wait_recv()
        partial_ref[rows_of(devices[2]), low] = (
            partial_ref[rows_of(devices[2]), low].astype(jnp.float32) + in_x[0, :, small].astype(jnp.float32)
        ).astype(jnp.bfloat16)
        last_y = r_copy(chunk, 8, partial_ref.at[rows_of(devices[2]), low], last_ref.at[0, :, small], me + up)
        far_y.wait_recv()
        partial_ref[rows_of(devices[1]), high] = (
            partial_ref[rows_of(devices[1]), high].astype(jnp.float32) + in_y[0, :, small].astype(jnp.float32)
        ).astype(jnp.bfloat16)
        last_x = r_copy(chunk, 9, partial_ref.at[rows_of(devices[1]), high], last_ref.at[1, :, small], me + across)
        lasts[chunk] = (near_x, last_y, near_y, last_x)

    def embed(chunk):
        low, high, small = halves(chunk)
        near_x, last_y, near_y, last_x = lasts[chunk]
        pieces = []
        for at, (place, near, last, side) in enumerate(((low, near_x, last_y, in_x), (high, near_y, last_x, in_y))):
            near.wait_recv()
            last.wait_recv()
            total = (
                partial_ref[rows_of(me), place].astype(jnp.float32)
                + side[1, :, small].astype(jnp.float32) + last_ref[at, :, small].astype(jnp.float32)
            )
            rows = (total + b2_ref[:, place]).astype(jnp.bfloat16)
            send_ref[:, place] = jnp.dot(selector, rows, preferred_element_type=jnp.float32).astype(jnp.bfloat16)
        cut = pl.ds(chunk * wide, wide)
        z_copies[chunk] = [
            z_copy(chunk, place, send_ref.at[block_of(peers[place]), cut], arrived_ref.at[own_block, cut])
            for place in range(groups - 1)
        ]
        arrived_ref[own_block, cut] = send_ref[own_block, cut]

    sequence_all = Gather(rows_ref, slots, wide, a_send, a_recv)

    def choose(chunk):
        cut = pl.ds(chunk * wide, wide)
        if chunk == 0:
            loads[3].wait()
            for item in mark_copies:
                item.wait_recv()
            own_square[...] = jnp.zeros_like(own_square)
        image_here = jnp.dot(picker, arrived_marks[...], preferred_element_type=jnp.float32)[:, :1] > 0.5
        for item in z_copies[chunk]:
            item.wait_recv()
        picked = jnp.dot(picker, arrived_ref[:, cut], preferred_element_type=jnp.float32)
        sequence = jnp.where(image_here, picked, text_ref[:, cut].astype(jnp.float32))
        squares = sequence * sequence
        total = squares[:, :128]
        for at in range(128, wide, 128):
            total = total + squares[:, at:at + 128]
        own_square[pl.ds(0, slots), :] += total
        rows_ref[pl.ds(pl.multiple_of(me * slots, slots), slots), cut] = (
            sequence * gain_ref[:, cut]
        ).astype(jnp.bfloat16)
        sequence_all.begin(chunk)

    square_copies = []

    def share_squares():
        square_ref[me] = jnp.broadcast_to(jnp.sum(own_square[...].T, axis=0, keepdims=True), square_ref.shape[1:])
        for place, other in enumerate(others):
            square_copies.append(
                remote(square_ref.at[me], square_ref.at[me], s_send.at[place], s_recv.at[place], {"mp": other})
            )

    queries = q_ref.shape[1]
    columns = kv_ref.shape[0]

    def project_into(chunk, at, size, weight, dims):
        value = lax.dot_general(
            rows_ref[:, pl.ds(chunk * wide, wide)], weight, (((1,), (dims,)), ((), ())), preferred_element_type=jnp.float32
        )
        place = pl.ds(at, size)
        if chunk:
            value = value + acc_ref[:, place]
        acc_ref[:, place] = value

    def project_kv(chunk):
        sequence_all.finish(chunk)
        if chunk == 0:
            loads[1].wait()
            loads[4].wait()
        project_into(chunk, queries, columns, kv_ref[:, pl.ds(chunk * wide, wide)], 1)

    def project_q(chunk):
        for at, size in tiles_of(queries):
            project_into(chunk, at, size, q_ref[pl.ds(chunk * wide, wide), pl.ds(at, size)], 0)

    def stage(run, chunk):
        if 0 <= chunk < steps:
            run(chunk)

    for step in range(steps + 6):
        stage(second, step)
        stage(add_mates, step - 1)
        stage(via, step - 2)
        stage(embed, step - 3)
        stage(choose, step - 4)
        if step - 4 == steps - 1:
            share_squares()
        stage(sequence_all.forward, step - 5)
        stage(sequence_all.corner, step - 6)
        stage(project_kv, step - 7)
        stage(project_q, step - 7)
    for item in square_copies:
        item.wait_recv()
    project_kv(steps - 1)

    scales = [
        lax.rsqrt(column_of(square_ref[rank, pl.ds(0, 1), pl.ds(0, slots)]) / width + epsilon) for rank in range(ranks)
    ]
    length = ranks * slots
    scaled = jnp.concatenate(
        [acc_ref[pl.ds(rank * slots, slots), pl.ds(queries, columns)] * scales[rank] for rank in range(ranks)], axis=0
    )
    bias = jnp.concatenate([kvb_ref[pl.ds(0, 1), :], kvb_ref[pl.ds(1, 1), :]], axis=1)
    both = (scaled + bias).astype(jnp.bfloat16)
    dims = columns // (2 * KVH)
    row = iota((columns, columns), 0)
    wanted = (row // dims) % 2 * (dims * KVH) + row % dims * KVH + row // (2 * dims)
    turn = jnp.where(iota((columns, columns), 1) == wanted, 1.0, 0.0).astype(jnp.bfloat16)
    turned_ref[...] = lax.dot_general(
        turn, both, (((1,), (1,)), ((), ())), preferred_element_type=jnp.float32
    ).astype(jnp.bfloat16)
    heads_here = queries // HD
    group_size = QH // KVH

    def head_rows(device):
        return pl.ds(pl.multiple_of(device * heads_here // group_size * (2 * dims), 2 * dims), 2 * dims)

    head_copies = [
        remote(turned_ref.at[head_rows(other)], heads_ref.at[me], k_send.at[place], k_recv.at[place], {"mp": other})
        for place, other in enumerate(others)
    ]
    heads_ref[me] = turned_ref[head_rows(me), :]
    project_q(steps - 1)
    for rank in range(ranks):
        some = pl.ds(rank * slots, slots)
        query_ref[some, :] = (acc_ref[some, pl.ds(0, queries)] * scales[rank] + qb_ref[...]).astype(jnp.bfloat16)
    for item in head_copies:
        item.wait_recv()
    tall = 256
    keys = heads_ref[:, pl.ds(0, dims), :].reshape(ranks * dims, length)
    values = heads_ref[:, pl.ds(dims, dims), :].reshape(ranks * dims, length)
    for block in range(length // tall):
        reach = (block + 1) * tall
        allowed = iota((tall, reach), 0) + block * tall >= iota((tall, reach), 1)
        for head in range(heads_here):
            place = pl.ds(head * HD, HD)
            scores = jnp.dot(
                query_ref[pl.ds(block * tall, tall), place], keys[:, :reach], preferred_element_type=jnp.float32
            ) * HD ** (-0.5)
            scores = jnp.where(allowed, scores, -1e30)
            weights = jnp.exp(scores - jnp.max(scores, axis=-1, keepdims=True))
            weights = (weights * (1.0 / jnp.sum(weights, axis=-1, keepdims=True))).astype(jnp.bfloat16)
            out_ref[pl.ds(block * tall, tall), place] = lax.dot_general(
                weights, values[:, :reach], (((1,), (1,)), ((), ())), preferred_element_type=jnp.float32
            ).astype(jnp.bfloat16)
    for item in pending:
        item.wait_send()


def fused(
    patches, window_ids, owner, slot_of_row, text, vit_norm, vit_qkv_w, vit_qkv_b, vit_out_w, merge_norm,
    w1, b1, w2, b2, gain, q_w, q_b, kv_w, kv_b, collective_id,
):
    groups, ranks = lax.axis_size("dp"), lax.axis_size("mp")
    mine = owner.shape[0]
    parts = patches.shape[0] // mine
    slots, width = text.shape
    steps = STEPS
    half = width // 2
    queries, columns = q_w.shape[1], 2 * kv_w.shape[2]
    length = ranks * slots
    vmem = pl.BlockSpec(memory_space=pltpu.VMEM)
    hbm = pl.BlockSpec(memory_space=pl.ANY)
    dma = pltpu.SemaphoreType.DMA
    bf16, f32 = jnp.bfloat16, jnp.float32
    return pl.pallas_call(
        functools.partial(fused_kernel, groups, ranks, steps, parts),
        out_shape=jax.ShapeDtypeStruct((length, queries), bf16),
        in_specs=[vmem] * 11 + [hbm] * 8,
        out_specs=vmem,
        scratch_shapes=[
            pltpu.VMEM(patches.shape, bf16),
            pltpu.VMEM(vit_qkv_w.shape, bf16),
            pltpu.VMEM(vit_out_w.shape, bf16),
            pltpu.VMEM((vit_qkv_w.shape[1], patches.shape[0]), bf16),
            pltpu.VMEM((vit_out_w.shape[0], patches.shape[0]), f32),
            pltpu.VMEM(w1.shape, bf16),
            pltpu.VMEM(w2.shape, bf16),
            pltpu.VMEM(q_w.shape, bf16),
            pltpu.VMEM((columns, width), bf16),
            pltpu.VMEM((slots, width), bf16),
            pltpu.VMEM((ranks * mine, w1.shape[0]), bf16),
            pltpu.VMEM((ranks * mine, w1.shape[1]), f32),
            pltpu.VMEM((ranks * mine, w1.shape[1]), bf16),
            pltpu.VMEM((ranks * mine, width), bf16),
            pltpu.VMEM((4, mine, width), bf16),
            pltpu.VMEM((2, mine, half), bf16),
            pltpu.VMEM((2, mine, half), bf16),
            pltpu.VMEM((2, mine, half), bf16),
            pltpu.VMEM((slots, width), bf16),
            pltpu.VMEM((slots, width), bf16),
            pltpu.VMEM((slots, 128), bf16),
            pltpu.VMEM((slots, 128), bf16),
            pltpu.VMEM((length, width), bf16),
            pltpu.VMEM((length, queries + columns), f32),
            pltpu.VMEM((128, 128), f32),
            pltpu.VMEM((ranks, 8, 128), f32),
            pltpu.VMEM((columns, length), bf16),
            pltpu.VMEM((ranks, columns // KVH, length), bf16),
            pltpu.VMEM((length, queries), bf16),
            dma((8,)),
            dma((parts, 11)), dma((parts, 11)),
            dma((steps, 10)), dma((steps, 10)),
            dma((steps + 1, groups - 1)), dma((steps + 1, groups - 1)),
            dma((steps, 11)), dma((steps, 11)),
            dma((ranks - 1,)), dma((ranks - 1,)),
            dma((ranks - 1,)), dma((ranks - 1,)),
        ],
        compiler_params=pltpu.CompilerParams(collective_id=collective_id, has_side_effects=True, vmem_limit_bytes=TOP),
        cost_estimate=pl.CostEstimate(flops=2 * length * width * (queries + columns), bytes_accessed=12 * length * width, transcendentals=0),
    )(
        window_ids, owner.reshape(1, -1), slot_of_row, vit_norm, vit_qkv_b, merge_norm, b1,
        b2.reshape(1, -1), gain.reshape(1, -1), q_b.reshape(1, -1), kv_b,
        patches, vit_qkv_w, vit_out_w, w1, w2, q_w, kv_w.transpose(0, 2, 1).reshape(columns, width), text,
    )


def vision_block(patches, window_ids, vit_norm, vit_qkv_w, vit_qkv_b, vit_out_w, merge_norm):
    normed = rms_norm(patches, vit_norm).astype(jnp.bfloat16)
    projected = (jnp.dot(normed, vit_qkv_w, preferred_element_type=jnp.float32) + vit_qkv_b).astype(
        jnp.bfloat16
    )
    blocks = window_ids.shape[0]
    width = window_ids.shape[1]
    inner_width = vit_out_w.shape[0]
    heads = inner_width // VHD
    shaped = projected.reshape(blocks, width, 3, heads, VHD)
    scores = jnp.einsum(
        "bqhd,bkhd->bhqk", shaped[:, :, 0], shaped[:, :, 1], preferred_element_type=jnp.float32
    ) * VHD ** (-0.5)
    in_window = window_ids[:, None, :, None] == window_ids[:, None, None, :]
    scores = jnp.where(in_window, scores, -1e30)
    peak = jnp.max(scores, axis=-1, keepdims=True)
    weights = jnp.exp(scores - peak)
    weights = (weights / jnp.sum(weights, axis=-1, keepdims=True)).astype(jnp.bfloat16)
    mixture = jnp.einsum(
        "bhqk,bkhd->bqhd", weights, shaped[:, :, 2], preferred_element_type=jnp.float32
    )
    mixture = mixture.astype(jnp.bfloat16).reshape(blocks * width, inner_width)
    residual = (
        patches.astype(jnp.float32)
        + jnp.dot(mixture, vit_out_w, preferred_element_type=jnp.float32)
    ).astype(jnp.bfloat16)
    merged = rms_norm(residual, merge_norm).astype(jnp.bfloat16)
    return merged.reshape(blocks * width // 4, 4 * patches.shape[1])


def shards(
    patches,
    window_ids,
    owner,
    slot_of_row,
    text_embeds,
    vit_norm,
    vit_qkv_w,
    vit_qkv_b,
    vit_out_w,
    merge_norm,
    merge_w1,
    merge_b1,
    merge_w2,
    merge_b2,
    llm_norm,
    q_w,
    q_b,
    kv_w,
    kv_b,
):
    if lax.axis_size("mp") == 8:
        return fused(
            patches, window_ids, owner, slot_of_row, text_embeds, vit_norm, vit_qkv_w, vit_qkv_b, vit_out_w,
            merge_norm, merge_w1, merge_b1, merge_w2, merge_b2, llm_norm, q_w, q_b, kv_w, kv_b, 2,
        )
    merged = vision_block(
        patches, window_ids, vit_norm, vit_qkv_w, vit_qkv_b, vit_out_w, merge_norm
    )
    rows_all = gather_mp(merged, 0)
    hidden = jax.nn.gelu(
        jnp.dot(rows_all, merge_w1, preferred_element_type=jnp.float32) + merge_b1,
        approximate=False,
    ).astype(jnp.bfloat16)
    own_rows = scatter_mp(
        jnp.dot(hidden, merge_w2, preferred_element_type=jnp.float32).astype(jnp.bfloat16), 1
    )
    embedded = (own_rows + merge_b2).astype(jnp.bfloat16)
    seq_rows = text_embeds.shape[0]
    groups = lax.axis_size("dp")
    capacity = seq_rows // groups
    target_group = owner[:, 0]
    onehot = (target_group[:, None] == jnp.arange(groups, dtype=jnp.int32)[None, :]).astype(
        jnp.int32
    )
    rank_in = jnp.sum((jnp.cumsum(onehot, axis=0) - onehot) * onehot, axis=1)
    send_slot = target_group * capacity + rank_in
    selector = send_slot[None, :] == jnp.arange(seq_rows, dtype=jnp.int32)[:, None]
    query_cols = q_w.shape[1]
    kv_cols = kv_w.shape[2]
    if lax.axis_size("mp") == 8:
        picker = slot_of_row[0][:, None] == jnp.arange(seq_rows, dtype=jnp.int32)[None, :]
        kv_both = jnp.concatenate([kv_w[0], kv_w[1]], axis=1)
        projected, squares = handover(embedded, selector, picker, text_embeds, llm_norm, q_w, kv_both, 2)
        squares = squares[:, 0, :seq_rows].reshape(-1, 1)
        projected = projected * lax.rsqrt(squares / text_embeds.shape[1] + epsilon)
    else:
        buffer = jnp.dot(
            selector.astype(jnp.bfloat16), embedded, preferred_element_type=jnp.float32
        ).astype(jnp.bfloat16)
        buffer = buffer.reshape(groups, capacity, embedded.shape[1])
        counts = jnp.broadcast_to(jnp.sum(onehot, axis=0)[:, None, None], (groups, 8, 128))
        arrived, arrived_counts = exchange((buffer, counts), "dp", lambda target: target, 2)
        arrived = arrived.reshape(seq_rows, embedded.shape[1])
        chosen = slot_of_row[0]
        places = jnp.arange(seq_rows, dtype=jnp.int32)
        filled = places % capacity < jnp.repeat(arrived_counts[:, 0, 0], capacity)
        chooser = (chosen[:, None] == places[None, :]) & filled[None, :]
        picked = jnp.dot(chooser.astype(jnp.bfloat16), arrived, preferred_element_type=jnp.float32)
        image_here = jnp.any(chooser, axis=1)[:, None]
        sequence = jnp.where(image_here, picked, text_embeds.astype(jnp.float32))
        llm_normed = rms_norm(sequence, llm_norm).astype(jnp.bfloat16)
        shard_rows = gather_mp(llm_normed, 3)
        projected = jnp.concatenate(
            [
                jnp.dot(shard_rows, q_w, preferred_element_type=jnp.float32),
                jnp.dot(shard_rows, kv_w[0], preferred_element_type=jnp.float32),
                jnp.dot(shard_rows, kv_w[1], preferred_element_type=jnp.float32),
            ],
            axis=1,
        )
    length = projected.shape[0]
    queries = (projected[:, :query_cols] + q_b).astype(jnp.bfloat16)
    key_rows = (projected[:, query_cols : query_cols + kv_cols] + kv_b[0]).astype(jnp.bfloat16)
    value_rows = (projected[:, query_cols + kv_cols :] + kv_b[1]).astype(jnp.bfloat16)
    heads_here = query_cols // HD
    group_size = QH // KVH
    dims_here = kv_cols // KVH

    def head_major(columns):
        return columns.T.reshape(dims_here, KVH, length).swapaxes(0, 1)

    stacked = jnp.stack([head_major(key_rows), head_major(value_rows)], axis=1)
    (own_head,) = exchange((stacked,), "mp", lambda target: target * heads_here // group_size, 4)
    key_cols = own_head[:, 0].reshape(HD, length)
    value_cols = own_head[:, 1].reshape(HD, length)
    query_heads = queries.reshape(length, heads_here, HD)
    scores = jnp.einsum(
        "qhd,dk->hqk", query_heads, key_cols, preferred_element_type=jnp.float32
    ) * HD ** (-0.5)
    allowed = jnp.arange(length)[:, None] >= jnp.arange(length)[None, :]
    scores = jnp.where(allowed[None], scores, -1e30)
    peak = jnp.max(scores, axis=-1, keepdims=True)
    weights = jnp.exp(scores - peak)
    weights = (weights / jnp.sum(weights, axis=-1, keepdims=True)).astype(jnp.bfloat16)
    mixture = jnp.einsum("hqk,dk->qhd", weights, value_cols, preferred_element_type=jnp.float32)
    return mixture.astype(jnp.bfloat16).reshape(length, query_cols)


def solution(mesh):
    return jax.shard_map(
        shards,
        mesh=mesh,
        in_specs=(
            P(("dp", "mp"), None),
            P(("dp", "mp"), None),
            P(("dp", "mp"), None),
            P(("dp", "mp"), None),
            P(("dp", "mp"), None),
            P(),
            P(),
            P(),
            P(),
            P(),
            P(None, "mp"),
            P("mp"),
            P("mp", None),
            P(),
            P(),
            P(None, "mp"),
            P("mp"),
            P(None, None, "mp"),
            P(None, "mp"),
        ),
        out_specs=P("dp", "mp"),
        check_vma=False,
    )
```

```python
import functools
import jax
import jax.numpy as jnp
from jax import lax
from jax.experimental import pallas as pl
from jax.experimental.pallas import tpu as pltpu
from jax.sharding import PartitionSpec as P

VHD = 80
HD = 128
QH = 32
KVH = 4

MESH = pl.DeviceIdType.MESH
LIMIT = 60 * 1024 * 1024


def corners():
    me = lax.axis_index("mp")
    core, first, second = me % 2, (me // 2) % 2, me // 4
    partner = 1 - 2 * core
    across = 2 - 4 * first
    up = 4 - 8 * second
    return me, partner, across, up


def greet(axis, others):
    barrier = pltpu.get_barrier_semaphore()
    for other in others:
        pl.semaphore_signal(barrier, inc=1, device_id={axis: other}, device_id_type=MESH)
    pl.semaphore_wait(barrier, len(others))


def gather_kernel(rows, in_ref, out_ref, local_sem, send_sem, recv_sem):
    me, partner, across, up = corners()
    greet("mp", (me + partner, me + across, me + up))
    half = rows // 2

    def piece(device, part):
        if part is None:
            return out_ref.at[pl.ds(pl.multiple_of(device * rows, rows), rows)]
        return out_ref.at[pl.ds(pl.multiple_of(device * rows + part * half, half), half)]

    def own(part):
        return in_ref if part is None else in_ref.at[pl.ds(part * half, half)]

    def copy(index, device, part, target, mine=False):
        return pltpu.make_async_remote_copy(
            src_ref=own(part) if mine else piece(device, part),
            dst_ref=piece(device, part),
            send_sem=send_sem.at[index],
            recv_sem=recv_sem.at[index],
            device_id={"mp": target},
            device_id_type=MESH,
        )

    x0 = copy(0, me, 0, me + across, True)
    y1 = copy(4, me, 1, me + up, True)
    x1 = copy(1, me, 1, me + across, True)
    y0 = copy(3, me, 0, me + up, True)
    mate = copy(6, me, None, me + partner, True)
    for item in (x0, y1, x1, y0, mate):
        item.start()
    keep = pltpu.make_async_copy(in_ref, piece(me, None), local_sem)
    keep.start()
    x0.wait_recv()
    far0 = copy(5, me + across, 0, me + up)
    far0.start()
    y1.wait_recv()
    far1 = copy(2, me + up, 1, me + across)
    far1.start()
    x1.wait_recv()
    mate_x = copy(7, me + across, None, me + partner)
    mate_x.start()
    y0.wait_recv()
    mate_y = copy(8, me + up, None, me + partner)
    mate_y.start()
    far0.wait_recv()
    mate_f0 = copy(9, me + across + up, 0, me + partner)
    mate_f0.start()
    far1.wait_recv()
    mate_f1 = copy(10, me + across + up, 1, me + partner)
    mate_f1.start()
    for item in (mate, mate_x, mate_y, mate_f0, mate_f1):
        item.wait_recv()
    for item in (x0, x1, y0, y1, far0, far1, mate, mate_x, mate_y, mate_f0, mate_f1):
        item.wait_send()
    keep.wait()


def gather_mp(block, collective_id):
    ranks = lax.axis_size("mp")
    if ranks != 8:
        return lax.all_gather(block, "mp", axis=0, tiled=True)
    rows, columns = block.shape
    return pl.pallas_call(
        functools.partial(gather_kernel, rows),
        out_shape=jax.ShapeDtypeStruct((ranks * rows, columns), block.dtype),
        in_specs=[pl.BlockSpec(memory_space=pltpu.VMEM)],
        out_specs=pl.BlockSpec(memory_space=pl.ANY),
        scratch_shapes=[
            pltpu.SemaphoreType.DMA,
            pltpu.SemaphoreType.DMA((11,)),
            pltpu.SemaphoreType.DMA((11,)),
        ],
        compiler_params=pltpu.CompilerParams(collective_id=collective_id, has_side_effects=True),
        cost_estimate=pl.CostEstimate(flops=0, bytes_accessed=ranks * block.size * 2, transcendentals=0),
    )(block)


def scatter_kernel(in_ref, out_ref, mate_ref, sum_ref, in_x, in_y, via_ref, last_ref, send_sem, recv_sem):
    me, partner, across, up = corners()
    greet("mp", (me + partner, me + across, me + up))
    columns = in_ref.shape[2]
    half = columns // 2
    step = min(half, 1024)
    devices = (me + across + up, me + across, me + up, me)

    def copy(index, src, dst, target):
        return pltpu.make_async_remote_copy(
            src_ref=src, dst_ref=dst, send_sem=send_sem.at[index], recv_sem=recv_sem.at[index],
            device_id={"mp": target}, device_id_type=MESH,
        )

    def tiles(body):
        def run(i, carry):
            body(pl.multiple_of(i * step, step))
            return carry
        lax.fori_loop(0, half // step, run, 0)

    mates = []
    for slot in range(4):
        item = copy(slot, in_ref.at[devices[slot] + partner], mate_ref.at[slot], me + partner)
        item.start()
        mates.append(item)

    def add_mate(slot):
        mates[slot].wait_recv()
        for part in range(2):
            def body(at):
                cut = pl.ds(part * half + at, step)
                sum_ref[slot, :, cut] = (
                    in_ref[devices[slot], :, cut].astype(jnp.float32) + mate_ref[slot, :, cut].astype(jnp.float32)
                ).astype(jnp.bfloat16)
            tiles(body)

    low, high = pl.ds(0, half), pl.ds(half, half)
    add_mate(0)
    far_x = copy(4, sum_ref.at[0, :, low], in_x.at[0], me + across)
    far_x.start()
    far_y = copy(5, sum_ref.at[0, :, high], in_y.at[0], me + up)
    far_y.start()
    add_mate(1)
    near_x = copy(6, sum_ref.at[1, :, low], in_x.at[1], me + across)
    near_x.start()
    add_mate(2)
    near_y = copy(7, sum_ref.at[2, :, high], in_y.at[1], me + up)
    near_y.start()
    add_mate(3)
    far_x.wait_recv()

    def via_low(at):
        cut = pl.ds(at, step)
        via_ref[0, :, cut] = (
            sum_ref[2, :, cut].astype(jnp.float32) + in_x[0, :, cut].astype(jnp.float32)
        ).astype(jnp.bfloat16)
    tiles(via_low)
    last_y = copy(8, via_ref.at[0], last_ref.at[0], me + up)
    last_y.start()
    far_y.wait_recv()

    def via_high(at):
        cut = pl.ds(at, step)
        via_ref[1, :, cut] = (
            sum_ref[1, :, pl.ds(half + at, step)].astype(jnp.float32) + in_y[0, :, cut].astype(jnp.float32)
        ).astype(jnp.bfloat16)
    tiles(via_high)
    last_x = copy(9, via_ref.at[1], last_ref.at[1], me + across)
    last_x.start()
    near_x.wait_recv()
    last_y.wait_recv()

    def own_low(at):
        cut = pl.ds(at, step)
        out_ref[:, cut] = (
            sum_ref[3, :, cut].astype(jnp.float32)
            + in_x[1, :, cut].astype(jnp.float32) + last_ref[0, :, cut].astype(jnp.float32)
        )
    tiles(own_low)
    near_y.wait_recv()
    last_x.wait_recv()

    def own_high(at):
        cut, wide = pl.ds(at, step), pl.ds(half + at, step)
        out_ref[:, wide] = (
            sum_ref[3, :, wide].astype(jnp.float32)
            + in_y[1, :, cut].astype(jnp.float32) + last_ref[1, :, cut].astype(jnp.float32)
        )
    tiles(own_high)
    for item in mates + [far_x, far_y, near_x, near_y, last_x, last_y]:
        item.wait_send()


def scatter_mp(partial, collective_id):
    ranks = lax.axis_size("mp")
    if ranks != 8:
        return lax.psum_scatter(partial, "mp", scatter_dimension=0, tiled=True).astype(jnp.float32)
    rows, columns = partial.shape[0] // ranks, partial.shape[1]
    half = columns // 2
    return pl.pallas_call(
        scatter_kernel,
        out_shape=jax.ShapeDtypeStruct((rows, columns), jnp.float32),
        in_specs=[pl.BlockSpec(memory_space=pltpu.VMEM)],
        out_specs=pl.BlockSpec(memory_space=pltpu.VMEM),
        scratch_shapes=[
            pltpu.VMEM((4, rows, columns), jnp.bfloat16),
            pltpu.VMEM((4, rows, columns), jnp.bfloat16),
            pltpu.VMEM((2, rows, half), jnp.bfloat16),
            pltpu.VMEM((2, rows, half), jnp.bfloat16),
            pltpu.VMEM((2, rows, half), jnp.bfloat16),
            pltpu.VMEM((2, rows, half), jnp.bfloat16),
            pltpu.SemaphoreType.DMA((10,)),
            pltpu.SemaphoreType.DMA((10,)),
        ],
        compiler_params=pltpu.CompilerParams(collective_id=collective_id, has_side_effects=True),
        cost_estimate=pl.CostEstimate(flops=0, bytes_accessed=partial.size * 4, transcendentals=0),
    )(partial.reshape(ranks, rows, columns))


def exchange_kernel(axis, ranks, pick, count, *refs):
    ins, outs = refs[:count], refs[count:2 * count]
    local_sem, send_sem, recv_sem = refs[2 * count:]
    me = lax.axis_index(axis)
    targets = [lax.rem(me + step, ranks) for step in range(1, ranks)]
    greet(axis, targets)
    copies = []
    for index in range(count):
        for place, target in enumerate(targets):
            item = pltpu.make_async_remote_copy(
                src_ref=ins[index].at[pick(target)], dst_ref=outs[index].at[me],
                send_sem=send_sem.at[index, place], recv_sem=recv_sem.at[index, place],
                device_id={axis: target}, device_id_type=MESH,
            )
            item.start()
            copies.append(item)
        item = pltpu.make_async_copy(ins[index].at[pick(me)], outs[index].at[me], local_sem.at[index])
        item.start()
        copies.append(item)
    for item in copies:
        item.wait()


def exchange(arrays, axis, pick, collective_id):
    ranks = lax.axis_size(axis)
    return pl.pallas_call(
        functools.partial(exchange_kernel, axis, ranks, pick, len(arrays)),
        out_shape=[jax.ShapeDtypeStruct((ranks,) + a.shape[1:], a.dtype) for a in arrays],
        in_specs=[pl.BlockSpec(memory_space=pltpu.VMEM)] * len(arrays),
        out_specs=[pl.BlockSpec(memory_space=pltpu.VMEM)] * len(arrays),
        scratch_shapes=[
            pltpu.SemaphoreType.DMA((len(arrays),)),
            pltpu.SemaphoreType.DMA((len(arrays), ranks - 1)),
            pltpu.SemaphoreType.DMA((len(arrays), ranks - 1)),
        ],
        compiler_params=pltpu.CompilerParams(collective_id=collective_id, has_side_effects=True),
        cost_estimate=pl.CostEstimate(flops=0, bytes_accessed=4 * sum(a.size for a in arrays), transcendentals=0),
    )(*arrays)


CHUNKS = 4


def handover_kernel(
    groups, ranks, emb_ref, selector_ref, marks_ref, picker_ref, text_ref, gain_ref, q_ref, kv_ref,
    out_ref, square_ref,
    send_ref, arrived_ref, arrived_marks, rows_ref, q_here, kv_here, own_square,
    load_sem, z_send, z_recv, send_sem, recv_sem, s_send, s_recv,
):
    me, partner, across, up = corners()
    group = lax.axis_index("dp")
    peers = [lax.rem(group + step, groups) for step in range(1, groups)]
    others = [lax.rem(me + step, ranks) for step in range(1, ranks)]
    loads = [pltpu.make_async_copy(q_ref, q_here, load_sem.at[0]), pltpu.make_async_copy(kv_ref, kv_here, load_sem.at[1])]
    for item in loads:
        item.start()
    barrier = pltpu.get_barrier_semaphore()
    for peer in peers:
        pl.semaphore_signal(barrier, inc=1, device_id={"dp": peer}, device_id_type=MESH)
    for other in others:
        pl.semaphore_signal(barrier, inc=1, device_id={"mp": other}, device_id_type=MESH)
    pl.semaphore_wait(barrier, groups + ranks - 2)

    slots, width = text_ref.shape
    room = slots // groups
    wide = width // CHUNKS
    half = slots // 2

    def block_of(index):
        return pl.ds(pl.multiple_of(index * room, room), room)

    own_block = block_of(group)
    pending = []

    def z_copy(index, place, src, dst):
        item = pltpu.make_async_remote_copy(
            src_ref=src, dst_ref=dst, send_sem=z_send.at[index, place], recv_sem=z_recv.at[index, place],
            device_id={"dp": peers[place]}, device_id_type=MESH,
        )
        item.start()
        pending.append(item)
        return item

    mark_copies = [
        z_copy(CHUNKS, place, marks_ref.at[block_of(peers[place])], arrived_marks.at[own_block])
        for place in range(groups - 1)
    ]
    arrived_marks[own_block, :] = marks_ref[own_block, :]
    z_copies = []
    for chunk in range(CHUNKS):
        cut = pl.ds(chunk * wide, wide)
        send_ref[:, cut] = jnp.dot(
            selector_ref[...], emb_ref[:, cut], preferred_element_type=jnp.float32
        ).astype(jnp.bfloat16)
        z_copies.append([
            z_copy(chunk, place, send_ref.at[block_of(peers[place]), cut], arrived_ref.at[own_block, cut])
            for place in range(groups - 1)
        ])
        arrived_ref[own_block, cut] = send_ref[own_block, cut]

    def piece(device, part, cut):
        if part is None:
            return rows_ref.at[pl.ds(pl.multiple_of(device * slots, slots), slots), cut]
        return rows_ref.at[pl.ds(pl.multiple_of(device * slots + part * half, half), half), cut]

    def copy(chunk, index, device, part, target):
        ref = piece(device, part, pl.ds(chunk * wide, wide))
        item = pltpu.make_async_remote_copy(
            src_ref=ref, dst_ref=ref, send_sem=send_sem.at[chunk, index], recv_sem=recv_sem.at[chunk, index],
            device_id={"mp": target}, device_id_type=MESH,
        )
        item.start()
        pending.append(item)
        return item

    for item in mark_copies:
        item.wait_recv()
    image_here = jnp.dot(picker_ref[...], arrived_marks[...], preferred_element_type=jnp.float32)[:, :1] > 0.5
    own_square[...] = jnp.zeros_like(own_square)
    firsts, mates = [], []

    def choose(chunk):
        cut = pl.ds(chunk * wide, wide)
        for item in z_copies[chunk]:
            item.wait_recv()
        picked = jnp.dot(picker_ref[...], arrived_ref[:, cut], preferred_element_type=jnp.float32)
        sequence = jnp.where(image_here, picked, text_ref[:, cut].astype(jnp.float32))
        squares = sequence * sequence
        total = squares[:, :128]
        for at in range(128, wide, 128):
            total = total + squares[:, at:at + 128]
        own_square[pl.ds(0, slots), :] += total
        rows_ref[pl.ds(pl.multiple_of(me * slots, slots), slots), cut] = (
            sequence * gain_ref[:, cut]
        ).astype(jnp.bfloat16)
        x0 = copy(chunk, 0, me, 0, me + across)
        y1 = copy(chunk, 4, me, 1, me + up)
        x1 = copy(chunk, 1, me, 1, me + across)
        y0 = copy(chunk, 3, me, 0, me + up)
        mate = copy(chunk, 6, me, None, me + partner)
        firsts.append((x0, y1, x1, y0))
        mates.append([mate])

    def forward(chunk):
        x0, y1, x1, y0 = firsts[chunk]
        x0.wait_recv()
        far0 = copy(chunk, 5, me + across, 0, me + up)
        y1.wait_recv()
        far1 = copy(chunk, 2, me + up, 1, me + across)
        x1.wait_recv()
        mates[chunk].append(copy(chunk, 7, me + across, None, me + partner))
        y0.wait_recv()
        mates[chunk].append(copy(chunk, 8, me + up, None, me + partner))
        firsts[chunk] = (far0, far1)

    def corner(chunk):
        far0, far1 = firsts[chunk]
        far0.wait_recv()
        mates[chunk].append(copy(chunk, 9, me + across + up, 0, me + partner))
        far1.wait_recv()
        mates[chunk].append(copy(chunk, 10, me + across + up, 1, me + partner))

    queries = q_here.shape[1]
    height = 256

    def project(chunk):
        cut = pl.ds(chunk * wide, wide)
        for item in mates[chunk]:
            item.wait_recv()
        if chunk == 0:
            for item in loads:
                item.wait()

        def run(i, carry):
            some = pl.ds(pl.multiple_of(i * height, height), height)
            left = jnp.dot(rows_ref[some, cut], q_here[cut, :], preferred_element_type=jnp.float32)
            right = jnp.dot(rows_ref[some, cut], kv_here[cut, :], preferred_element_type=jnp.float32)
            if chunk:
                left = left + out_ref[some, pl.ds(0, queries)]
                right = right + out_ref[some, pl.ds(queries, kv_here.shape[1])]
            out_ref[some, pl.ds(0, queries)] = left
            out_ref[some, pl.ds(queries, kv_here.shape[1])] = right
            return carry
        lax.fori_loop(0, ranks * slots // height, run, 0)

    for chunk in range(CHUNKS):
        choose(chunk)
        if chunk > 0:
            forward(chunk - 1)
        if chunk > 1:
            corner(chunk - 2)
            project(chunk - 2)
    square_ref[me] = jnp.broadcast_to(jnp.sum(own_square[...].T, axis=0, keepdims=True), square_ref.shape[1:])
    forward(CHUNKS - 1)
    square_copies = []
    for place, other in enumerate(others):
        item = pltpu.make_async_remote_copy(
            src_ref=square_ref.at[me], dst_ref=square_ref.at[me], send_sem=s_send.at[place], recv_sem=s_recv.at[place],
            device_id={"mp": other}, device_id_type=MESH,
        )
        item.start()
        square_copies.append(item)
    corner(CHUNKS - 2)
    project(CHUNKS - 2)
    corner(CHUNKS - 1)
    project(CHUNKS - 1)
    for item in square_copies:
        item.wait()
    for item in pending:
        item.wait_send()


def handover(embedded, selector, picker, text, gain, q_w, kv_both, collective_id):
    groups, ranks = lax.axis_size("dp"), lax.axis_size("mp")
    slots, width = text.shape
    marks = jnp.broadcast_to(jnp.sum(selector, axis=1, keepdims=True), (slots, 128)).astype(jnp.bfloat16)
    columns = q_w.shape[1] + kv_both.shape[1]
    vmem = pl.BlockSpec(memory_space=pltpu.VMEM)
    hbm = pl.BlockSpec(memory_space=pl.ANY)
    return pl.pallas_call(
        functools.partial(handover_kernel, groups, ranks),
        out_shape=[
            jax.ShapeDtypeStruct((ranks * slots, columns), jnp.float32),
            jax.ShapeDtypeStruct((ranks, 8, 128), jnp.float32),
        ],
        in_specs=[vmem] * 6 + [hbm] * 2,
        out_specs=[vmem] * 2,
        scratch_shapes=[
            pltpu.VMEM((slots, width), jnp.bfloat16),
            pltpu.VMEM((slots, width), jnp.bfloat16),
            pltpu.VMEM((slots, 128), jnp.bfloat16),
            pltpu.VMEM((ranks * slots, width), jnp.bfloat16),
            pltpu.VMEM(q_w.shape, q_w.dtype),
            pltpu.VMEM(kv_both.shape, kv_both.dtype),
            pltpu.VMEM((128, 128), jnp.float32),
            pltpu.SemaphoreType.DMA((2,)),
            pltpu.SemaphoreType.DMA((CHUNKS + 1, groups - 1)),
            pltpu.SemaphoreType.DMA((CHUNKS + 1, groups - 1)),
            pltpu.SemaphoreType.DMA((CHUNKS, 11)),
            pltpu.SemaphoreType.DMA((CHUNKS, 11)),
            pltpu.SemaphoreType.DMA((ranks - 1,)),
            pltpu.SemaphoreType.DMA((ranks - 1,)),
        ],
        compiler_params=pltpu.CompilerParams(collective_id=collective_id, has_side_effects=True, vmem_limit_bytes=LIMIT),
        cost_estimate=pl.CostEstimate(flops=2 * ranks * slots * width * columns, bytes_accessed=12 * ranks * slots * width, transcendentals=0),
    )(embedded, selector.astype(jnp.bfloat16), marks, picker.astype(jnp.bfloat16), text, gain.reshape(1, -1), q_w, kv_both)


epsilon = 1e-06

def rms_norm(inputs, gain):
    inputs = inputs.astype(jnp.float32)
    return inputs * lax.rsqrt(jnp.mean(inputs * inputs, axis=-1, keepdims=True) + epsilon) * gain


STEPS = 8
WIDE = 256
TOP = 63 * 1024 * 1024


def tiles_of(width):
    return [(at, min(WIDE, width - at)) for at in range(0, width, WIDE)]


def fused_kernel(
    groups, ranks, steps, parts,
    ids_hbm, vnorm_hbm, vbias_hbm, mnorm_hbm, owner_hbm, slots_hbm, b1_hbm, b2_hbm, gain_hbm, qb_hbm, kvb_hbm,
    patches_hbm, vqkv_hbm, vout_hbm, w1_hbm, w2_hbm, q_hbm, kv_hbm, text_hbm,
    out_ref,
    ids_ref, vnorm_ref, vbias_ref, mnorm_ref, owner_ref, slots_ref, b1_ref, b2_ref, gain_ref, qb_ref, kvb_ref,
    small_sem, patches_ref, vqkv_ref, vout_ref, vturn_ref, vmix_ref, w1_ref, w2_ref, q_ref, kv_ref, text_ref,
    all_ref, hidden_acc, hidden_ref, partial_ref, mate_ref, in_x, in_y, last_ref,
    send_ref, arrived_ref, marks_ref, arrived_marks, rows_ref, acc_ref, own_square, square_ref,
    turned_ref, heads_ref, query_ref,
    load_sem, g_send, g_recv, r_send, r_recv, z_send, z_recv, a_send, a_recv, s_send, s_recv, k_send, k_recv,
):
    me, partner, across, up = corners()
    group = lax.axis_index("dp")
    peers = [lax.rem(group + step, groups) for step in range(1, groups)]
    others = [lax.rem(me + step, ranks) for step in range(1, ranks)]
    loads = [
        pltpu.make_async_copy(src, dst, load_sem.at[at])
        for at, (src, dst) in enumerate((
            (w1_hbm, w1_ref), (kv_hbm, kv_ref), (w2_hbm, w2_ref), (text_hbm, text_ref), (q_hbm, q_ref),
            (patches_hbm, patches_ref), (vqkv_hbm, vqkv_ref), (vout_hbm, vout_ref),
        ))
    ]
    smalls = [
        pltpu.make_async_copy(src, dst, small_sem.at[at])
        for at, (src, dst) in enumerate((
            (ids_hbm, ids_ref), (vnorm_hbm, vnorm_ref), (vbias_hbm, vbias_ref), (mnorm_hbm, mnorm_ref),
            (owner_hbm, owner_ref), (slots_hbm, slots_ref), (b1_hbm, b1_ref), (b2_hbm, b2_ref),
            (gain_hbm, gain_ref), (qb_hbm, qb_ref), (kvb_hbm, kvb_ref),
        ))
    ]
    loads[5].start()
    smalls[0].start()
    smalls[1].start()
    loads[6].start()
    loads[7].start()
    for item in smalls[2:]:
        item.start()
    barrier = pltpu.get_barrier_semaphore()
    for peer in peers:
        pl.semaphore_signal(barrier, inc=1, device_id={"dp": peer}, device_id_type=MESH)
    for other in others:
        pl.semaphore_signal(barrier, inc=1, device_id={"mp": other}, device_id_type=MESH)
    pending = []

    def iota(shape, axis):
        return lax.broadcasted_iota(jnp.int32, shape, axis)

    def column_of(row):
        size = row.shape[1]
        eye = iota((size, size), 0) == iota((size, size), 1)
        return jnp.sum(jnp.where(eye, row, 0.0), axis=1, keepdims=True)

    patch_rows, vision_width = patches_ref.shape
    mine = patch_rows // parts
    inner = vout_ref.shape[0]
    vision_heads = inner // VHD
    smalls[0].wait()
    smalls[1].wait()
    ids_row = ids_ref[...].astype(jnp.float32)
    in_window = column_of(ids_row) == ids_row
    loads[5].wait()
    normed = rms_norm(patches_ref[...], vnorm_ref[...].reshape(1, -1)).astype(jnp.bfloat16)
    loads[6].wait()
    for item in smalls[2:]:
        item.wait()
    for item in loads[:5]:
        item.start()
    for at, size in tiles_of(3 * inner):
        value = jnp.dot(normed, vqkv_ref[:, pl.ds(at, size)], preferred_element_type=jnp.float32)
        value = (value + vbias_ref[pl.ds(at, size)].reshape(1, -1)).astype(jnp.bfloat16).astype(jnp.float32)
        for low in range(0, size, 128):
            vturn_ref[pl.ds(at + low, 128), :] = value[:, low:low + 128].T.astype(jnp.bfloat16)
    for head in range(vision_heads):
        query, key, content = (vturn_ref[pl.ds(which * inner + head * VHD, VHD), :] for which in range(3))
        scores = lax.dot_general(
            key, query, (((0,), (0,)), ((), ())), preferred_element_type=jnp.float32
        ) * VHD ** (-0.5)
        scores = jnp.where(in_window, scores, -1e30)
        weights = jnp.exp(scores - jnp.max(scores, axis=0, keepdims=True))
        weights = (weights * (1.0 / jnp.sum(weights, axis=0, keepdims=True))).astype(jnp.bfloat16)
        vmix_ref[pl.ds(head * VHD, VHD), :] = jnp.dot(content, weights, preferred_element_type=jnp.float32)
    loads[7].wait()
    mixed = jnp.concatenate(
        [vmix_ref[pl.ds(at, 128), :].T.astype(jnp.bfloat16) for at in range(0, inner, 128)], axis=1
    )
    residual = (
        patches_ref[...].astype(jnp.float32) + jnp.dot(mixed, vout_ref[...], preferred_element_type=jnp.float32)
    ).astype(jnp.bfloat16)
    merged = rms_norm(residual, mnorm_ref[...].reshape(1, -1)).astype(jnp.bfloat16)
    row = iota((patch_rows, patch_rows), 0)
    regroup = jnp.where(
        iota((patch_rows, patch_rows), 1) == row % mine * parts + row // mine, 1.0, 0.0
    ).astype(jnp.bfloat16)
    regrouped = jnp.dot(regroup, merged, preferred_element_type=jnp.float32).astype(jnp.bfloat16)
    own_rows = pl.ds(pl.multiple_of(me * mine, mine), mine)
    for part in range(parts):
        all_ref[own_rows, pl.ds(part * vision_width, vision_width)] = regrouped[part * mine:(part + 1) * mine, :]
    pl.semaphore_wait(barrier, groups + ranks - 2)

    def remote(src, dst, send, recv, where):
        item = pltpu.make_async_remote_copy(
            src_ref=src, dst_ref=dst, send_sem=send, recv_sem=recv, device_id=where, device_id_type=MESH,
        )
        item.start()
        pending.append(item)
        return item

    class Gather:
        def __init__(self, ref, count, width, send, recv):
            self.ref, self.count, self.width, self.send, self.recv = ref, count, width, send, recv
            self.firsts, self.mates = {}, {}

        def cut(self, chunk):
            return pl.ds(chunk * self.width, self.width)

        def copy(self, chunk, index, device, part, target):
            size = self.count if part is None else self.count // 2
            shift = 0 if part is None else part * size
            ref = self.ref.at[pl.ds(pl.multiple_of(device * self.count + shift, size), size), self.cut(chunk)]
            return remote(ref, ref, self.send.at[chunk, index], self.recv.at[chunk, index], {"mp": target})

        def begin(self, chunk):
            x0 = self.copy(chunk, 0, me, 0, me + across)
            y1 = self.copy(chunk, 4, me, 1, me + up)
            x1 = self.copy(chunk, 1, me, 1, me + across)
            y0 = self.copy(chunk, 3, me, 0, me + up)
            self.mates[chunk] = [self.copy(chunk, 6, me, None, me + partner)]
            self.firsts[chunk] = (x0, y1, x1, y0)

        def forward(self, chunk):
            x0, y1, x1, y0 = self.firsts[chunk]
            x0.wait_recv()
            far0 = self.copy(chunk, 5, me + across, 0, me + up)
            y1.wait_recv()
            far1 = self.copy(chunk, 2, me + up, 1, me + across)
            x1.wait_recv()
            self.mates[chunk].append(self.copy(chunk, 7, me + across, None, me + partner))
            y0.wait_recv()
            self.mates[chunk].append(self.copy(chunk, 8, me + up, None, me + partner))
            self.firsts[chunk] = (far0, far1)

        def corner(self, chunk):
            far0, far1 = self.firsts[chunk]
            far0.wait_recv()
            self.mates[chunk].append(self.copy(chunk, 9, me + across + up, 0, me + partner))
            far1.wait_recv()
            self.mates[chunk].append(self.copy(chunk, 10, me + across + up, 1, me + partner))

        def finish(self, chunk):
            for item in self.mates[chunk]:
                item.wait_recv()

    merged_all = Gather(all_ref, mine, vision_width, g_send, g_recv)
    for part in range(parts):
        merged_all.begin(part)

    slots, width = text_ref.shape
    room = slots // groups
    wide = width // steps
    half = wide // 2

    own_row = owner_ref[...].astype(jnp.float32)
    same = column_of(own_row) == own_row
    before = iota((mine, mine), 0) < iota((mine, mine), 1)
    rank_row = jnp.sum(jnp.where(same & before, 1.0, 0.0), axis=0, keepdims=True)
    slot_row = own_row * room + rank_row
    selected = jnp.where(iota((slots, mine), 0).astype(jnp.float32) == slot_row, 1.0, 0.0)
    selector = selected.astype(jnp.bfloat16)
    marks_ref[...] = jnp.broadcast_to(jnp.sum(selected, axis=1, keepdims=True), marks_ref.shape).astype(jnp.bfloat16)
    slot_col = column_of(slots_ref[...].astype(jnp.float32))
    picker = jnp.where(slot_col == iota((slots, slots), 1).astype(jnp.float32), 1.0, 0.0).astype(jnp.bfloat16)

    def block_of(index):
        return pl.ds(pl.multiple_of(index * room, room), room)

    own_block = block_of(group)

    def z_copy(index, place, src, dst):
        return remote(src, dst, z_send.at[index, place], z_recv.at[index, place], {"dp": peers[place]})

    mark_copies = [
        z_copy(steps, place, marks_ref.at[block_of(peers[place])], arrived_marks.at[own_block])
        for place in range(groups - 1)
    ]
    arrived_marks[own_block, :] = marks_ref[own_block, :]

    def first(part):
        cut = merged_all.cut(part)
        for at, size in tiles_of(hidden_acc.shape[1]):
            value = jnp.dot(all_ref[:, cut], w1_ref[cut, pl.ds(at, size)], preferred_element_type=jnp.float32)
            if part:
                value = value + hidden_acc[:, pl.ds(at, size)]
            if part < parts - 1:
                hidden_acc[:, pl.ds(at, size)] = value
            else:
                value = value + b1_ref[pl.ds(at, size)].reshape(1, -1)
                value = 0.5 * value * (1.0 + lax.erf(value * (2.0 ** -0.5)))
                hidden_ref[:, pl.ds(at, size)] = value.astype(jnp.bfloat16)

    for part in range(parts):
        merged_all.forward(part)
    loads[0].wait()
    for part in range(parts):
        merged_all.corner(part)
        if part:
            merged_all.finish(part - 1)
            first(part - 1)
    merged_all.finish(parts - 1)
    first(parts - 1)
    loads[2].wait()

    devices = (me + across + up, me + across, me + up, me)

    def rows_of(device):
        return pl.ds(pl.multiple_of(device * mine, mine), mine)

    reduce_mates, outward, lasts, z_copies = {}, {}, {}, {}

    def r_copy(chunk, index, src, dst, target):
        return remote(src, dst, r_send.at[chunk, index], r_recv.at[chunk, index], {"mp": target})

    def halves(chunk):
        return pl.ds(chunk * wide, half), pl.ds(chunk * wide + half, half), pl.ds(chunk * half, half)

    def second(chunk):
        for at, size in tiles_of(wide):
            cut = pl.ds(chunk * wide + at, size)
            partial_ref[:, cut] = jnp.dot(
                hidden_ref[...], w2_ref[:, cut], preferred_element_type=jnp.float32
            ).astype(jnp.bfloat16)
        cut = pl.ds(chunk * wide, wide)
        reduce_mates[chunk] = [
            r_copy(chunk, slot, partial_ref.at[rows_of(devices[slot] + partner), cut], mate_ref.at[slot, :, cut], me + partner)
            for slot in range(4)
        ]

    def add_mates(chunk):
        low, high, small = halves(chunk)
        cut = pl.ds(chunk * wide, wide)

        def add(slot):
            reduce_mates[chunk][slot].wait_recv()
            partial_ref[rows_of(devices[slot]), cut] = (
                partial_ref[rows_of(devices[slot]), cut].astype(jnp.float32) + mate_ref[slot, :, cut].astype(jnp.float32)
            ).astype(jnp.bfloat16)

        add(0)
        far_x = r_copy(chunk, 4, partial_ref.at[rows_of(devices[0]), low], in_x.at[0, :, small], me + across)
        far_y = r_copy(chunk, 5, partial_ref.at[rows_of(devices[0]), high], in_y.at[0, :, small], me + up)
        add(1)
        near_x = r_copy(chunk, 6, partial_ref.at[rows_of(devices[1]), low], in_x.at[1, :, small], me + across)
        add(2)
        near_y = r_copy(chunk, 7, partial_ref.at[rows_of(devices[2]), high], in_y.at[1, :, small], me + up)
        add(3)
        outward[chunk] = (far_x, far_y, near_x, near_y)

    def via(chunk):
        low, high, small = halves(chunk)
        far_x, far_y, near_x, near_y = outward[chunk]
        far_x.wait_recv()
        partial_ref[rows_of(devices[2]), low] = (
            partial_ref[rows_of(devices[2]), low].astype(jnp.float32) + in_x[0, :, small].astype(jnp.float32)
        ).astype(jnp.bfloat16)
        last_y = r_copy(chunk, 8, partial_ref.at[rows_of(devices[2]), low], last_ref.at[0, :, small], me + up)
        far_y.wait_recv()
        partial_ref[rows_of(devices[1]), high] = (
            partial_ref[rows_of(devices[1]), high].astype(jnp.float32) + in_y[0, :, small].astype(jnp.float32)
        ).astype(jnp.bfloat16)
        last_x = r_copy(chunk, 9, partial_ref.at[rows_of(devices[1]), high], last_ref.at[1, :, small], me + across)
        lasts[chunk] = (near_x, last_y, near_y, last_x)

    def embed(chunk):
        low, high, small = halves(chunk)
        near_x, last_y, near_y, last_x = lasts[chunk]
        pieces = []
        for at, (place, near, last, side) in enumerate(((low, near_x, last_y, in_x), (high, near_y, last_x, in_y))):
            near.wait_recv()
            last.wait_recv()
            total = (
                partial_ref[rows_of(me), place].astype(jnp.float32)
                + side[1, :, small].astype(jnp.float32) + last_ref[at, :, small].astype(jnp.float32)
            )
            rows = (total + b2_ref[:, place]).astype(jnp.bfloat16)
            send_ref[:, place] = jnp.dot(selector, rows, preferred_element_type=jnp.float32).astype(jnp.bfloat16)
        cut = pl.ds(chunk * wide, wide)
        z_copies[chunk] = [
            z_copy(chunk, place, send_ref.at[block_of(peers[place]), cut], arrived_ref.at[own_block, cut])
            for place in range(groups - 1)
        ]
        arrived_ref[own_block, cut] = send_ref[own_block, cut]

    sequence_all = Gather(rows_ref, slots, wide, a_send, a_recv)

    def choose(chunk):
        cut = pl.ds(chunk * wide, wide)
        if chunk == 0:
            loads[3].wait()
            for item in mark_copies:
                item.wait_recv()
            own_square[...] = jnp.zeros_like(own_square)
        image_here = jnp.dot(picker, arrived_marks[...], preferred_element_type=jnp.float32)[:, :1] > 0.5
        for item in z_copies[chunk]:
            item.wait_recv()
        picked = jnp.dot(picker, arrived_ref[:, cut], preferred_element_type=jnp.float32)
        sequence = jnp.where(image_here, picked, text_ref[:, cut].astype(jnp.float32))
        squares = sequence * sequence
        total = squares[:, :128]
        for at in range(128, wide, 128):
            total = total + squares[:, at:at + 128]
        own_square[pl.ds(0, slots), :] += total
        rows_ref[pl.ds(pl.multiple_of(me * slots, slots), slots), cut] = (
            sequence * gain_ref[:, cut]
        ).astype(jnp.bfloat16)
        sequence_all.begin(chunk)

    square_copies = []

    def share_squares():
        square_ref[me] = jnp.broadcast_to(jnp.sum(own_square[...].T, axis=0, keepdims=True), square_ref.shape[1:])
        for place, other in enumerate(others):
            square_copies.append(
                remote(square_ref.at[me], square_ref.at[me], s_send.at[place], s_recv.at[place], {"mp": other})
            )

    queries = q_ref.shape[1]
    columns = kv_ref.shape[0]

    def project_into(chunk, at, size, weight, dims):
        value = lax.dot_general(
            rows_ref[:, pl.ds(chunk * wide, wide)], weight, (((1,), (dims,)), ((), ())), preferred_element_type=jnp.float32
        )
        place = pl.ds(at, size)
        if chunk:
            value = value + acc_ref[:, place]
        acc_ref[:, place] = value

    def project_kv(chunk):
        sequence_all.finish(chunk)
        if chunk == 0:
            loads[1].wait()
            loads[4].wait()
        project_into(chunk, queries, columns, kv_ref[:, pl.ds(chunk * wide, wide)], 1)

    def project_q(chunk):
        for at, size in tiles_of(queries):
            project_into(chunk, at, size, q_ref[pl.ds(chunk * wide, wide), pl.ds(at, size)], 0)

    def stage(run, chunk):
        if 0 <= chunk < steps:
            run(chunk)

    for step in range(steps + 6):
        stage(second, step)
        stage(add_mates, step - 1)
        stage(via, step - 2)
        stage(embed, step - 3)
        stage(choose, step - 4)
        if step - 4 == steps - 1:
            share_squares()
        stage(sequence_all.forward, step - 5)
        stage(sequence_all.corner, step - 6)
        stage(project_kv, step - 7)
        stage(project_q, step - 7)
    for item in square_copies:
        item.wait_recv()
    project_kv(steps - 1)

    scales = [
        lax.rsqrt(column_of(square_ref[rank, pl.ds(0, 1), pl.ds(0, slots)]) / width + epsilon) for rank in range(ranks)
    ]
    length = ranks * slots
    scaled = jnp.concatenate(
        [acc_ref[pl.ds(rank * slots, slots), pl.ds(queries, columns)] * scales[rank] for rank in range(ranks)], axis=0
    )
    bias = jnp.concatenate([kvb_ref[pl.ds(0, 1), :], kvb_ref[pl.ds(1, 1), :]], axis=1)
    both = (scaled + bias).astype(jnp.bfloat16)
    dims = columns // (2 * KVH)
    row = iota((columns, columns), 0)
    wanted = (row // dims) % 2 * (dims * KVH) + row % dims * KVH + row // (2 * dims)
    turn = jnp.where(iota((columns, columns), 1) == wanted, 1.0, 0.0).astype(jnp.bfloat16)
    turned_ref[...] = lax.dot_general(
        turn, both, (((1,), (1,)), ((), ())), preferred_element_type=jnp.float32
    ).astype(jnp.bfloat16)
    heads_here = queries // HD
    group_size = QH // KVH

    def head_rows(device):
        return pl.ds(pl.multiple_of(device * heads_here // group_size * (2 * dims), 2 * dims), 2 * dims)

    head_copies = [
        remote(turned_ref.at[head_rows(other)], heads_ref.at[me], k_send.at[place], k_recv.at[place], {"mp": other})
        for place, other in enumerate(others)
    ]
    heads_ref[me] = turned_ref[head_rows(me), :]
    project_q(steps - 1)
    for rank in range(ranks):
        some = pl.ds(rank * slots, slots)
        query_ref[some, :] = (acc_ref[some, pl.ds(0, queries)] * scales[rank] + qb_ref[...]).astype(jnp.bfloat16)
    for item in head_copies:
        item.wait_recv()
    tall = 128
    keys = heads_ref[:, pl.ds(0, dims), :].reshape(ranks * dims, length)
    values = heads_ref[:, pl.ds(dims, dims), :].reshape(ranks * dims, length)
    allowed = iota((tall, tall), 0) >= iota((tall, tall), 1)
    for block in range(length // tall):
        reach = (block + 1) * tall
        some = pl.ds(block * tall, tall)
        weighted = []
        for head in range(heads_here):
            scores = jnp.dot(
                query_ref[some, pl.ds(head * HD, HD)], keys[:, :reach], preferred_element_type=jnp.float32
            ) * HD ** (-0.5)
            last = jnp.where(allowed, scores[:, block * tall:], -1e30)
            scores = jnp.concatenate([scores[:, :block * tall], last], axis=1) if block else last
            weights = jnp.exp(scores - jnp.max(scores, axis=-1, keepdims=True))
            total = jnp.sum(weights, axis=-1, keepdims=True)
            weighted.append((weights.astype(jnp.bfloat16), total))
        out_ref[some, :] = jnp.concatenate([
            lax.dot_general(
                weights, values[:, :reach], (((1,), (1,)), ((), ())), preferred_element_type=jnp.float32
            ) * (1.0 / total)
            for weights, total in weighted
        ], axis=1).astype(jnp.bfloat16)
    for item in pending:
        item.wait_send()


def fused(
    patches, window_ids, owner, slot_of_row, text, vit_norm, vit_qkv_w, vit_qkv_b, vit_out_w, merge_norm,
    w1, b1, w2, b2, gain, q_w, q_b, kv_w, kv_b, collective_id,
):
    groups, ranks = lax.axis_size("dp"), lax.axis_size("mp")
    mine = owner.shape[0]
    parts = patches.shape[0] // mine
    slots, width = text.shape
    steps = STEPS
    half = width // 2
    queries, columns = q_w.shape[1], 2 * kv_w.shape[2]
    length = ranks * slots
    hbm = pl.BlockSpec(memory_space=pl.ANY)
    dma = pltpu.SemaphoreType.DMA
    bf16, f32 = jnp.bfloat16, jnp.float32
    smalls = (
        window_ids, vit_norm, vit_qkv_b, merge_norm, owner.reshape(1, -1), slot_of_row, b1,
        b2.reshape(1, -1), gain.reshape(1, -1), q_b.reshape(1, -1), kv_b,
    )
    return pl.pallas_call(
        functools.partial(fused_kernel, groups, ranks, steps, parts),
        out_shape=jax.ShapeDtypeStruct((length, queries), bf16),
        in_specs=[hbm] * 19,
        out_specs=pl.BlockSpec(memory_space=pltpu.VMEM),
        scratch_shapes=[pltpu.VMEM(item.shape, item.dtype) for item in smalls] + [
            dma((len(smalls),)),
            pltpu.VMEM(patches.shape, bf16),
            pltpu.VMEM(vit_qkv_w.shape, bf16),
            pltpu.VMEM(vit_out_w.shape, bf16),
            pltpu.VMEM((vit_qkv_w.shape[1], patches.shape[0]), bf16),
            pltpu.VMEM((vit_out_w.shape[0], patches.shape[0]), f32),
            pltpu.VMEM(w1.shape, bf16),
            pltpu.VMEM(w2.shape, bf16),
            pltpu.VMEM(q_w.shape, bf16),
            pltpu.VMEM((columns, width), bf16),
            pltpu.VMEM((slots, width), bf16),
            pltpu.VMEM((ranks * mine, w1.shape[0]), bf16),
            pltpu.VMEM((ranks * mine, w1.shape[1]), f32),
            pltpu.VMEM((ranks * mine, w1.shape[1]), bf16),
            pltpu.VMEM((ranks * mine, width), bf16),
            pltpu.VMEM((4, mine, width), bf16),
            pltpu.VMEM((2, mine, half), bf16),
            pltpu.VMEM((2, mine, half), bf16),
            pltpu.VMEM((2, mine, half), bf16),
            pltpu.VMEM((slots, width), bf16),
            pltpu.VMEM((slots, width), bf16),
            pltpu.VMEM((slots, 128), bf16),
            pltpu.VMEM((slots, 128), bf16),
            pltpu.VMEM((length, width), bf16),
            pltpu.VMEM((length, queries + columns), f32),
            pltpu.VMEM((128, 128), f32),
            pltpu.VMEM((ranks, 8, 128), f32),
            pltpu.VMEM((columns, length), bf16),
            pltpu.VMEM((ranks, columns // KVH, length), bf16),
            pltpu.VMEM((length, queries), bf16),
            dma((8,)),
            dma((parts, 11)), dma((parts, 11)),
            dma((steps, 10)), dma((steps, 10)),
            dma((steps + 1, groups - 1)), dma((steps + 1, groups - 1)),
            dma((steps, 11)), dma((steps, 11)),
            dma((ranks - 1,)), dma((ranks - 1,)),
            dma((ranks - 1,)), dma((ranks - 1,)),
        ],
        compiler_params=pltpu.CompilerParams(collective_id=collective_id, has_side_effects=True, vmem_limit_bytes=TOP),
        cost_estimate=pl.CostEstimate(flops=2 * length * width * (queries + columns), bytes_accessed=12 * length * width, transcendentals=0),
    )(
        *smalls, patches, vit_qkv_w, vit_out_w, w1, w2, q_w, kv_w.transpose(0, 2, 1).reshape(columns, width), text,
    )


def vision_block(patches, window_ids, vit_norm, vit_qkv_w, vit_qkv_b, vit_out_w, merge_norm):
    normed = rms_norm(patches, vit_norm).astype(jnp.bfloat16)
    projected = (jnp.dot(normed, vit_qkv_w, preferred_element_type=jnp.float32) + vit_qkv_b).astype(
        jnp.bfloat16
    )
    blocks = window_ids.shape[0]
    width = window_ids.shape[1]
    inner_width = vit_out_w.shape[0]
    heads = inner_width // VHD
    shaped = projected.reshape(blocks, width, 3, heads, VHD)
    scores = jnp.einsum(
        "bqhd,bkhd->bhqk", shaped[:, :, 0], shaped[:, :, 1], preferred_element_type=jnp.float32
    ) * VHD ** (-0.5)
    in_window = window_ids[:, None, :, None] == window_ids[:, None, None, :]
    scores = jnp.where(in_window, scores, -1e30)
    peak = jnp.max(scores, axis=-1, keepdims=True)
    weights = jnp.exp(scores - peak)
    weights = (weights / jnp.sum(weights, axis=-1, keepdims=True)).astype(jnp.bfloat16)
    mixture = jnp.einsum(
        "bhqk,bkhd->bqhd", weights, shaped[:, :, 2], preferred_element_type=jnp.float32
    )
    mixture = mixture.astype(jnp.bfloat16).reshape(blocks * width, inner_width)
    residual = (
        patches.astype(jnp.float32)
        + jnp.dot(mixture, vit_out_w, preferred_element_type=jnp.float32)
    ).astype(jnp.bfloat16)
    merged = rms_norm(residual, merge_norm).astype(jnp.bfloat16)
    return merged.reshape(blocks * width // 4, 4 * patches.shape[1])


def shards(
    patches,
    window_ids,
    owner,
    slot_of_row,
    text_embeds,
    vit_norm,
    vit_qkv_w,
    vit_qkv_b,
    vit_out_w,
    merge_norm,
    merge_w1,
    merge_b1,
    merge_w2,
    merge_b2,
    llm_norm,
    q_w,
    q_b,
    kv_w,
    kv_b,
):
    if lax.axis_size("mp") == 8:
        return fused(
            patches, window_ids, owner, slot_of_row, text_embeds, vit_norm, vit_qkv_w, vit_qkv_b, vit_out_w,
            merge_norm, merge_w1, merge_b1, merge_w2, merge_b2, llm_norm, q_w, q_b, kv_w, kv_b, 2,
        )
    merged = vision_block(
        patches, window_ids, vit_norm, vit_qkv_w, vit_qkv_b, vit_out_w, merge_norm
    )
    rows_all = gather_mp(merged, 0)
    hidden = jax.nn.gelu(
        jnp.dot(rows_all, merge_w1, preferred_element_type=jnp.float32) + merge_b1,
        approximate=False,
    ).astype(jnp.bfloat16)
    own_rows = scatter_mp(
        jnp.dot(hidden, merge_w2, preferred_element_type=jnp.float32).astype(jnp.bfloat16), 1
    )
    embedded = (own_rows + merge_b2).astype(jnp.bfloat16)
    seq_rows = text_embeds.shape[0]
    groups = lax.axis_size("dp")
    capacity = seq_rows // groups
    target_group = owner[:, 0]
    onehot = (target_group[:, None] == jnp.arange(groups, dtype=jnp.int32)[None, :]).astype(
        jnp.int32
    )
    rank_in = jnp.sum((jnp.cumsum(onehot, axis=0) - onehot) * onehot, axis=1)
    send_slot = target_group * capacity + rank_in
    selector = send_slot[None, :] == jnp.arange(seq_rows, dtype=jnp.int32)[:, None]
    query_cols = q_w.shape[1]
    kv_cols = kv_w.shape[2]
    if lax.axis_size("mp") == 8:
        picker = slot_of_row[0][:, None] == jnp.arange(seq_rows, dtype=jnp.int32)[None, :]
        kv_both = jnp.concatenate([kv_w[0], kv_w[1]], axis=1)
        projected, squares = handover(embedded, selector, picker, text_embeds, llm_norm, q_w, kv_both, 2)
        squares = squares[:, 0, :seq_rows].reshape(-1, 1)
        projected = projected * lax.rsqrt(squares / text_embeds.shape[1] + epsilon)
    else:
        buffer = jnp.dot(
            selector.astype(jnp.bfloat16), embedded, preferred_element_type=jnp.float32
        ).astype(jnp.bfloat16)
        buffer = buffer.reshape(groups, capacity, embedded.shape[1])
        counts = jnp.broadcast_to(jnp.sum(onehot, axis=0)[:, None, None], (groups, 8, 128))
        arrived, arrived_counts = exchange((buffer, counts), "dp", lambda target: target, 2)
        arrived = arrived.reshape(seq_rows, embedded.shape[1])
        chosen = slot_of_row[0]
        places = jnp.arange(seq_rows, dtype=jnp.int32)
        filled = places % capacity < jnp.repeat(arrived_counts[:, 0, 0], capacity)
        chooser = (chosen[:, None] == places[None, :]) & filled[None, :]
        picked = jnp.dot(chooser.astype(jnp.bfloat16), arrived, preferred_element_type=jnp.float32)
        image_here = jnp.any(chooser, axis=1)[:, None]
        sequence = jnp.where(image_here, picked, text_embeds.astype(jnp.float32))
        llm_normed = rms_norm(sequence, llm_norm).astype(jnp.bfloat16)
        shard_rows = gather_mp(llm_normed, 3)
        projected = jnp.concatenate(
            [
                jnp.dot(shard_rows, q_w, preferred_element_type=jnp.float32),
                jnp.dot(shard_rows, kv_w[0], preferred_element_type=jnp.float32),
                jnp.dot(shard_rows, kv_w[1], preferred_element_type=jnp.float32),
            ],
            axis=1,
        )
    length = projected.shape[0]
    queries = (projected[:, :query_cols] + q_b).astype(jnp.bfloat16)
    key_rows = (projected[:, query_cols : query_cols + kv_cols] + kv_b[0]).astype(jnp.bfloat16)
    value_rows = (projected[:, query_cols + kv_cols :] + kv_b[1]).astype(jnp.bfloat16)
    heads_here = query_cols // HD
    group_size = QH // KVH
    dims_here = kv_cols // KVH

    def head_major(columns):
        return columns.T.reshape(dims_here, KVH, length).swapaxes(0, 1)

    stacked = jnp.stack([head_major(key_rows), head_major(value_rows)], axis=1)
    (own_head,) = exchange((stacked,), "mp", lambda target: target * heads_here // group_size, 4)
    key_cols = own_head[:, 0].reshape(HD, length)
    value_cols = own_head[:, 1].reshape(HD, length)
    query_heads = queries.reshape(length, heads_here, HD)
    scores = jnp.einsum(
        "qhd,dk->hqk", query_heads, key_cols, preferred_element_type=jnp.float32
    ) * HD ** (-0.5)
    allowed = jnp.arange(length)[:, None] >= jnp.arange(length)[None, :]
    scores = jnp.where(allowed[None], scores, -1e30)
    peak = jnp.max(scores, axis=-1, keepdims=True)
    weights = jnp.exp(scores - peak)
    weights = (weights / jnp.sum(weights, axis=-1, keepdims=True)).astype(jnp.bfloat16)
    mixture = jnp.einsum("hqk,dk->qhd", weights, value_cols, preferred_element_type=jnp.float32)
    return mixture.astype(jnp.bfloat16).reshape(length, query_cols)


def solution(mesh):
    return jax.shard_map(
        shards,
        mesh=mesh,
        in_specs=(
            P(("dp", "mp"), None),
            P(("dp", "mp"), None),
            P(("dp", "mp"), None),
            P(("dp", "mp"), None),
            P(("dp", "mp"), None),
            P(),
            P(),
            P(),
            P(),
            P(),
            P(None, "mp"),
            P("mp"),
            P("mp", None),
            P(),
            P(),
            P(None, "mp"),
            P("mp"),
            P(None, None, "mp"),
            P(None, "mp"),
        ),
        out_specs=P("dp", "mp"),
        check_vma=False,
    )
```

```python
import functools
import jax
import jax.numpy as jnp
from jax import lax
from jax.experimental import pallas as pl
from jax.experimental.pallas import tpu as pltpu
from jax.sharding import PartitionSpec as P

VHD = 80
HD = 128
QH = 32
KVH = 4

MESH = pl.DeviceIdType.MESH
LIMIT = 60 * 1024 * 1024


def corners():
    me = lax.axis_index("mp")
    core, first, second = me % 2, (me // 2) % 2, me // 4
    partner = 1 - 2 * core
    across = 2 - 4 * first
    up = 4 - 8 * second
    return me, partner, across, up


def greet(axis, others):
    barrier = pltpu.get_barrier_semaphore()
    for other in others:
        pl.semaphore_signal(barrier, inc=1, device_id={axis: other}, device_id_type=MESH)
    pl.semaphore_wait(barrier, len(others))


def gather_kernel(rows, in_ref, out_ref, local_sem, send_sem, recv_sem):
    me, partner, across, up = corners()
    greet("mp", (me + partner, me + across, me + up))
    half = rows // 2

    def piece(device, part):
        if part is None:
            return out_ref.at[pl.ds(pl.multiple_of(device * rows, rows), rows)]
        return out_ref.at[pl.ds(pl.multiple_of(device * rows + part * half, half), half)]

    def own(part):
        return in_ref if part is None else in_ref.at[pl.ds(part * half, half)]

    def copy(index, device, part, target, mine=False):
        return pltpu.make_async_remote_copy(
            src_ref=own(part) if mine else piece(device, part),
            dst_ref=piece(device, part),
            send_sem=send_sem.at[index],
            recv_sem=recv_sem.at[index],
            device_id={"mp": target},
            device_id_type=MESH,
        )

    x0 = copy(0, me, 0, me + across, True)
    y1 = copy(4, me, 1, me + up, True)
    x1 = copy(1, me, 1, me + across, True)
    y0 = copy(3, me, 0, me + up, True)
    mate = copy(6, me, None, me + partner, True)
    for item in (x0, y1, x1, y0, mate):
        item.start()
    keep = pltpu.make_async_copy(in_ref, piece(me, None), local_sem)
    keep.start()
    x0.wait_recv()
    far0 = copy(5, me + across, 0, me + up)
    far0.start()
    y1.wait_recv()
    far1 = copy(2, me + up, 1, me + across)
    far1.start()
    x1.wait_recv()
    mate_x = copy(7, me + across, None, me + partner)
    mate_x.start()
    y0.wait_recv()
    mate_y = copy(8, me + up, None, me + partner)
    mate_y.start()
    far0.wait_recv()
    mate_f0 = copy(9, me + across + up, 0, me + partner)
    mate_f0.start()
    far1.wait_recv()
    mate_f1 = copy(10, me + across + up, 1, me + partner)
    mate_f1.start()
    for item in (mate, mate_x, mate_y, mate_f0, mate_f1):
        item.wait_recv()
    for item in (x0, x1, y0, y1, far0, far1, mate, mate_x, mate_y, mate_f0, mate_f1):
        item.wait_send()
    keep.wait()


def gather_mp(block, collective_id):
    ranks = lax.axis_size("mp")
    if ranks != 8:
        return lax.all_gather(block, "mp", axis=0, tiled=True)
    rows, columns = block.shape
    return pl.pallas_call(
        functools.partial(gather_kernel, rows),
        out_shape=jax.ShapeDtypeStruct((ranks * rows, columns), block.dtype),
        in_specs=[pl.BlockSpec(memory_space=pltpu.VMEM)],
        out_specs=pl.BlockSpec(memory_space=pl.ANY),
        scratch_shapes=[
            pltpu.SemaphoreType.DMA,
            pltpu.SemaphoreType.DMA((11,)),
            pltpu.SemaphoreType.DMA((11,)),
        ],
        compiler_params=pltpu.CompilerParams(collective_id=collective_id, has_side_effects=True),
        cost_estimate=pl.CostEstimate(flops=0, bytes_accessed=ranks * block.size * 2, transcendentals=0),
    )(block)


def scatter_kernel(in_ref, out_ref, mate_ref, sum_ref, in_x, in_y, via_ref, last_ref, send_sem, recv_sem):
    me, partner, across, up = corners()
    greet("mp", (me + partner, me + across, me + up))
    columns = in_ref.shape[2]
    half = columns // 2
    step = min(half, 1024)
    devices = (me + across + up, me + across, me + up, me)

    def copy(index, src, dst, target):
        return pltpu.make_async_remote_copy(
            src_ref=src, dst_ref=dst, send_sem=send_sem.at[index], recv_sem=recv_sem.at[index],
            device_id={"mp": target}, device_id_type=MESH,
        )

    def tiles(body):
        def run(i, carry):
            body(pl.multiple_of(i * step, step))
            return carry
        lax.fori_loop(0, half // step, run, 0)

    mates = []
    for slot in range(4):
        item = copy(slot, in_ref.at[devices[slot] + partner], mate_ref.at[slot], me + partner)
        item.start()
        mates.append(item)

    def add_mate(slot):
        mates[slot].wait_recv()
        for part in range(2):
            def body(at):
                cut = pl.ds(part * half + at, step)
                sum_ref[slot, :, cut] = (
                    in_ref[devices[slot], :, cut].astype(jnp.float32) + mate_ref[slot, :, cut].astype(jnp.float32)
                ).astype(jnp.bfloat16)
            tiles(body)

    low, high = pl.ds(0, half), pl.ds(half, half)
    add_mate(0)
    far_x = copy(4, sum_ref.at[0, :, low], in_x.at[0], me + across)
    far_x.start()
    far_y = copy(5, sum_ref.at[0, :, high], in_y.at[0], me + up)
    far_y.start()
    add_mate(1)
    near_x = copy(6, sum_ref.at[1, :, low], in_x.at[1], me + across)
    near_x.start()
    add_mate(2)
    near_y = copy(7, sum_ref.at[2, :, high], in_y.at[1], me + up)
    near_y.start()
    add_mate(3)
    far_x.wait_recv()

    def via_low(at):
        cut = pl.ds(at, step)
        via_ref[0, :, cut] = (
            sum_ref[2, :, cut].astype(jnp.float32) + in_x[0, :, cut].astype(jnp.float32)
        ).astype(jnp.bfloat16)
    tiles(via_low)
    last_y = copy(8, via_ref.at[0], last_ref.at[0], me + up)
    last_y.start()
    far_y.wait_recv()

    def via_high(at):
        cut = pl.ds(at, step)
        via_ref[1, :, cut] = (
            sum_ref[1, :, pl.ds(half + at, step)].astype(jnp.float32) + in_y[0, :, cut].astype(jnp.float32)
        ).astype(jnp.bfloat16)
    tiles(via_high)
    last_x = copy(9, via_ref.at[1], last_ref.at[1], me + across)
    last_x.start()
    near_x.wait_recv()
    last_y.wait_recv()

    def own_low(at):
        cut = pl.ds(at, step)
        out_ref[:, cut] = (
            sum_ref[3, :, cut].astype(jnp.float32)
            + in_x[1, :, cut].astype(jnp.float32) + last_ref[0, :, cut].astype(jnp.float32)
        )
    tiles(own_low)
    near_y.wait_recv()
    last_x.wait_recv()

    def own_high(at):
        cut, wide = pl.ds(at, step), pl.ds(half + at, step)
        out_ref[:, wide] = (
            sum_ref[3, :, wide].astype(jnp.float32)
            + in_y[1, :, cut].astype(jnp.float32) + last_ref[1, :, cut].astype(jnp.float32)
        )
    tiles(own_high)
    for item in mates + [far_x, far_y, near_x, near_y, last_x, last_y]:
        item.wait_send()


def scatter_mp(partial, collective_id):
    ranks = lax.axis_size("mp")
    if ranks != 8:
        return lax.psum_scatter(partial, "mp", scatter_dimension=0, tiled=True).astype(jnp.float32)
    rows, columns = partial.shape[0] // ranks, partial.shape[1]
    half = columns // 2
    return pl.pallas_call(
        scatter_kernel,
        out_shape=jax.ShapeDtypeStruct((rows, columns), jnp.float32),
        in_specs=[pl.BlockSpec(memory_space=pltpu.VMEM)],
        out_specs=pl.BlockSpec(memory_space=pltpu.VMEM),
        scratch_shapes=[
            pltpu.VMEM((4, rows, columns), jnp.bfloat16),
            pltpu.VMEM((4, rows, columns), jnp.bfloat16),
            pltpu.VMEM((2, rows, half), jnp.bfloat16),
            pltpu.VMEM((2, rows, half), jnp.bfloat16),
            pltpu.VMEM((2, rows, half), jnp.bfloat16),
            pltpu.VMEM((2, rows, half), jnp.bfloat16),
            pltpu.SemaphoreType.DMA((10,)),
            pltpu.SemaphoreType.DMA((10,)),
        ],
        compiler_params=pltpu.CompilerParams(collective_id=collective_id, has_side_effects=True),
        cost_estimate=pl.CostEstimate(flops=0, bytes_accessed=partial.size * 4, transcendentals=0),
    )(partial.reshape(ranks, rows, columns))


def exchange_kernel(axis, ranks, pick, count, *refs):
    ins, outs = refs[:count], refs[count:2 * count]
    local_sem, send_sem, recv_sem = refs[2 * count:]
    me = lax.axis_index(axis)
    targets = [lax.rem(me + step, ranks) for step in range(1, ranks)]
    greet(axis, targets)
    copies = []
    for index in range(count):
        for place, target in enumerate(targets):
            item = pltpu.make_async_remote_copy(
                src_ref=ins[index].at[pick(target)], dst_ref=outs[index].at[me],
                send_sem=send_sem.at[index, place], recv_sem=recv_sem.at[index, place],
                device_id={axis: target}, device_id_type=MESH,
            )
            item.start()
            copies.append(item)
        item = pltpu.make_async_copy(ins[index].at[pick(me)], outs[index].at[me], local_sem.at[index])
        item.start()
        copies.append(item)
    for item in copies:
        item.wait()


def exchange(arrays, axis, pick, collective_id):
    ranks = lax.axis_size(axis)
    return pl.pallas_call(
        functools.partial(exchange_kernel, axis, ranks, pick, len(arrays)),
        out_shape=[jax.ShapeDtypeStruct((ranks,) + a.shape[1:], a.dtype) for a in arrays],
        in_specs=[pl.BlockSpec(memory_space=pltpu.VMEM)] * len(arrays),
        out_specs=[pl.BlockSpec(memory_space=pltpu.VMEM)] * len(arrays),
        scratch_shapes=[
            pltpu.SemaphoreType.DMA((len(arrays),)),
            pltpu.SemaphoreType.DMA((len(arrays), ranks - 1)),
            pltpu.SemaphoreType.DMA((len(arrays), ranks - 1)),
        ],
        compiler_params=pltpu.CompilerParams(collective_id=collective_id, has_side_effects=True),
        cost_estimate=pl.CostEstimate(flops=0, bytes_accessed=4 * sum(a.size for a in arrays), transcendentals=0),
    )(*arrays)


CHUNKS = 4


def handover_kernel(
    groups, ranks, emb_ref, selector_ref, marks_ref, picker_ref, text_ref, gain_ref, q_ref, kv_ref,
    out_ref, square_ref,
    send_ref, arrived_ref, arrived_marks, rows_ref, q_here, kv_here, own_square,
    load_sem, z_send, z_recv, send_sem, recv_sem, s_send, s_recv,
):
    me, partner, across, up = corners()
    group = lax.axis_index("dp")
    peers = [lax.rem(group + step, groups) for step in range(1, groups)]
    others = [lax.rem(me + step, ranks) for step in range(1, ranks)]
    loads = [pltpu.make_async_copy(q_ref, q_here, load_sem.at[0]), pltpu.make_async_copy(kv_ref, kv_here, load_sem.at[1])]
    for item in loads:
        item.start()
    barrier = pltpu.get_barrier_semaphore()
    for peer in peers:
        pl.semaphore_signal(barrier, inc=1, device_id={"dp": peer}, device_id_type=MESH)
    for other in others:
        pl.semaphore_signal(barrier, inc=1, device_id={"mp": other}, device_id_type=MESH)
    pl.semaphore_wait(barrier, groups + ranks - 2)

    slots, width = text_ref.shape
    room = slots // groups
    wide = width // CHUNKS
    half = slots // 2

    def block_of(index):
        return pl.ds(pl.multiple_of(index * room, room), room)

    own_block = block_of(group)
    pending = []

    def z_copy(index, place, src, dst):
        item = pltpu.make_async_remote_copy(
            src_ref=src, dst_ref=dst, send_sem=z_send.at[index, place], recv_sem=z_recv.at[index, place],
            device_id={"dp": peers[place]}, device_id_type=MESH,
        )
        item.start()
        pending.append(item)
        return item

    mark_copies = [
        z_copy(CHUNKS, place, marks_ref.at[block_of(peers[place])], arrived_marks.at[own_block])
        for place in range(groups - 1)
    ]
    arrived_marks[own_block, :] = marks_ref[own_block, :]
    z_copies = []
    for chunk in range(CHUNKS):
        cut = pl.ds(chunk * wide, wide)
        send_ref[:, cut] = jnp.dot(
            selector_ref[...], emb_ref[:, cut], preferred_element_type=jnp.float32
        ).astype(jnp.bfloat16)
        z_copies.append([
            z_copy(chunk, place, send_ref.at[block_of(peers[place]), cut], arrived_ref.at[own_block, cut])
            for place in range(groups - 1)
        ])
        arrived_ref[own_block, cut] = send_ref[own_block, cut]

    def piece(device, part, cut):
        if part is None:
            return rows_ref.at[pl.ds(pl.multiple_of(device * slots, slots), slots), cut]
        return rows_ref.at[pl.ds(pl.multiple_of(device * slots + part * half, half), half), cut]

    def copy(chunk, index, device, part, target):
        ref = piece(device, part, pl.ds(chunk * wide, wide))
        item = pltpu.make_async_remote_copy(
            src_ref=ref, dst_ref=ref, send_sem=send_sem.at[chunk, index], recv_sem=recv_sem.at[chunk, index],
            device_id={"mp": target}, device_id_type=MESH,
        )
        item.start()
        pending.append(item)
        return item

    for item in mark_copies:
        item.wait_recv()
    image_here = jnp.dot(picker_ref[...], arrived_marks[...], preferred_element_type=jnp.float32)[:, :1] > 0.5
    own_square[...] = jnp.zeros_like(own_square)
    firsts, mates = [], []

    def choose(chunk):
        cut = pl.ds(chunk * wide, wide)
        for item in z_copies[chunk]:
            item.wait_recv()
        picked = jnp.dot(picker_ref[...], arrived_ref[:, cut], preferred_element_type=jnp.float32)
        sequence = jnp.where(image_here, picked, text_ref[:, cut].astype(jnp.float32))
        squares = sequence * sequence
        total = squares[:, :128]
        for at in range(128, wide, 128):
            total = total + squares[:, at:at + 128]
        own_square[pl.ds(0, slots), :] += total
        rows_ref[pl.ds(pl.multiple_of(me * slots, slots), slots), cut] = (
            sequence * gain_ref[:, cut]
        ).astype(jnp.bfloat16)
        x0 = copy(chunk, 0, me, 0, me + across)
        y1 = copy(chunk, 4, me, 1, me + up)
        x1 = copy(chunk, 1, me, 1, me + across)
        y0 = copy(chunk, 3, me, 0, me + up)
        mate = copy(chunk, 6, me, None, me + partner)
        firsts.append((x0, y1, x1, y0))
        mates.append([mate])

    def forward(chunk):
        x0, y1, x1, y0 = firsts[chunk]
        x0.wait_recv()
        far0 = copy(chunk, 5, me + across, 0, me + up)
        y1.wait_recv()
        far1 = copy(chunk, 2, me + up, 1, me + across)
        x1.wait_recv()
        mates[chunk].append(copy(chunk, 7, me + across, None, me + partner))
        y0.wait_recv()
        mates[chunk].append(copy(chunk, 8, me + up, None, me + partner))
        firsts[chunk] = (far0, far1)

    def corner(chunk):
        far0, far1 = firsts[chunk]
        far0.wait_recv()
        mates[chunk].append(copy(chunk, 9, me + across + up, 0, me + partner))
        far1.wait_recv()
        mates[chunk].append(copy(chunk, 10, me + across + up, 1, me + partner))

    queries = q_here.shape[1]
    height = 256

    def project(chunk):
        cut = pl.ds(chunk * wide, wide)
        for item in mates[chunk]:
            item.wait_recv()
        if chunk == 0:
            for item in loads:
                item.wait()

        def run(i, carry):
            some = pl.ds(pl.multiple_of(i * height, height), height)
            left = jnp.dot(rows_ref[some, cut], q_here[cut, :], preferred_element_type=jnp.float32)
            right = jnp.dot(rows_ref[some, cut], kv_here[cut, :], preferred_element_type=jnp.float32)
            if chunk:
                left = left + out_ref[some, pl.ds(0, queries)]
                right = right + out_ref[some, pl.ds(queries, kv_here.shape[1])]
            out_ref[some, pl.ds(0, queries)] = left
            out_ref[some, pl.ds(queries, kv_here.shape[1])] = right
            return carry
        lax.fori_loop(0, ranks * slots // height, run, 0)

    for chunk in range(CHUNKS):
        choose(chunk)
        if chunk > 0:
            forward(chunk - 1)
        if chunk > 1:
            corner(chunk - 2)
            project(chunk - 2)
    square_ref[me] = jnp.broadcast_to(jnp.sum(own_square[...].T, axis=0, keepdims=True), square_ref.shape[1:])
    forward(CHUNKS - 1)
    square_copies = []
    for place, other in enumerate(others):
        item = pltpu.make_async_remote_copy(
            src_ref=square_ref.at[me], dst_ref=square_ref.at[me], send_sem=s_send.at[place], recv_sem=s_recv.at[place],
            device_id={"mp": other}, device_id_type=MESH,
        )
        item.start()
        square_copies.append(item)
    corner(CHUNKS - 2)
    project(CHUNKS - 2)
    corner(CHUNKS - 1)
    project(CHUNKS - 1)
    for item in square_copies:
        item.wait()
    for item in pending:
        item.wait_send()


def handover(embedded, selector, picker, text, gain, q_w, kv_both, collective_id):
    groups, ranks = lax.axis_size("dp"), lax.axis_size("mp")
    slots, width = text.shape
    marks = jnp.broadcast_to(jnp.sum(selector, axis=1, keepdims=True), (slots, 128)).astype(jnp.bfloat16)
    columns = q_w.shape[1] + kv_both.shape[1]
    vmem = pl.BlockSpec(memory_space=pltpu.VMEM)
    hbm = pl.BlockSpec(memory_space=pl.ANY)
    return pl.pallas_call(
        functools.partial(handover_kernel, groups, ranks),
        out_shape=[
            jax.ShapeDtypeStruct((ranks * slots, columns), jnp.float32),
            jax.ShapeDtypeStruct((ranks, 8, 128), jnp.float32),
        ],
        in_specs=[vmem] * 6 + [hbm] * 2,
        out_specs=[vmem] * 2,
        scratch_shapes=[
            pltpu.VMEM((slots, width), jnp.bfloat16),
            pltpu.VMEM((slots, width), jnp.bfloat16),
            pltpu.VMEM((slots, 128), jnp.bfloat16),
            pltpu.VMEM((ranks * slots, width), jnp.bfloat16),
            pltpu.VMEM(q_w.shape, q_w.dtype),
            pltpu.VMEM(kv_both.shape, kv_both.dtype),
            pltpu.VMEM((128, 128), jnp.float32),
            pltpu.SemaphoreType.DMA((2,)),
            pltpu.SemaphoreType.DMA((CHUNKS + 1, groups - 1)),
            pltpu.SemaphoreType.DMA((CHUNKS + 1, groups - 1)),
            pltpu.SemaphoreType.DMA((CHUNKS, 11)),
            pltpu.SemaphoreType.DMA((CHUNKS, 11)),
            pltpu.SemaphoreType.DMA((ranks - 1,)),
            pltpu.SemaphoreType.DMA((ranks - 1,)),
        ],
        compiler_params=pltpu.CompilerParams(collective_id=collective_id, has_side_effects=True, vmem_limit_bytes=LIMIT),
        cost_estimate=pl.CostEstimate(flops=2 * ranks * slots * width * columns, bytes_accessed=12 * ranks * slots * width, transcendentals=0),
    )(embedded, selector.astype(jnp.bfloat16), marks, picker.astype(jnp.bfloat16), text, gain.reshape(1, -1), q_w, kv_both)


epsilon = 1e-06

def rms_norm(inputs, gain):
    inputs = inputs.astype(jnp.float32)
    return inputs * lax.rsqrt(jnp.mean(inputs * inputs, axis=-1, keepdims=True) + epsilon) * gain


UNITS = (4, 6, 6, 6, 6, 4)
WIDE = 256
TOP = 63 * 1024 * 1024


def tiles_of(width):
    return [(at, min(WIDE, width - at)) for at in range(0, width, WIDE)]


def fused_kernel(
    groups, ranks, spans, parts,
    ids_hbm, vnorm_hbm, vbias_hbm, mnorm_hbm, owner_hbm, slots_hbm, b1_hbm, b2_hbm, gain_hbm, qb_hbm, kvb_hbm,
    patches_hbm, vqkv_hbm, vout_hbm, w1_hbm, w2_hbm, q_hbm, kv_hbm, text_hbm,
    out_ref,
    ids_ref, vnorm_ref, vbias_ref, mnorm_ref, owner_ref, slots_ref, b1_ref, b2_ref, gain_ref, qb_ref, kvb_ref,
    small_sem, patches_ref, vqkv_ref, vout_ref, vturn_ref, vmix_ref, w1_ref, w2_ref, q_ref, kv_ref, text_ref,
    all_ref, hidden_acc, hidden_ref, partial_ref, mate_ref, in_x, in_y, last_ref,
    send_ref, arrived_ref, marks_ref, arrived_marks, rows_ref, acc_ref, own_square, square_ref,
    turned_ref, heads_ref, query_ref,
    load_sem, g_send, g_recv, r_send, r_recv, z_send, z_recv, a_send, a_recv, s_send, s_recv, k_send, k_recv,
):
    me, partner, across, up = corners()
    group = lax.axis_index("dp")
    peers = [lax.rem(group + step, groups) for step in range(1, groups)]
    others = [lax.rem(me + step, ranks) for step in range(1, ranks)]
    loads = [
        pltpu.make_async_copy(src, dst, load_sem.at[at])
        for at, (src, dst) in enumerate((
            (w1_hbm, w1_ref), (kv_hbm, kv_ref), (w2_hbm, w2_ref), (text_hbm, text_ref), (q_hbm, q_ref),
            (patches_hbm, patches_ref), (vqkv_hbm, vqkv_ref), (vout_hbm, vout_ref),
        ))
    ]
    smalls = [
        pltpu.make_async_copy(src, dst, small_sem.at[at])
        for at, (src, dst) in enumerate((
            (ids_hbm, ids_ref), (vnorm_hbm, vnorm_ref), (vbias_hbm, vbias_ref), (mnorm_hbm, mnorm_ref),
            (owner_hbm, owner_ref), (slots_hbm, slots_ref), (b1_hbm, b1_ref), (b2_hbm, b2_ref),
            (gain_hbm, gain_ref), (qb_hbm, qb_ref), (kvb_hbm, kvb_ref),
        ))
    ]
    loads[5].start()
    smalls[0].start()
    smalls[1].start()
    loads[6].start()
    loads[7].start()
    for item in smalls[2:]:
        item.start()
    barrier = pltpu.get_barrier_semaphore()
    for peer in peers:
        pl.semaphore_signal(barrier, inc=1, device_id={"dp": peer}, device_id_type=MESH)
    for other in others:
        pl.semaphore_signal(barrier, inc=1, device_id={"mp": other}, device_id_type=MESH)
    pending = []

    def iota(shape, axis):
        return lax.broadcasted_iota(jnp.int32, shape, axis)

    def column_of(row):
        size = row.shape[1]
        eye = iota((size, size), 0) == iota((size, size), 1)
        return jnp.sum(jnp.where(eye, row, 0.0), axis=1, keepdims=True)

    patch_rows, vision_width = patches_ref.shape
    mine = patch_rows // parts
    inner = vout_ref.shape[0]
    vision_heads = inner // VHD
    smalls[0].wait()
    smalls[1].wait()
    ids_row = ids_ref[...].astype(jnp.float32)
    in_window = column_of(ids_row) == ids_row
    loads[5].wait()
    normed = rms_norm(patches_ref[...], vnorm_ref[...].reshape(1, -1)).astype(jnp.bfloat16)
    loads[6].wait()
    for item in smalls[2:]:
        item.wait()
    for item in loads[:5]:
        item.start()
    for at, size in tiles_of(3 * inner):
        value = jnp.dot(normed, vqkv_ref[:, pl.ds(at, size)], preferred_element_type=jnp.float32)
        value = (value + vbias_ref[pl.ds(at, size)].reshape(1, -1)).astype(jnp.bfloat16).astype(jnp.float32)
        for low in range(0, size, 128):
            vturn_ref[pl.ds(at + low, 128), :] = value[:, low:low + 128].T.astype(jnp.bfloat16)
    for head in range(vision_heads):
        query, key, content = (vturn_ref[pl.ds(which * inner + head * VHD, VHD), :] for which in range(3))
        scores = lax.dot_general(
            key, query, (((0,), (0,)), ((), ())), preferred_element_type=jnp.float32
        ) * VHD ** (-0.5)
        scores = jnp.where(in_window, scores, -1e30)
        weights = jnp.exp(scores - jnp.max(scores, axis=0, keepdims=True))
        weights = (weights * (1.0 / jnp.sum(weights, axis=0, keepdims=True))).astype(jnp.bfloat16)
        vmix_ref[pl.ds(head * VHD, VHD), :] = jnp.dot(content, weights, preferred_element_type=jnp.float32)
    loads[7].wait()
    mixed = jnp.concatenate(
        [vmix_ref[pl.ds(at, 128), :].T.astype(jnp.bfloat16) for at in range(0, inner, 128)], axis=1
    )
    residual = (
        patches_ref[...].astype(jnp.float32) + jnp.dot(mixed, vout_ref[...], preferred_element_type=jnp.float32)
    ).astype(jnp.bfloat16)
    merged = rms_norm(residual, mnorm_ref[...].reshape(1, -1)).astype(jnp.bfloat16)
    row = iota((patch_rows, patch_rows), 0)
    regroup = jnp.where(
        iota((patch_rows, patch_rows), 1) == row % mine * parts + row // mine, 1.0, 0.0
    ).astype(jnp.bfloat16)
    regrouped = jnp.dot(regroup, merged, preferred_element_type=jnp.float32).astype(jnp.bfloat16)
    own_rows = pl.ds(pl.multiple_of(me * mine, mine), mine)
    for part in range(parts):
        all_ref[own_rows, pl.ds(part * vision_width, vision_width)] = regrouped[part * mine:(part + 1) * mine, :]
    pl.semaphore_wait(barrier, groups + ranks - 2)

    def remote(src, dst, send, recv, where):
        item = pltpu.make_async_remote_copy(
            src_ref=src, dst_ref=dst, send_sem=send, recv_sem=recv, device_id=where, device_id_type=MESH,
        )
        item.start()
        pending.append(item)
        return item

    class Gather:
        def __init__(self, ref, count, width, send, recv):
            self.ref, self.count, self.width, self.send, self.recv = ref, count, width, send, recv
            self.firsts, self.mates = {}, {}

        def cut(self, chunk):
            return pl.ds(*self.width[chunk])

        def copy(self, chunk, index, device, part, target):
            size = self.count if part is None else self.count // 2
            shift = 0 if part is None else part * size
            ref = self.ref.at[pl.ds(pl.multiple_of(device * self.count + shift, size), size), self.cut(chunk)]
            return remote(ref, ref, self.send.at[chunk, index], self.recv.at[chunk, index], {"mp": target})

        def begin(self, chunk):
            x0 = self.copy(chunk, 0, me, 0, me + across)
            y1 = self.copy(chunk, 4, me, 1, me + up)
            x1 = self.copy(chunk, 1, me, 1, me + across)
            y0 = self.copy(chunk, 3, me, 0, me + up)
            self.mates[chunk] = [self.copy(chunk, 6, me, None, me + partner)]
            self.firsts[chunk] = (x0, y1, x1, y0)

        def forward(self, chunk):
            x0, y1, x1, y0 = self.firsts[chunk]
            x0.wait_recv()
            far0 = self.copy(chunk, 5, me + across, 0, me + up)
            y1.wait_recv()
            far1 = self.copy(chunk, 2, me + up, 1, me + across)
            x1.wait_recv()
            self.mates[chunk].append(self.copy(chunk, 7, me + across, None, me + partner))
            y0.wait_recv()
            self.mates[chunk].append(self.copy(chunk, 8, me + up, None, me + partner))
            self.firsts[chunk] = (far0, far1)

        def corner(self, chunk):
            far0, far1 = self.firsts[chunk]
            far0.wait_recv()
            self.mates[chunk].append(self.copy(chunk, 9, me + across + up, 0, me + partner))
            far1.wait_recv()
            self.mates[chunk].append(self.copy(chunk, 10, me + across + up, 1, me + partner))

        def finish(self, chunk):
            for item in self.mates[chunk]:
                item.wait_recv()

    merged_all = Gather(all_ref, mine, [(part * vision_width, vision_width) for part in range(parts)], g_send, g_recv)
    for part in range(parts):
        merged_all.begin(part)

    slots, width = text_ref.shape
    room = slots // groups
    steps = len(spans)

    own_row = owner_ref[...].astype(jnp.float32)
    same = column_of(own_row) == own_row
    before = iota((mine, mine), 0) < iota((mine, mine), 1)
    rank_row = jnp.sum(jnp.where(same & before, 1.0, 0.0), axis=0, keepdims=True)
    slot_row = own_row * room + rank_row
    selected = jnp.where(iota((slots, mine), 0).astype(jnp.float32) == slot_row, 1.0, 0.0)
    selector = selected.astype(jnp.bfloat16)
    marks_ref[...] = jnp.broadcast_to(jnp.sum(selected, axis=1, keepdims=True), marks_ref.shape).astype(jnp.bfloat16)
    slot_col = column_of(slots_ref[...].astype(jnp.float32))
    picker = jnp.where(slot_col == iota((slots, slots), 1).astype(jnp.float32), 1.0, 0.0).astype(jnp.bfloat16)

    def block_of(index):
        return pl.ds(pl.multiple_of(index * room, room), room)

    own_block = block_of(group)

    def z_copy(index, place, src, dst):
        return remote(src, dst, z_send.at[index, place], z_recv.at[index, place], {"dp": peers[place]})

    mark_copies = [
        z_copy(steps, place, marks_ref.at[block_of(peers[place])], arrived_marks.at[own_block])
        for place in range(groups - 1)
    ]
    arrived_marks[own_block, :] = marks_ref[own_block, :]

    def first(part):
        cut = merged_all.cut(part)
        for at, size in tiles_of(hidden_acc.shape[1]):
            value = jnp.dot(all_ref[:, cut], w1_ref[cut, pl.ds(at, size)], preferred_element_type=jnp.float32)
            if part:
                value = value + hidden_acc[:, pl.ds(at, size)]
            if part < parts - 1:
                hidden_acc[:, pl.ds(at, size)] = value
            else:
                value = value + b1_ref[pl.ds(at, size)].reshape(1, -1)
                value = 0.5 * value * (1.0 + lax.erf(value * (2.0 ** -0.5)))
                hidden_ref[:, pl.ds(at, size)] = value.astype(jnp.bfloat16)

    for part in range(parts):
        merged_all.forward(part)
    loads[0].wait()
    for part in range(parts):
        merged_all.corner(part)
        if part:
            merged_all.finish(part - 1)
            first(part - 1)
    merged_all.finish(parts - 1)
    first(parts - 1)
    loads[2].wait()

    devices = (me + across + up, me + across, me + up, me)

    def rows_of(device):
        return pl.ds(pl.multiple_of(device * mine, mine), mine)

    reduce_mates, outward, lasts, z_copies = {}, {}, {}, {}

    def r_copy(chunk, index, src, dst, target):
        return remote(src, dst, r_send.at[chunk, index], r_recv.at[chunk, index], {"mp": target})

    def halves(chunk):
        start, wide = spans[chunk]
        half = wide // 2
        return pl.ds(start, half), pl.ds(start + half, half), pl.ds(start // 2, half)

    def second(chunk):
        start, wide = spans[chunk]
        for at, size in tiles_of(wide):
            cut = pl.ds(start + at, size)
            partial_ref[:, cut] = jnp.dot(
                hidden_ref[...], w2_ref[:, cut], preferred_element_type=jnp.float32
            ).astype(jnp.bfloat16)
        cut = pl.ds(*spans[chunk])
        reduce_mates[chunk] = [
            r_copy(chunk, slot, partial_ref.at[rows_of(devices[slot] + partner), cut], mate_ref.at[slot, :, cut], me + partner)
            for slot in range(4)
        ]

    def add_mates(chunk):
        low, high, small = halves(chunk)
        cut = pl.ds(*spans[chunk])

        def add(slot):
            reduce_mates[chunk][slot].wait_recv()
            partial_ref[rows_of(devices[slot]), cut] = (
                partial_ref[rows_of(devices[slot]), cut].astype(jnp.float32) + mate_ref[slot, :, cut].astype(jnp.float32)
            ).astype(jnp.bfloat16)

        add(0)
        far_x = r_copy(chunk, 4, partial_ref.at[rows_of(devices[0]), low], in_x.at[0, :, small], me + across)
        far_y = r_copy(chunk, 5, partial_ref.at[rows_of(devices[0]), high], in_y.at[0, :, small], me + up)
        add(1)
        near_x = r_copy(chunk, 6, partial_ref.at[rows_of(devices[1]), low], in_x.at[1, :, small], me + across)
        add(2)
        near_y = r_copy(chunk, 7, partial_ref.at[rows_of(devices[2]), high], in_y.at[1, :, small], me + up)
        add(3)
        outward[chunk] = (far_x, far_y, near_x, near_y)

    def via(chunk):
        low, high, small = halves(chunk)
        far_x, far_y, near_x, near_y = outward[chunk]
        far_x.wait_recv()
        partial_ref[rows_of(devices[2]), low] = (
            partial_ref[rows_of(devices[2]), low].astype(jnp.float32) + in_x[0, :, small].astype(jnp.float32)
        ).astype(jnp.bfloat16)
        last_y = r_copy(chunk, 8, partial_ref.at[rows_of(devices[2]), low], last_ref.at[0, :, small], me + up)
        far_y.wait_recv()
        partial_ref[rows_of(devices[1]), high] = (
            partial_ref[rows_of(devices[1]), high].astype(jnp.float32) + in_y[0, :, small].astype(jnp.float32)
        ).astype(jnp.bfloat16)
        last_x = r_copy(chunk, 9, partial_ref.at[rows_of(devices[1]), high], last_ref.at[1, :, small], me + across)
        lasts[chunk] = (near_x, last_y, near_y, last_x)

    def embed(chunk):
        low, high, small = halves(chunk)
        near_x, last_y, near_y, last_x = lasts[chunk]
        pieces = []
        for at, (place, near, last, side) in enumerate(((low, near_x, last_y, in_x), (high, near_y, last_x, in_y))):
            near.wait_recv()
            last.wait_recv()
            total = (
                partial_ref[rows_of(me), place].astype(jnp.float32)
                + side[1, :, small].astype(jnp.float32) + last_ref[at, :, small].astype(jnp.float32)
            )
            rows = (total + b2_ref[:, place]).astype(jnp.bfloat16)
            send_ref[:, place] = jnp.dot(selector, rows, preferred_element_type=jnp.float32).astype(jnp.bfloat16)
        cut = pl.ds(*spans[chunk])
        z_copies[chunk] = [
            z_copy(chunk, place, send_ref.at[block_of(peers[place]), cut], arrived_ref.at[own_block, cut])
            for place in range(groups - 1)
        ]
        arrived_ref[own_block, cut] = send_ref[own_block, cut]

    sequence_all = Gather(rows_ref, slots, spans, a_send, a_recv)

    def choose(chunk):
        cut = pl.ds(*spans[chunk])
        if chunk == 0:
            loads[3].wait()
            for item in mark_copies:
                item.wait_recv()
            own_square[...] = jnp.zeros_like(own_square)
        image_here = jnp.dot(picker, arrived_marks[...], preferred_element_type=jnp.float32)[:, :1] > 0.5
        for item in z_copies[chunk]:
            item.wait_recv()
        picked = jnp.dot(picker, arrived_ref[:, cut], preferred_element_type=jnp.float32)
        sequence = jnp.where(image_here, picked, text_ref[:, cut].astype(jnp.float32))
        squares = sequence * sequence
        total = squares[:, :128]
        for at in range(128, spans[chunk][1], 128):
            total = total + squares[:, at:at + 128]
        own_square[pl.ds(0, slots), :] += total
        rows_ref[pl.ds(pl.multiple_of(me * slots, slots), slots), cut] = (
            sequence * gain_ref[:, cut]
        ).astype(jnp.bfloat16)
        sequence_all.begin(chunk)

    square_copies = []

    def share_squares():
        square_ref[me] = jnp.broadcast_to(jnp.sum(own_square[...].T, axis=0, keepdims=True), square_ref.shape[1:])
        for place, other in enumerate(others):
            square_copies.append(
                remote(square_ref.at[me], square_ref.at[me], s_send.at[place], s_recv.at[place], {"mp": other})
            )

    queries = q_ref.shape[1]
    columns = kv_ref.shape[0]

    def project_into(chunk, at, size, weight, dims):
        value = lax.dot_general(
            rows_ref[:, pl.ds(*spans[chunk])], weight, (((1,), (dims,)), ((), ())), preferred_element_type=jnp.float32
        )
        place = pl.ds(at, size)
        if chunk:
            value = value + acc_ref[:, place]
        acc_ref[:, place] = value

    def project_kv(chunk):
        sequence_all.finish(chunk)
        if chunk == 0:
            loads[1].wait()
            loads[4].wait()
        project_into(chunk, queries, columns, kv_ref[:, pl.ds(*spans[chunk])], 1)

    def project_q(chunk):
        for at, size in tiles_of(queries):
            project_into(chunk, at, size, q_ref[pl.ds(*spans[chunk]), pl.ds(at, size)], 0)

    def stage(run, chunk):
        if 0 <= chunk < steps:
            run(chunk)

    for step in range(steps + 7):
        stage(second, step - 0)
        stage(add_mates, step - 1)
        stage(via, step - 2)
        stage(embed, step - 3)
        stage(choose, step - 5)
        if step - 5 == steps - 1:
            share_squares()
        stage(sequence_all.forward, step - 6)
        stage(sequence_all.corner, step - 7)
        stage(project_kv, step - 8)
        stage(project_q, step - 8)
    for item in square_copies:
        item.wait_recv()
    project_kv(steps - 1)

    scales = [
        lax.rsqrt(column_of(square_ref[rank, pl.ds(0, 1), pl.ds(0, slots)]) / width + epsilon) for rank in range(ranks)
    ]
    length = ranks * slots
    scaled = jnp.concatenate(
        [acc_ref[pl.ds(rank * slots, slots), pl.ds(queries, columns)] * scales[rank] for rank in range(ranks)], axis=0
    )
    bias = jnp.concatenate([kvb_ref[pl.ds(0, 1), :], kvb_ref[pl.ds(1, 1), :]], axis=1)
    both = (scaled + bias).astype(jnp.bfloat16)
    dims = columns // (2 * KVH)
    row = iota((columns, columns), 0)
    wanted = (row // dims) % 2 * (dims * KVH) + row % dims * KVH + row // (2 * dims)
    turn = jnp.where(iota((columns, columns), 1) == wanted, 1.0, 0.0).astype(jnp.bfloat16)
    turned_ref[...] = lax.dot_general(
        turn, both, (((1,), (1,)), ((), ())), preferred_element_type=jnp.float32
    ).astype(jnp.bfloat16)
    heads_here = queries // HD
    group_size = QH // KVH

    def head_rows(device):
        return pl.ds(pl.multiple_of(device * heads_here // group_size * (2 * dims), 2 * dims), 2 * dims)

    head_copies = [
        remote(turned_ref.at[head_rows(other)], heads_ref.at[me], k_send.at[place], k_recv.at[place], {"mp": other})
        for place, other in enumerate(others)
    ]
    heads_ref[me] = turned_ref[head_rows(me), :]
    project_q(steps - 1)
    for rank in range(ranks):
        some = pl.ds(rank * slots, slots)
        query_ref[some, :] = (acc_ref[some, pl.ds(0, queries)] * scales[rank] + qb_ref[...]).astype(jnp.bfloat16)
    for item in head_copies:
        item.wait_recv()
    tall = 128
    keys = heads_ref[:, pl.ds(0, dims), :].reshape(ranks * dims, length)
    values = heads_ref[:, pl.ds(dims, dims), :].reshape(ranks * dims, length)
    allowed = iota((tall, tall), 0) >= iota((tall, tall), 1)
    for block in range(length // tall):
        reach = (block + 1) * tall
        some = pl.ds(block * tall, tall)
        weighted = []
        for head in range(heads_here):
            scores = jnp.dot(
                query_ref[some, pl.ds(head * HD, HD)], keys[:, :reach], preferred_element_type=jnp.float32
            ) * HD ** (-0.5)
            last = jnp.where(allowed, scores[:, block * tall:], -1e30)
            scores = jnp.concatenate([scores[:, :block * tall], last], axis=1) if block else last
            weights = jnp.exp(scores - jnp.max(scores, axis=-1, keepdims=True))
            total = jnp.sum(weights, axis=-1, keepdims=True)
            weighted.append((weights.astype(jnp.bfloat16), total))
        out_ref[some, :] = jnp.concatenate([
            lax.dot_general(
                weights, values[:, :reach], (((1,), (1,)), ((), ())), preferred_element_type=jnp.float32
            ) * (1.0 / total)
            for weights, total in weighted
        ], axis=1).astype(jnp.bfloat16)
    for item in pending:
        item.wait_send()


def fused(
    patches, window_ids, owner, slot_of_row, text, vit_norm, vit_qkv_w, vit_qkv_b, vit_out_w, merge_norm,
    w1, b1, w2, b2, gain, q_w, q_b, kv_w, kv_b, collective_id,
):
    groups, ranks = lax.axis_size("dp"), lax.axis_size("mp")
    mine = owner.shape[0]
    parts = patches.shape[0] // mine
    slots, width = text.shape
    unit = width // sum(UNITS)
    spans = [(sum(UNITS[:at]) * unit, size * unit) for at, size in enumerate(UNITS)]
    steps = len(spans)
    half = width // 2
    queries, columns = q_w.shape[1], 2 * kv_w.shape[2]
    length = ranks * slots
    hbm = pl.BlockSpec(memory_space=pl.ANY)
    dma = pltpu.SemaphoreType.DMA
    bf16, f32 = jnp.bfloat16, jnp.float32
    smalls = (
        window_ids, vit_norm, vit_qkv_b, merge_norm, owner.reshape(1, -1), slot_of_row, b1,
        b2.reshape(1, -1), gain.reshape(1, -1), q_b.reshape(1, -1), kv_b,
    )
    return pl.pallas_call(
        functools.partial(fused_kernel, groups, ranks, spans, parts),
        out_shape=jax.ShapeDtypeStruct((length, queries), bf16),
        in_specs=[hbm] * 19,
        out_specs=pl.BlockSpec(memory_space=pltpu.VMEM),
        scratch_shapes=[pltpu.VMEM(item.shape, item.dtype) for item in smalls] + [
            dma((len(smalls),)),
            pltpu.VMEM(patches.shape, bf16),
            pltpu.VMEM(vit_qkv_w.shape, bf16),
            pltpu.VMEM(vit_out_w.shape, bf16),
            pltpu.VMEM((vit_qkv_w.shape[1], patches.shape[0]), bf16),
            pltpu.VMEM((vit_out_w.shape[0], patches.shape[0]), f32),
            pltpu.VMEM(w1.shape, bf16),
            pltpu.VMEM(w2.shape, bf16),
            pltpu.VMEM(q_w.shape, bf16),
            pltpu.VMEM((columns, width), bf16),
            pltpu.VMEM((slots, width), bf16),
            pltpu.VMEM((ranks * mine, w1.shape[0]), bf16),
            pltpu.VMEM((ranks * mine, w1.shape[1]), f32),
            pltpu.VMEM((ranks * mine, w1.shape[1]), bf16),
            pltpu.VMEM((ranks * mine, width), bf16),
            pltpu.VMEM((4, mine, width), bf16),
            pltpu.VMEM((2, mine, half), bf16),
            pltpu.VMEM((2, mine, half), bf16),
            pltpu.VMEM((2, mine, half), bf16),
            pltpu.VMEM((slots, width), bf16),
            pltpu.VMEM((slots, width), bf16),
            pltpu.VMEM((slots, 128), bf16),
            pltpu.VMEM((slots, 128), bf16),
            pltpu.VMEM((length, width), bf16),
            pltpu.VMEM((length, queries + columns), f32),
            pltpu.VMEM((128, 128), f32),
            pltpu.VMEM((ranks, 8, 128), f32),
            pltpu.VMEM((columns, length), bf16),
            pltpu.VMEM((ranks, columns // KVH, length), bf16),
            pltpu.VMEM((length, queries), bf16),
            dma((8,)),
            dma((parts, 11)), dma((parts, 11)),
            dma((steps, 10)), dma((steps, 10)),
            dma((steps + 1, groups - 1)), dma((steps + 1, groups - 1)),
            dma((steps, 11)), dma((steps, 11)),
            dma((ranks - 1,)), dma((ranks - 1,)),
            dma((ranks - 1,)), dma((ranks - 1,)),
        ],
        compiler_params=pltpu.CompilerParams(collective_id=collective_id, has_side_effects=True, vmem_limit_bytes=TOP),
        cost_estimate=pl.CostEstimate(flops=2 * length * width * (queries + columns), bytes_accessed=12 * length * width, transcendentals=0),
    )(
        *smalls, patches, vit_qkv_w, vit_out_w, w1, w2, q_w, kv_w.transpose(0, 2, 1).reshape(columns, width), text,
    )


def vision_block(patches, window_ids, vit_norm, vit_qkv_w, vit_qkv_b, vit_out_w, merge_norm):
    normed = rms_norm(patches, vit_norm).astype(jnp.bfloat16)
    projected = (jnp.dot(normed, vit_qkv_w, preferred_element_type=jnp.float32) + vit_qkv_b).astype(
        jnp.bfloat16
    )
    blocks = window_ids.shape[0]
    width = window_ids.shape[1]
    inner_width = vit_out_w.shape[0]
    heads = inner_width // VHD
    shaped = projected.reshape(blocks, width, 3, heads, VHD)
    scores = jnp.einsum(
        "bqhd,bkhd->bhqk", shaped[:, :, 0], shaped[:, :, 1], preferred_element_type=jnp.float32
    ) * VHD ** (-0.5)
    in_window = window_ids[:, None, :, None] == window_ids[:, None, None, :]
    scores = jnp.where(in_window, scores, -1e30)
    peak = jnp.max(scores, axis=-1, keepdims=True)
    weights = jnp.exp(scores - peak)
    weights = (weights / jnp.sum(weights, axis=-1, keepdims=True)).astype(jnp.bfloat16)
    mixture = jnp.einsum(
        "bhqk,bkhd->bqhd", weights, shaped[:, :, 2], preferred_element_type=jnp.float32
    )
    mixture = mixture.astype(jnp.bfloat16).reshape(blocks * width, inner_width)
    residual = (
        patches.astype(jnp.float32)
        + jnp.dot(mixture, vit_out_w, preferred_element_type=jnp.float32)
    ).astype(jnp.bfloat16)
    merged = rms_norm(residual, merge_norm).astype(jnp.bfloat16)
    return merged.reshape(blocks * width // 4, 4 * patches.shape[1])


def shards(
    patches,
    window_ids,
    owner,
    slot_of_row,
    text_embeds,
    vit_norm,
    vit_qkv_w,
    vit_qkv_b,
    vit_out_w,
    merge_norm,
    merge_w1,
    merge_b1,
    merge_w2,
    merge_b2,
    llm_norm,
    q_w,
    q_b,
    kv_w,
    kv_b,
):
    if lax.axis_size("mp") == 8:
        return fused(
            patches, window_ids, owner, slot_of_row, text_embeds, vit_norm, vit_qkv_w, vit_qkv_b, vit_out_w,
            merge_norm, merge_w1, merge_b1, merge_w2, merge_b2, llm_norm, q_w, q_b, kv_w, kv_b, 2,
        )
    merged = vision_block(
        patches, window_ids, vit_norm, vit_qkv_w, vit_qkv_b, vit_out_w, merge_norm
    )
    rows_all = gather_mp(merged, 0)
    hidden = jax.nn.gelu(
        jnp.dot(rows_all, merge_w1, preferred_element_type=jnp.float32) + merge_b1,
        approximate=False,
    ).astype(jnp.bfloat16)
    own_rows = scatter_mp(
        jnp.dot(hidden, merge_w2, preferred_element_type=jnp.float32).astype(jnp.bfloat16), 1
    )
    embedded = (own_rows + merge_b2).astype(jnp.bfloat16)
    seq_rows = text_embeds.shape[0]
    groups = lax.axis_size("dp")
    capacity = seq_rows // groups
    target_group = owner[:, 0]
    onehot = (target_group[:, None] == jnp.arange(groups, dtype=jnp.int32)[None, :]).astype(
        jnp.int32
    )
    rank_in = jnp.sum((jnp.cumsum(onehot, axis=0) - onehot) * onehot, axis=1)
    send_slot = target_group * capacity + rank_in
    selector = send_slot[None, :] == jnp.arange(seq_rows, dtype=jnp.int32)[:, None]
    query_cols = q_w.shape[1]
    kv_cols = kv_w.shape[2]
    if lax.axis_size("mp") == 8:
        picker = slot_of_row[0][:, None] == jnp.arange(seq_rows, dtype=jnp.int32)[None, :]
        kv_both = jnp.concatenate([kv_w[0], kv_w[1]], axis=1)
        projected, squares = handover(embedded, selector, picker, text_embeds, llm_norm, q_w, kv_both, 2)
        squares = squares[:, 0, :seq_rows].reshape(-1, 1)
        projected = projected * lax.rsqrt(squares / text_embeds.shape[1] + epsilon)
    else:
        buffer = jnp.dot(
            selector.astype(jnp.bfloat16), embedded, preferred_element_type=jnp.float32
        ).astype(jnp.bfloat16)
        buffer = buffer.reshape(groups, capacity, embedded.shape[1])
        counts = jnp.broadcast_to(jnp.sum(onehot, axis=0)[:, None, None], (groups, 8, 128))
        arrived, arrived_counts = exchange((buffer, counts), "dp", lambda target: target, 2)
        arrived = arrived.reshape(seq_rows, embedded.shape[1])
        chosen = slot_of_row[0]
        places = jnp.arange(seq_rows, dtype=jnp.int32)
        filled = places % capacity < jnp.repeat(arrived_counts[:, 0, 0], capacity)
        chooser = (chosen[:, None] == places[None, :]) & filled[None, :]
        picked = jnp.dot(chooser.astype(jnp.bfloat16), arrived, preferred_element_type=jnp.float32)
        image_here = jnp.any(chooser, axis=1)[:, None]
        sequence = jnp.where(image_here, picked, text_embeds.astype(jnp.float32))
        llm_normed = rms_norm(sequence, llm_norm).astype(jnp.bfloat16)
        shard_rows = gather_mp(llm_normed, 3)
        projected = jnp.concatenate(
            [
                jnp.dot(shard_rows, q_w, preferred_element_type=jnp.float32),
                jnp.dot(shard_rows, kv_w[0], preferred_element_type=jnp.float32),
                jnp.dot(shard_rows, kv_w[1], preferred_element_type=jnp.float32),
            ],
            axis=1,
        )
    length = projected.shape[0]
    queries = (projected[:, :query_cols] + q_b).astype(jnp.bfloat16)
    key_rows = (projected[:, query_cols : query_cols + kv_cols] + kv_b[0]).astype(jnp.bfloat16)
    value_rows = (projected[:, query_cols + kv_cols :] + kv_b[1]).astype(jnp.bfloat16)
    heads_here = query_cols // HD
    group_size = QH // KVH
    dims_here = kv_cols // KVH

    def head_major(columns):
        return columns.T.reshape(dims_here, KVH, length).swapaxes(0, 1)

    stacked = jnp.stack([head_major(key_rows), head_major(value_rows)], axis=1)
    (own_head,) = exchange((stacked,), "mp", lambda target: target * heads_here // group_size, 4)
    key_cols = own_head[:, 0].reshape(HD, length)
    value_cols = own_head[:, 1].reshape(HD, length)
    query_heads = queries.reshape(length, heads_here, HD)
    scores = jnp.einsum(
        "qhd,dk->hqk", query_heads, key_cols, preferred_element_type=jnp.float32
    ) * HD ** (-0.5)
    allowed = jnp.arange(length)[:, None] >= jnp.arange(length)[None, :]
    scores = jnp.where(allowed[None], scores, -1e30)
    peak = jnp.max(scores, axis=-1, keepdims=True)
    weights = jnp.exp(scores - peak)
    weights = (weights / jnp.sum(weights, axis=-1, keepdims=True)).astype(jnp.bfloat16)
    mixture = jnp.einsum("hqk,dk->qhd", weights, value_cols, preferred_element_type=jnp.float32)
    return mixture.astype(jnp.bfloat16).reshape(length, query_cols)


def solution(mesh):
    return jax.shard_map(
        shards,
        mesh=mesh,
        in_specs=(
            P(("dp", "mp"), None),
            P(("dp", "mp"), None),
            P(("dp", "mp"), None),
            P(("dp", "mp"), None),
            P(("dp", "mp"), None),
            P(),
            P(),
            P(),
            P(),
            P(),
            P(None, "mp"),
            P("mp"),
            P("mp", None),
            P(),
            P(),
            P(None, "mp"),
            P("mp"),
            P(None, None, "mp"),
            P(None, "mp"),
        ),
        out_specs=P("dp", "mp"),
        check_vma=False,
    )
```

```python
import functools
import jax
import jax.numpy as jnp
from jax import lax
from jax.experimental import pallas as pl
from jax.experimental.pallas import tpu as pltpu
from jax.sharding import PartitionSpec as P

VHD = 80
HD = 128
QH = 32
KVH = 4

MESH = pl.DeviceIdType.MESH
LIMIT = 60 * 1024 * 1024


def corners():
    me = lax.axis_index("mp")
    core, first, second = me % 2, (me // 2) % 2, me // 4
    partner = 1 - 2 * core
    across = 2 - 4 * first
    up = 4 - 8 * second
    return me, partner, across, up


def greet(axis, others):
    barrier = pltpu.get_barrier_semaphore()
    for other in others:
        pl.semaphore_signal(barrier, inc=1, device_id={axis: other}, device_id_type=MESH)
    pl.semaphore_wait(barrier, len(others))


def gather_kernel(rows, in_ref, out_ref, local_sem, send_sem, recv_sem):
    me, partner, across, up = corners()
    greet("mp", (me + partner, me + across, me + up))
    half = rows // 2

    def piece(device, part):
        if part is None:
            return out_ref.at[pl.ds(pl.multiple_of(device * rows, rows), rows)]
        return out_ref.at[pl.ds(pl.multiple_of(device * rows + part * half, half), half)]

    def own(part):
        return in_ref if part is None else in_ref.at[pl.ds(part * half, half)]

    def copy(index, device, part, target, mine=False):
        return pltpu.make_async_remote_copy(
            src_ref=own(part) if mine else piece(device, part),
            dst_ref=piece(device, part),
            send_sem=send_sem.at[index],
            recv_sem=recv_sem.at[index],
            device_id={"mp": target},
            device_id_type=MESH,
        )

    x0 = copy(0, me, 0, me + across, True)
    y1 = copy(4, me, 1, me + up, True)
    x1 = copy(1, me, 1, me + across, True)
    y0 = copy(3, me, 0, me + up, True)
    mate = copy(6, me, None, me + partner, True)
    for item in (x0, y1, x1, y0, mate):
        item.start()
    keep = pltpu.make_async_copy(in_ref, piece(me, None), local_sem)
    keep.start()
    x0.wait_recv()
    far0 = copy(5, me + across, 0, me + up)
    far0.start()
    y1.wait_recv()
    far1 = copy(2, me + up, 1, me + across)
    far1.start()
    x1.wait_recv()
    mate_x = copy(7, me + across, None, me + partner)
    mate_x.start()
    y0.wait_recv()
    mate_y = copy(8, me + up, None, me + partner)
    mate_y.start()
    far0.wait_recv()
    mate_f0 = copy(9, me + across + up, 0, me + partner)
    mate_f0.start()
    far1.wait_recv()
    mate_f1 = copy(10, me + across + up, 1, me + partner)
    mate_f1.start()
    for item in (mate, mate_x, mate_y, mate_f0, mate_f1):
        item.wait_recv()
    for item in (x0, x1, y0, y1, far0, far1, mate, mate_x, mate_y, mate_f0, mate_f1):
        item.wait_send()
    keep.wait()


def gather_mp(block, collective_id):
    ranks = lax.axis_size("mp")
    if ranks != 8:
        return lax.all_gather(block, "mp", axis=0, tiled=True)
    rows, columns = block.shape
    return pl.pallas_call(
        functools.partial(gather_kernel, rows),
        out_shape=jax.ShapeDtypeStruct((ranks * rows, columns), block.dtype),
        in_specs=[pl.BlockSpec(memory_space=pltpu.VMEM)],
        out_specs=pl.BlockSpec(memory_space=pl.ANY),
        scratch_shapes=[
            pltpu.SemaphoreType.DMA,
            pltpu.SemaphoreType.DMA((11,)),
            pltpu.SemaphoreType.DMA((11,)),
        ],
        compiler_params=pltpu.CompilerParams(collective_id=collective_id, has_side_effects=True),
        cost_estimate=pl.CostEstimate(flops=0, bytes_accessed=ranks * block.size * 2, transcendentals=0),
    )(block)


def scatter_kernel(in_ref, out_ref, mate_ref, sum_ref, in_x, in_y, via_ref, last_ref, send_sem, recv_sem):
    me, partner, across, up = corners()
    greet("mp", (me + partner, me + across, me + up))
    columns = in_ref.shape[2]
    half = columns // 2
    step = min(half, 1024)
    devices = (me + across + up, me + across, me + up, me)

    def copy(index, src, dst, target):
        return pltpu.make_async_remote_copy(
            src_ref=src, dst_ref=dst, send_sem=send_sem.at[index], recv_sem=recv_sem.at[index],
            device_id={"mp": target}, device_id_type=MESH,
        )

    def tiles(body):
        def run(i, carry):
            body(pl.multiple_of(i * step, step))
            return carry
        lax.fori_loop(0, half // step, run, 0)

    mates = []
    for slot in range(4):
        item = copy(slot, in_ref.at[devices[slot] + partner], mate_ref.at[slot], me + partner)
        item.start()
        mates.append(item)

    def add_mate(slot):
        mates[slot].wait_recv()
        for part in range(2):
            def body(at):
                cut = pl.ds(part * half + at, step)
                sum_ref[slot, :, cut] = (
                    in_ref[devices[slot], :, cut].astype(jnp.float32) + mate_ref[slot, :, cut].astype(jnp.float32)
                ).astype(jnp.bfloat16)
            tiles(body)

    low, high = pl.ds(0, half), pl.ds(half, half)
    add_mate(0)
    far_x = copy(4, sum_ref.at[0, :, low], in_x.at[0], me + across)
    far_x.start()
    far_y = copy(5, sum_ref.at[0, :, high], in_y.at[0], me + up)
    far_y.start()
    add_mate(1)
    near_x = copy(6, sum_ref.at[1, :, low], in_x.at[1], me + across)
    near_x.start()
    add_mate(2)
    near_y = copy(7, sum_ref.at[2, :, high], in_y.at[1], me + up)
    near_y.start()
    add_mate(3)
    far_x.wait_recv()

    def via_low(at):
        cut = pl.ds(at, step)
        via_ref[0, :, cut] = (
            sum_ref[2, :, cut].astype(jnp.float32) + in_x[0, :, cut].astype(jnp.float32)
        ).astype(jnp.bfloat16)
    tiles(via_low)
    last_y = copy(8, via_ref.at[0], last_ref.at[0], me + up)
    last_y.start()
    far_y.wait_recv()

    def via_high(at):
        cut = pl.ds(at, step)
        via_ref[1, :, cut] = (
            sum_ref[1, :, pl.ds(half + at, step)].astype(jnp.float32) + in_y[0, :, cut].astype(jnp.float32)
        ).astype(jnp.bfloat16)
    tiles(via_high)
    last_x = copy(9, via_ref.at[1], last_ref.at[1], me + across)
    last_x.start()
    near_x.wait_recv()
    last_y.wait_recv()

    def own_low(at):
        cut = pl.ds(at, step)
        out_ref[:, cut] = (
            sum_ref[3, :, cut].astype(jnp.float32)
            + in_x[1, :, cut].astype(jnp.float32) + last_ref[0, :, cut].astype(jnp.float32)
        )
    tiles(own_low)
    near_y.wait_recv()
    last_x.wait_recv()

    def own_high(at):
        cut, wide = pl.ds(at, step), pl.ds(half + at, step)
        out_ref[:, wide] = (
            sum_ref[3, :, wide].astype(jnp.float32)
            + in_y[1, :, cut].astype(jnp.float32) + last_ref[1, :, cut].astype(jnp.float32)
        )
    tiles(own_high)
    for item in mates + [far_x, far_y, near_x, near_y, last_x, last_y]:
        item.wait_send()


def scatter_mp(partial, collective_id):
    ranks = lax.axis_size("mp")
    if ranks != 8:
        return lax.psum_scatter(partial, "mp", scatter_dimension=0, tiled=True).astype(jnp.float32)
    rows, columns = partial.shape[0] // ranks, partial.shape[1]
    half = columns // 2
    return pl.pallas_call(
        scatter_kernel,
        out_shape=jax.ShapeDtypeStruct((rows, columns), jnp.float32),
        in_specs=[pl.BlockSpec(memory_space=pltpu.VMEM)],
        out_specs=pl.BlockSpec(memory_space=pltpu.VMEM),
        scratch_shapes=[
            pltpu.VMEM((4, rows, columns), jnp.bfloat16),
            pltpu.VMEM((4, rows, columns), jnp.bfloat16),
            pltpu.VMEM((2, rows, half), jnp.bfloat16),
            pltpu.VMEM((2, rows, half), jnp.bfloat16),
            pltpu.VMEM((2, rows, half), jnp.bfloat16),
            pltpu.VMEM((2, rows, half), jnp.bfloat16),
            pltpu.SemaphoreType.DMA((10,)),
            pltpu.SemaphoreType.DMA((10,)),
        ],
        compiler_params=pltpu.CompilerParams(collective_id=collective_id, has_side_effects=True),
        cost_estimate=pl.CostEstimate(flops=0, bytes_accessed=partial.size * 4, transcendentals=0),
    )(partial.reshape(ranks, rows, columns))


def exchange_kernel(axis, ranks, pick, count, *refs):
    ins, outs = refs[:count], refs[count:2 * count]
    local_sem, send_sem, recv_sem = refs[2 * count:]
    me = lax.axis_index(axis)
    targets = [lax.rem(me + step, ranks) for step in range(1, ranks)]
    greet(axis, targets)
    copies = []
    for index in range(count):
        for place, target in enumerate(targets):
            item = pltpu.make_async_remote_copy(
                src_ref=ins[index].at[pick(target)], dst_ref=outs[index].at[me],
                send_sem=send_sem.at[index, place], recv_sem=recv_sem.at[index, place],
                device_id={axis: target}, device_id_type=MESH,
            )
            item.start()
            copies.append(item)
        item = pltpu.make_async_copy(ins[index].at[pick(me)], outs[index].at[me], local_sem.at[index])
        item.start()
        copies.append(item)
    for item in copies:
        item.wait()


def exchange(arrays, axis, pick, collective_id):
    ranks = lax.axis_size(axis)
    return pl.pallas_call(
        functools.partial(exchange_kernel, axis, ranks, pick, len(arrays)),
        out_shape=[jax.ShapeDtypeStruct((ranks,) + a.shape[1:], a.dtype) for a in arrays],
        in_specs=[pl.BlockSpec(memory_space=pltpu.VMEM)] * len(arrays),
        out_specs=[pl.BlockSpec(memory_space=pltpu.VMEM)] * len(arrays),
        scratch_shapes=[
            pltpu.SemaphoreType.DMA((len(arrays),)),
            pltpu.SemaphoreType.DMA((len(arrays), ranks - 1)),
            pltpu.SemaphoreType.DMA((len(arrays), ranks - 1)),
        ],
        compiler_params=pltpu.CompilerParams(collective_id=collective_id, has_side_effects=True),
        cost_estimate=pl.CostEstimate(flops=0, bytes_accessed=4 * sum(a.size for a in arrays), transcendentals=0),
    )(*arrays)


CHUNKS = 4


def handover_kernel(
    groups, ranks, emb_ref, selector_ref, marks_ref, picker_ref, text_ref, gain_ref, q_ref, kv_ref,
    out_ref, square_ref,
    send_ref, arrived_ref, arrived_marks, rows_ref, q_here, kv_here, own_square,
    load_sem, z_send, z_recv, send_sem, recv_sem, s_send, s_recv,
):
    me, partner, across, up = corners()
    group = lax.axis_index("dp")
    peers = [lax.rem(group + step, groups) for step in range(1, groups)]
    others = [lax.rem(me + step, ranks) for step in range(1, ranks)]
    loads = [pltpu.make_async_copy(q_ref, q_here, load_sem.at[0]), pltpu.make_async_copy(kv_ref, kv_here, load_sem.at[1])]
    for item in loads:
        item.start()
    barrier = pltpu.get_barrier_semaphore()
    for peer in peers:
        pl.semaphore_signal(barrier, inc=1, device_id={"dp": peer}, device_id_type=MESH)
    for other in others:
        pl.semaphore_signal(barrier, inc=1, device_id={"mp": other}, device_id_type=MESH)
    pl.semaphore_wait(barrier, groups + ranks - 2)

    slots, width = text_ref.shape
    room = slots // groups
    wide = width // CHUNKS
    half = slots // 2

    def block_of(index):
        return pl.ds(pl.multiple_of(index * room, room), room)

    own_block = block_of(group)
    pending = []

    def z_copy(index, place, src, dst):
        item = pltpu.make_async_remote_copy(
            src_ref=src, dst_ref=dst, send_sem=z_send.at[index, place], recv_sem=z_recv.at[index, place],
            device_id={"dp": peers[place]}, device_id_type=MESH,
        )
        item.start()
        pending.append(item)
        return item

    mark_copies = [
        z_copy(CHUNKS, place, marks_ref.at[block_of(peers[place])], arrived_marks.at[own_block])
        for place in range(groups - 1)
    ]
    arrived_marks[own_block, :] = marks_ref[own_block, :]
    z_copies = []
    for chunk in range(CHUNKS):
        cut = pl.ds(chunk * wide, wide)
        send_ref[:, cut] = jnp.dot(
            selector_ref[...], emb_ref[:, cut], preferred_element_type=jnp.float32
        ).astype(jnp.bfloat16)
        z_copies.append([
            z_copy(chunk, place, send_ref.at[block_of(peers[place]), cut], arrived_ref.at[own_block, cut])
            for place in range(groups - 1)
        ])
        arrived_ref[own_block, cut] = send_ref[own_block, cut]

    def piece(device, part, cut):
        if part is None:
            return rows_ref.at[pl.ds(pl.multiple_of(device * slots, slots), slots), cut]
        return rows_ref.at[pl.ds(pl.multiple_of(device * slots + part * half, half), half), cut]

    def copy(chunk, index, device, part, target):
        ref = piece(device, part, pl.ds(chunk * wide, wide))
        item = pltpu.make_async_remote_copy(
            src_ref=ref, dst_ref=ref, send_sem=send_sem.at[chunk, index], recv_sem=recv_sem.at[chunk, index],
            device_id={"mp": target}, device_id_type=MESH,
        )
        item.start()
        pending.append(item)
        return item

    for item in mark_copies:
        item.wait_recv()
    image_here = jnp.dot(picker_ref[...], arrived_marks[...], preferred_element_type=jnp.float32)[:, :1] > 0.5
    own_square[...] = jnp.zeros_like(own_square)
    firsts, mates = [], []

    def choose(chunk):
        cut = pl.ds(chunk * wide, wide)
        for item in z_copies[chunk]:
            item.wait_recv()
        picked = jnp.dot(picker_ref[...], arrived_ref[:, cut], preferred_element_type=jnp.float32)
        sequence = jnp.where(image_here, picked, text_ref[:, cut].astype(jnp.float32))
        squares = sequence * sequence
        total = squares[:, :128]
        for at in range(128, wide, 128):
            total = total + squares[:, at:at + 128]
        own_square[pl.ds(0, slots), :] += total
        rows_ref[pl.ds(pl.multiple_of(me * slots, slots), slots), cut] = (
            sequence * gain_ref[:, cut]
        ).astype(jnp.bfloat16)
        x0 = copy(chunk, 0, me, 0, me + across)
        y1 = copy(chunk, 4, me, 1, me + up)
        x1 = copy(chunk, 1, me, 1, me + across)
        y0 = copy(chunk, 3, me, 0, me + up)
        mate = copy(chunk, 6, me, None, me + partner)
        firsts.append((x0, y1, x1, y0))
        mates.append([mate])

    def forward(chunk):
        x0, y1, x1, y0 = firsts[chunk]
        x0.wait_recv()
        far0 = copy(chunk, 5, me + across, 0, me + up)
        y1.wait_recv()
        far1 = copy(chunk, 2, me + up, 1, me + across)
        x1.wait_recv()
        mates[chunk].append(copy(chunk, 7, me + across, None, me + partner))
        y0.wait_recv()
        mates[chunk].append(copy(chunk, 8, me + up, None, me + partner))
        firsts[chunk] = (far0, far1)

    def corner(chunk):
        far0, far1 = firsts[chunk]
        far0.wait_recv()
        mates[chunk].append(copy(chunk, 9, me + across + up, 0, me + partner))
        far1.wait_recv()
        mates[chunk].append(copy(chunk, 10, me + across + up, 1, me + partner))

    queries = q_here.shape[1]
    height = 256

    def project(chunk):
        cut = pl.ds(chunk * wide, wide)
        for item in mates[chunk]:
            item.wait_recv()
        if chunk == 0:
            for item in loads:
                item.wait()

        def run(i, carry):
            some = pl.ds(pl.multiple_of(i * height, height), height)
            left = jnp.dot(rows_ref[some, cut], q_here[cut, :], preferred_element_type=jnp.float32)
            right = jnp.dot(rows_ref[some, cut], kv_here[cut, :], preferred_element_type=jnp.float32)
            if chunk:
                left = left + out_ref[some, pl.ds(0, queries)]
                right = right + out_ref[some, pl.ds(queries, kv_here.shape[1])]
            out_ref[some, pl.ds(0, queries)] = left
            out_ref[some, pl.ds(queries, kv_here.shape[1])] = right
            return carry
        lax.fori_loop(0, ranks * slots // height, run, 0)

    for chunk in range(CHUNKS):
        choose(chunk)
        if chunk > 0:
            forward(chunk - 1)
        if chunk > 1:
            corner(chunk - 2)
            project(chunk - 2)
    square_ref[me] = jnp.broadcast_to(jnp.sum(own_square[...].T, axis=0, keepdims=True), square_ref.shape[1:])
    forward(CHUNKS - 1)
    square_copies = []
    for place, other in enumerate(others):
        item = pltpu.make_async_remote_copy(
            src_ref=square_ref.at[me], dst_ref=square_ref.at[me], send_sem=s_send.at[place], recv_sem=s_recv.at[place],
            device_id={"mp": other}, device_id_type=MESH,
        )
        item.start()
        square_copies.append(item)
    corner(CHUNKS - 2)
    project(CHUNKS - 2)
    corner(CHUNKS - 1)
    project(CHUNKS - 1)
    for item in square_copies:
        item.wait()
    for item in pending:
        item.wait_send()


def handover(embedded, selector, picker, text, gain, q_w, kv_both, collective_id):
    groups, ranks = lax.axis_size("dp"), lax.axis_size("mp")
    slots, width = text.shape
    marks = jnp.broadcast_to(jnp.sum(selector, axis=1, keepdims=True), (slots, 128)).astype(jnp.bfloat16)
    columns = q_w.shape[1] + kv_both.shape[1]
    vmem = pl.BlockSpec(memory_space=pltpu.VMEM)
    hbm = pl.BlockSpec(memory_space=pl.ANY)
    return pl.pallas_call(
        functools.partial(handover_kernel, groups, ranks),
        out_shape=[
            jax.ShapeDtypeStruct((ranks * slots, columns), jnp.float32),
            jax.ShapeDtypeStruct((ranks, 8, 128), jnp.float32),
        ],
        in_specs=[vmem] * 6 + [hbm] * 2,
        out_specs=[vmem] * 2,
        scratch_shapes=[
            pltpu.VMEM((slots, width), jnp.bfloat16),
            pltpu.VMEM((slots, width), jnp.bfloat16),
            pltpu.VMEM((slots, 128), jnp.bfloat16),
            pltpu.VMEM((ranks * slots, width), jnp.bfloat16),
            pltpu.VMEM(q_w.shape, q_w.dtype),
            pltpu.VMEM(kv_both.shape, kv_both.dtype),
            pltpu.VMEM((128, 128), jnp.float32),
            pltpu.SemaphoreType.DMA((2,)),
            pltpu.SemaphoreType.DMA((CHUNKS + 1, groups - 1)),
            pltpu.SemaphoreType.DMA((CHUNKS + 1, groups - 1)),
            pltpu.SemaphoreType.DMA((CHUNKS, 11)),
            pltpu.SemaphoreType.DMA((CHUNKS, 11)),
            pltpu.SemaphoreType.DMA((ranks - 1,)),
            pltpu.SemaphoreType.DMA((ranks - 1,)),
        ],
        compiler_params=pltpu.CompilerParams(collective_id=collective_id, has_side_effects=True, vmem_limit_bytes=LIMIT),
        cost_estimate=pl.CostEstimate(flops=2 * ranks * slots * width * columns, bytes_accessed=12 * ranks * slots * width, transcendentals=0),
    )(embedded, selector.astype(jnp.bfloat16), marks, picker.astype(jnp.bfloat16), text, gain.reshape(1, -1), q_w, kv_both)


epsilon = 1e-06

def rms_norm(inputs, gain):
    inputs = inputs.astype(jnp.float32)
    return inputs * lax.rsqrt(jnp.mean(inputs * inputs, axis=-1, keepdims=True) + epsilon) * gain


UNITS = (4, 6, 6, 6, 6, 4)
WIDE = 256
TOP = 63 * 1024 * 1024


def tiles_of(width):
    return [(at, min(WIDE, width - at)) for at in range(0, width, WIDE)]


def fused_kernel(
    groups, ranks, spans, parts,
    ids_hbm, vnorm_hbm, vbias_hbm, mnorm_hbm, owner_hbm, slots_hbm, b1_hbm, b2_hbm, gain_hbm, qb_hbm, kvb_hbm,
    patches_hbm, vqkv_hbm, vout_hbm, w1_hbm, w2_hbm, q_hbm, kv_hbm, text_hbm,
    out_ref,
    ids_ref, vnorm_ref, vbias_ref, mnorm_ref, owner_ref, slots_ref, b1_ref, b2_ref, gain_ref, qb_ref, kvb_ref,
    small_sem, patches_ref, vqkv_ref, vout_ref, vturn_ref, vmix_ref, w1_ref, w2_ref, q_ref, kv_ref, text_ref,
    all_ref, hidden_acc, hidden_ref, partial_ref, mate_ref, in_x, in_y, last_ref,
    send_ref, arrived_ref, marks_ref, arrived_marks, rows_ref, acc_ref, own_square, square_ref,
    turned_ref, heads_ref, query_ref,
    load_sem, g_send, g_recv, r_send, r_recv, z_send, z_recv, a_send, a_recv, s_send, s_recv, k_send, k_recv,
):
    me, partner, across, up = corners()
    group = lax.axis_index("dp")
    peers = [lax.rem(group + step, groups) for step in range(1, groups)]
    others = [lax.rem(me + step, ranks) for step in range(1, ranks)]
    loads = [
        pltpu.make_async_copy(src, dst, load_sem.at[at])
        for at, (src, dst) in enumerate((
            (w1_hbm, w1_ref), (kv_hbm, kv_ref), (w2_hbm, w2_ref), (text_hbm, text_ref), (q_hbm, q_ref),
            (patches_hbm, patches_ref), (vqkv_hbm, vqkv_ref), (vout_hbm, vout_ref),
        ))
    ]
    smalls = [
        pltpu.make_async_copy(src, dst, small_sem.at[at])
        for at, (src, dst) in enumerate((
            (ids_hbm, ids_ref), (vnorm_hbm, vnorm_ref), (vbias_hbm, vbias_ref), (mnorm_hbm, mnorm_ref),
            (owner_hbm, owner_ref), (slots_hbm, slots_ref), (b1_hbm, b1_ref), (b2_hbm, b2_ref),
            (gain_hbm, gain_ref), (qb_hbm, qb_ref), (kvb_hbm, kvb_ref),
        ))
    ]
    loads[5].start()
    smalls[0].start()
    smalls[1].start()
    loads[6].start()
    loads[7].start()
    for item in smalls[2:]:
        item.start()
    barrier = pltpu.get_barrier_semaphore()
    for peer in peers:
        pl.semaphore_signal(barrier, inc=1, device_id={"dp": peer}, device_id_type=MESH)
    for other in others:
        pl.semaphore_signal(barrier, inc=1, device_id={"mp": other}, device_id_type=MESH)
    pending = []

    def iota(shape, axis):
        return lax.broadcasted_iota(jnp.int32, shape, axis)

    def column_of(row):
        size = row.shape[1]
        eye = iota((size, size), 0) == iota((size, size), 1)
        return jnp.sum(jnp.where(eye, row, 0.0), axis=1, keepdims=True)

    patch_rows, vision_width = patches_ref.shape
    mine = patch_rows // parts
    inner = vout_ref.shape[0]
    vision_heads = inner // VHD
    smalls[0].wait()
    smalls[1].wait()
    ids_row = ids_ref[...].astype(jnp.float32)
    in_window = column_of(ids_row) == ids_row
    loads[5].wait()
    normed = rms_norm(patches_ref[...], vnorm_ref[...].reshape(1, -1)).astype(jnp.bfloat16)
    loads[6].wait()
    for item in smalls[2:]:
        item.wait()
    for item in loads[:5]:
        item.start()
    for at, size in tiles_of(3 * inner):
        value = jnp.dot(normed, vqkv_ref[:, pl.ds(at, size)], preferred_element_type=jnp.float32)
        value = (value + vbias_ref[pl.ds(at, size)].reshape(1, -1)).astype(jnp.bfloat16).astype(jnp.float32)
        for low in range(0, size, 128):
            vturn_ref[pl.ds(at + low, 128), :] = value[:, low:low + 128].T.astype(jnp.bfloat16)
    def third(which, head):
        return vturn_ref[pl.ds(which * inner + head * VHD, VHD), :]

    all_scores = [
        jnp.where(in_window, lax.dot_general(
            third(1, head), third(0, head), (((0,), (0,)), ((), ())), preferred_element_type=jnp.float32
        ) * VHD ** (-0.5), -1e30)
        for head in range(vision_heads)
    ]
    all_weights = []
    for scores in all_scores:
        weights = jnp.exp(scores - jnp.max(scores, axis=0, keepdims=True))
        all_weights.append((weights * (1.0 / jnp.sum(weights, axis=0, keepdims=True))).astype(jnp.bfloat16))
    for head, weights in enumerate(all_weights):
        vmix_ref[pl.ds(head * VHD, VHD), :] = jnp.dot(third(2, head), weights, preferred_element_type=jnp.float32)
    loads[7].wait()
    mixed = jnp.concatenate(
        [vmix_ref[pl.ds(at, 128), :].T.astype(jnp.bfloat16) for at in range(0, inner, 128)], axis=1
    )
    residual = (
        patches_ref[...].astype(jnp.float32) + jnp.dot(mixed, vout_ref[...], preferred_element_type=jnp.float32)
    ).astype(jnp.bfloat16)
    merged = rms_norm(residual, mnorm_ref[...].reshape(1, -1)).astype(jnp.bfloat16)
    row = iota((patch_rows, patch_rows), 0)
    regroup = jnp.where(
        iota((patch_rows, patch_rows), 1) == row % mine * parts + row // mine, 1.0, 0.0
    ).astype(jnp.bfloat16)
    regrouped = jnp.dot(regroup, merged, preferred_element_type=jnp.float32).astype(jnp.bfloat16)
    own_rows = pl.ds(pl.multiple_of(me * mine, mine), mine)
    for part in range(parts):
        all_ref[own_rows, pl.ds(part * vision_width, vision_width)] = regrouped[part * mine:(part + 1) * mine, :]
    pl.semaphore_wait(barrier, groups + ranks - 2)

    def remote(src, dst, send, recv, where):
        item = pltpu.make_async_remote_copy(
            src_ref=src, dst_ref=dst, send_sem=send, recv_sem=recv, device_id=where, device_id_type=MESH,
        )
        item.start()
        pending.append(item)
        return item

    class Gather:
        def __init__(self, ref, count, width, send, recv):
            self.ref, self.count, self.width, self.send, self.recv = ref, count, width, send, recv
            self.firsts, self.mates = {}, {}

        def cut(self, chunk):
            return pl.ds(*self.width[chunk])

        def copy(self, chunk, index, device, part, target):
            size = self.count if part is None else self.count // 2
            shift = 0 if part is None else part * size
            ref = self.ref.at[pl.ds(pl.multiple_of(device * self.count + shift, size), size), self.cut(chunk)]
            return remote(ref, ref, self.send.at[chunk, index], self.recv.at[chunk, index], {"mp": target})

        def begin(self, chunk):
            x0 = self.copy(chunk, 0, me, 0, me + across)
            y1 = self.copy(chunk, 4, me, 1, me + up)
            x1 = self.copy(chunk, 1, me, 1, me + across)
            y0 = self.copy(chunk, 3, me, 0, me + up)
            self.mates[chunk] = [self.copy(chunk, 6, me, None, me + partner)]
            self.firsts[chunk] = (x0, y1, x1, y0)

        def forward(self, chunk):
            x0, y1, x1, y0 = self.firsts[chunk]
            x0.wait_recv()
            far0 = self.copy(chunk, 5, me + across, 0, me + up)
            y1.wait_recv()
            far1 = self.copy(chunk, 2, me + up, 1, me + across)
            x1.wait_recv()
            self.mates[chunk].append(self.copy(chunk, 7, me + across, None, me + partner))
            y0.wait_recv()
            self.mates[chunk].append(self.copy(chunk, 8, me + up, None, me + partner))
            self.firsts[chunk] = (far0, far1)

        def corner(self, chunk):
            far0, far1 = self.firsts[chunk]
            far0.wait_recv()
            self.mates[chunk].append(self.copy(chunk, 9, me + across + up, 0, me + partner))
            far1.wait_recv()
            self.mates[chunk].append(self.copy(chunk, 10, me + across + up, 1, me + partner))

        def finish(self, chunk):
            for item in self.mates[chunk]:
                item.wait_recv()

    merged_all = Gather(all_ref, mine, [(part * 2 * vision_width, 2 * vision_width) for part in range(parts // 2)], g_send, g_recv)
    parts = parts // 2
    for part in range(parts):
        merged_all.begin(part)

    slots, width = text_ref.shape
    room = slots // groups
    steps = len(spans)

    own_row = owner_ref[...].astype(jnp.float32)
    same = column_of(own_row) == own_row
    before = iota((mine, mine), 0) < iota((mine, mine), 1)
    rank_row = jnp.sum(jnp.where(same & before, 1.0, 0.0), axis=0, keepdims=True)
    slot_row = own_row * room + rank_row
    selected = jnp.where(iota((slots, mine), 0).astype(jnp.float32) == slot_row, 1.0, 0.0)
    selector = selected.astype(jnp.bfloat16)
    marks_ref[...] = jnp.broadcast_to(jnp.sum(selected, axis=1, keepdims=True), marks_ref.shape).astype(jnp.bfloat16)
    slot_col = column_of(slots_ref[...].astype(jnp.float32))
    picker = jnp.where(slot_col == iota((slots, slots), 1).astype(jnp.float32), 1.0, 0.0).astype(jnp.bfloat16)

    def block_of(index):
        return pl.ds(pl.multiple_of(index * room, room), room)

    own_block = block_of(group)

    def z_copy(index, place, src, dst):
        return remote(src, dst, z_send.at[index, place], z_recv.at[index, place], {"dp": peers[place]})

    mark_copies = [
        z_copy(steps, place, marks_ref.at[block_of(peers[place])], arrived_marks.at[own_block])
        for place in range(groups - 1)
    ]
    arrived_marks[own_block, :] = marks_ref[own_block, :]

    def first(part):
        cut = merged_all.cut(part)
        for at, size in tiles_of(hidden_acc.shape[1]):
            value = jnp.dot(all_ref[:, cut], w1_ref[cut, pl.ds(at, size)], preferred_element_type=jnp.float32)
            if part:
                value = value + hidden_acc[:, pl.ds(at, size)]
            if part < parts - 1:
                hidden_acc[:, pl.ds(at, size)] = value
            else:
                value = value + b1_ref[pl.ds(at, size)].reshape(1, -1)
                value = 0.5 * value * (1.0 + lax.erf(value * (2.0 ** -0.5)))
                hidden_ref[:, pl.ds(at, size)] = value.astype(jnp.bfloat16)

    for part in range(parts):
        merged_all.forward(part)
    loads[0].wait()
    for part in range(parts):
        merged_all.corner(part)
        if part:
            merged_all.finish(part - 1)
            first(part - 1)
    merged_all.finish(parts - 1)
    first(parts - 1)
    loads[2].wait()

    devices = (me + across + up, me + across, me + up, me)

    def rows_of(device):
        return pl.ds(pl.multiple_of(device * mine, mine), mine)

    reduce_mates, outward, lasts, z_copies = {}, {}, {}, {}

    def r_copy(chunk, index, src, dst, target):
        return remote(src, dst, r_send.at[chunk, index], r_recv.at[chunk, index], {"mp": target})

    def halves(chunk):
        start, wide = spans[chunk]
        half = wide // 2
        return pl.ds(start, half), pl.ds(start + half, half), pl.ds(start // 2, half)

    def second(chunk):
        start, wide = spans[chunk]
        for at, size in tiles_of(wide):
            cut = pl.ds(start + at, size)
            partial_ref[:, cut] = jnp.dot(
                hidden_ref[...], w2_ref[:, cut], preferred_element_type=jnp.float32
            ).astype(jnp.bfloat16)
        cut = pl.ds(*spans[chunk])
        reduce_mates[chunk] = [
            r_copy(chunk, slot, partial_ref.at[rows_of(devices[slot] + partner), cut], mate_ref.at[slot, :, cut], me + partner)
            for slot in range(4)
        ]

    def add_mates(chunk):
        low, high, small = halves(chunk)
        cut = pl.ds(*spans[chunk])

        def add(slot):
            reduce_mates[chunk][slot].wait_recv()
            partial_ref[rows_of(devices[slot]), cut] = (
                partial_ref[rows_of(devices[slot]), cut].astype(jnp.float32) + mate_ref[slot, :, cut].astype(jnp.float32)
            ).astype(jnp.bfloat16)

        add(0)
        far_x = r_copy(chunk, 4, partial_ref.at[rows_of(devices[0]), low], in_x.at[0, :, small], me + across)
        far_y = r_copy(chunk, 5, partial_ref.at[rows_of(devices[0]), high], in_y.at[0, :, small], me + up)
        add(1)
        near_x = r_copy(chunk, 6, partial_ref.at[rows_of(devices[1]), low], in_x.at[1, :, small], me + across)
        add(2)
        near_y = r_copy(chunk, 7, partial_ref.at[rows_of(devices[2]), high], in_y.at[1, :, small], me + up)
        add(3)
        outward[chunk] = (far_x, far_y, near_x, near_y)

    def via(chunk):
        low, high, small = halves(chunk)
        far_x, far_y, near_x, near_y = outward[chunk]
        far_x.wait_recv()
        partial_ref[rows_of(devices[2]), low] = (
            partial_ref[rows_of(devices[2]), low].astype(jnp.float32) + in_x[0, :, small].astype(jnp.float32)
        ).astype(jnp.bfloat16)
        last_y = r_copy(chunk, 8, partial_ref.at[rows_of(devices[2]), low], last_ref.at[0, :, small], me + up)
        far_y.wait_recv()
        partial_ref[rows_of(devices[1]), high] = (
            partial_ref[rows_of(devices[1]), high].astype(jnp.float32) + in_y[0, :, small].astype(jnp.float32)
        ).astype(jnp.bfloat16)
        last_x = r_copy(chunk, 9, partial_ref.at[rows_of(devices[1]), high], last_ref.at[1, :, small], me + across)
        lasts[chunk] = (near_x, last_y, near_y, last_x)

    def embed(chunk):
        low, high, small = halves(chunk)
        near_x, last_y, near_y, last_x = lasts[chunk]
        pieces = []
        for at, (place, near, last, side) in enumerate(((low, near_x, last_y, in_x), (high, near_y, last_x, in_y))):
            near.wait_recv()
            last.wait_recv()
            total = (
                partial_ref[rows_of(me), place].astype(jnp.float32)
                + side[1, :, small].astype(jnp.float32) + last_ref[at, :, small].astype(jnp.float32)
            )
            rows = (total + b2_ref[:, place]).astype(jnp.bfloat16)
            send_ref[:, place] = jnp.dot(selector, rows, preferred_element_type=jnp.float32).astype(jnp.bfloat16)
        cut = pl.ds(*spans[chunk])
        z_copies[chunk] = [
            z_copy(chunk, place, send_ref.at[block_of(peers[place]), cut], arrived_ref.at[own_block, cut])
            for place in range(groups - 1)
        ]
        arrived_ref[own_block, cut] = send_ref[own_block, cut]

    sequence_all = Gather(rows_ref, slots, spans, a_send, a_recv)

    def choose(chunk):
        cut = pl.ds(*spans[chunk])
        if chunk == 0:
            loads[3].wait()
            for item in mark_copies:
                item.wait_recv()
            own_square[...] = jnp.zeros_like(own_square)
        image_here = jnp.dot(picker, arrived_marks[...], preferred_element_type=jnp.float32)[:, :1] > 0.5
        for item in z_copies[chunk]:
            item.wait_recv()
        picked = jnp.dot(picker, arrived_ref[:, cut], preferred_element_type=jnp.float32)
        sequence = jnp.where(image_here, picked, text_ref[:, cut].astype(jnp.float32))
        squares = sequence * sequence
        total = squares[:, :128]
        for at in range(128, spans[chunk][1], 128):
            total = total + squares[:, at:at + 128]
        own_square[pl.ds(0, slots), :] += total
        rows_ref[pl.ds(pl.multiple_of(me * slots, slots), slots), cut] = (
            sequence * gain_ref[:, cut]
        ).astype(jnp.bfloat16)
        sequence_all.begin(chunk)

    square_copies = []

    def share_squares():
        square_ref[me] = jnp.broadcast_to(jnp.sum(own_square[...].T, axis=0, keepdims=True), square_ref.shape[1:])
        for place, other in enumerate(others):
            square_copies.append(
                remote(square_ref.at[me], square_ref.at[me], s_send.at[place], s_recv.at[place], {"mp": other})
            )

    queries = q_ref.shape[1]
    columns = kv_ref.shape[0]

    def project_into(chunk, at, size, weight, dims):
        value = lax.dot_general(
            rows_ref[:, pl.ds(*spans[chunk])], weight, (((1,), (dims,)), ((), ())), preferred_element_type=jnp.float32
        )
        place = pl.ds(at, size)
        if chunk:
            value = value + acc_ref[:, place]
        acc_ref[:, place] = value

    def project_kv(chunk):
        sequence_all.finish(chunk)
        if chunk == 0:
            loads[1].wait()
            loads[4].wait()
        project_into(chunk, queries, columns, kv_ref[:, pl.ds(*spans[chunk])], 1)

    def project_q(chunk):
        for at, size in tiles_of(queries):
            project_into(chunk, at, size, q_ref[pl.ds(*spans[chunk]), pl.ds(at, size)], 0)

    def stage(run, chunk):
        if 0 <= chunk < steps:
            run(chunk)

    for step in range(steps + 7):
        stage(second, step - 0)
        stage(add_mates, step - 1)
        stage(via, step - 2)
        stage(embed, step - 3)
        stage(project_kv, step - 8)
        stage(project_q, step - 8)
        stage(choose, step - 5)
        if step - 5 == steps - 1:
            share_squares()
        stage(sequence_all.forward, step - 6)
        stage(sequence_all.corner, step - 7)
    for item in square_copies:
        item.wait_recv()

    scales = [
        lax.rsqrt(column_of(square_ref[rank, pl.ds(0, 1), pl.ds(0, slots)]) / width + epsilon) for rank in range(ranks)
    ]
    bias = jnp.concatenate([kvb_ref[pl.ds(0, 1), :], kvb_ref[pl.ds(1, 1), :]], axis=1)
    length = ranks * slots
    project_kv(steps - 1)
    scaled = jnp.concatenate(
        [acc_ref[pl.ds(rank * slots, slots), pl.ds(queries, columns)] * scales[rank] for rank in range(ranks)], axis=0
    )
    both = (scaled + bias).astype(jnp.bfloat16)
    dims = columns // (2 * KVH)
    row = iota((columns, columns), 0)
    wanted = (row // dims) % 2 * (dims * KVH) + row % dims * KVH + row // (2 * dims)
    turn = jnp.where(iota((columns, columns), 1) == wanted, 1.0, 0.0).astype(jnp.bfloat16)
    turned_ref[...] = lax.dot_general(
        turn, both, (((1,), (1,)), ((), ())), preferred_element_type=jnp.float32
    ).astype(jnp.bfloat16)
    heads_here = queries // HD
    group_size = QH // KVH

    def head_rows(device):
        return pl.ds(pl.multiple_of(device * heads_here // group_size * (2 * dims), 2 * dims), 2 * dims)

    head_copies = [
        remote(turned_ref.at[head_rows(other)], heads_ref.at[me], k_send.at[place], k_recv.at[place], {"mp": other})
        for place, other in enumerate(others)
    ]
    heads_ref[me] = turned_ref[head_rows(me), :]
    project_q(steps - 1)
    for rank in range(ranks):
        some = pl.ds(rank * slots, slots)
        query_ref[some, :] = (acc_ref[some, pl.ds(0, queries)] * scales[rank] + qb_ref[...]).astype(jnp.bfloat16)
    for item in head_copies:
        item.wait_recv()
    tall = 128
    keys = heads_ref[:, pl.ds(0, dims), :].reshape(ranks * dims, length)
    values = heads_ref[:, pl.ds(dims, dims), :].reshape(ranks * dims, length)
    allowed = iota((tall, tall), 0) >= iota((tall, tall), 1)
    for block in range(length // tall):
        reach = (block + 1) * tall
        some = pl.ds(block * tall, tall)
        block_scores = [
            jnp.dot(query_ref[some, pl.ds(head * HD, HD)], keys[:, :reach], preferred_element_type=jnp.float32)
            for head in range(heads_here)
        ]
        weighted = []
        for scores in block_scores:
            last = jnp.where(allowed, scores[:, block * tall:], -1e30)
            scores = jnp.concatenate([scores[:, :block * tall], last], axis=1) if block else last
            weights = jnp.exp((scores - jnp.max(scores, axis=-1, keepdims=True)) * HD ** (-0.5))
            weighted.append((weights.astype(jnp.bfloat16), jnp.sum(weights, axis=-1, keepdims=True)))
        out_ref[some, :] = jnp.concatenate([
            lax.dot_general(
                weights, values[:, :reach], (((1,), (1,)), ((), ())), preferred_element_type=jnp.float32
            ) * (1.0 / total)
            for weights, total in weighted
        ], axis=1).astype(jnp.bfloat16)
    for item in pending:
        item.wait_send()


def fused(
    patches, window_ids, owner, slot_of_row, text, vit_norm, vit_qkv_w, vit_qkv_b, vit_out_w, merge_norm,
    w1, b1, w2, b2, gain, q_w, q_b, kv_w, kv_b, collective_id,
):
    groups, ranks = lax.axis_size("dp"), lax.axis_size("mp")
    mine = owner.shape[0]
    parts = patches.shape[0] // mine
    slots, width = text.shape
    unit = width // sum(UNITS)
    spans = [(sum(UNITS[:at]) * unit, size * unit) for at, size in enumerate(UNITS)]
    steps = len(spans)
    half = width // 2
    queries, columns = q_w.shape[1], 2 * kv_w.shape[2]
    length = ranks * slots
    hbm = pl.BlockSpec(memory_space=pl.ANY)
    dma = pltpu.SemaphoreType.DMA
    bf16, f32 = jnp.bfloat16, jnp.float32
    smalls = (
        window_ids, vit_norm, vit_qkv_b, merge_norm, owner.reshape(1, -1), slot_of_row, b1,
        b2.reshape(1, -1), gain.reshape(1, -1), q_b.reshape(1, -1), kv_b,
    )
    return pl.pallas_call(
        functools.partial(fused_kernel, groups, ranks, spans, parts),
        out_shape=jax.ShapeDtypeStruct((length, queries), bf16),
        in_specs=[hbm] * 19,
        out_specs=pl.BlockSpec(memory_space=pltpu.VMEM),
        scratch_shapes=[pltpu.VMEM(item.shape, item.dtype) for item in smalls] + [
            dma((len(smalls),)),
            pltpu.VMEM(patches.shape, bf16),
            pltpu.VMEM(vit_qkv_w.shape, bf16),
            pltpu.VMEM(vit_out_w.shape, bf16),
            pltpu.VMEM((vit_qkv_w.shape[1], patches.shape[0]), bf16),
            pltpu.VMEM((vit_out_w.shape[0], patches.shape[0]), f32),
            pltpu.VMEM(w1.shape, bf16),
            pltpu.VMEM(w2.shape, bf16),
            pltpu.VMEM(q_w.shape, bf16),
            pltpu.VMEM((columns, width), bf16),
            pltpu.VMEM((slots, width), bf16),
            pltpu.VMEM((ranks * mine, w1.shape[0]), bf16),
            pltpu.VMEM((ranks * mine, w1.shape[1]), f32),
            pltpu.VMEM((ranks * mine, w1.shape[1]), bf16),
            pltpu.VMEM((ranks * mine, width), bf16),
            pltpu.VMEM((4, mine, width), bf16),
            pltpu.VMEM((2, mine, half), bf16),
            pltpu.VMEM((2, mine, half), bf16),
            pltpu.VMEM((2, mine, half), bf16),
            pltpu.VMEM((slots, width), bf16),
            pltpu.VMEM((slots, width), bf16),
            pltpu.VMEM((slots, 128), bf16),
            pltpu.VMEM((slots, 128), bf16),
            pltpu.VMEM((length, width), bf16),
            pltpu.VMEM((length, queries + columns), f32),
            pltpu.VMEM((128, 128), f32),
            pltpu.VMEM((ranks, 8, 128), f32),
            pltpu.VMEM((columns, length), bf16),
            pltpu.VMEM((ranks, columns // KVH, length), bf16),
            pltpu.VMEM((length, queries), bf16),
            dma((8,)),
            dma((parts, 11)), dma((parts, 11)),
            dma((steps, 10)), dma((steps, 10)),
            dma((steps + 1, groups - 1)), dma((steps + 1, groups - 1)),
            dma((steps, 11)), dma((steps, 11)),
            dma((ranks - 1,)), dma((ranks - 1,)),
            dma((ranks - 1,)), dma((ranks - 1,)),
        ],
        compiler_params=pltpu.CompilerParams(collective_id=collective_id, has_side_effects=True, vmem_limit_bytes=TOP),
        cost_estimate=pl.CostEstimate(flops=2 * length * width * (queries + columns), bytes_accessed=12 * length * width, transcendentals=0),
    )(
        *smalls, patches, vit_qkv_w, vit_out_w, w1, w2, q_w, kv_w.transpose(0, 2, 1).reshape(columns, width), text,
    )


def vision_block(patches, window_ids, vit_norm, vit_qkv_w, vit_qkv_b, vit_out_w, merge_norm):
    normed = rms_norm(patches, vit_norm).astype(jnp.bfloat16)
    projected = (jnp.dot(normed, vit_qkv_w, preferred_element_type=jnp.float32) + vit_qkv_b).astype(
        jnp.bfloat16
    )
    blocks = window_ids.shape[0]
    width = window_ids.shape[1]
    inner_width = vit_out_w.shape[0]
    heads = inner_width // VHD
    shaped = projected.reshape(blocks, width, 3, heads, VHD)
    scores = jnp.einsum(
        "bqhd,bkhd->bhqk", shaped[:, :, 0], shaped[:, :, 1], preferred_element_type=jnp.float32
    ) * VHD ** (-0.5)
    in_window = window_ids[:, None, :, None] == window_ids[:, None, None, :]
    scores = jnp.where(in_window, scores, -1e30)
    peak = jnp.max(scores, axis=-1, keepdims=True)
    weights = jnp.exp(scores - peak)
    weights = (weights / jnp.sum(weights, axis=-1, keepdims=True)).astype(jnp.bfloat16)
    mixture = jnp.einsum(
        "bhqk,bkhd->bqhd", weights, shaped[:, :, 2], preferred_element_type=jnp.float32
    )
    mixture = mixture.astype(jnp.bfloat16).reshape(blocks * width, inner_width)
    residual = (
        patches.astype(jnp.float32)
        + jnp.dot(mixture, vit_out_w, preferred_element_type=jnp.float32)
    ).astype(jnp.bfloat16)
    merged = rms_norm(residual, merge_norm).astype(jnp.bfloat16)
    return merged.reshape(blocks * width // 4, 4 * patches.shape[1])


def shards(
    patches,
    window_ids,
    owner,
    slot_of_row,
    text_embeds,
    vit_norm,
    vit_qkv_w,
    vit_qkv_b,
    vit_out_w,
    merge_norm,
    merge_w1,
    merge_b1,
    merge_w2,
    merge_b2,
    llm_norm,
    q_w,
    q_b,
    kv_w,
    kv_b,
):
    if lax.axis_size("mp") == 8:
        return fused(
            patches, window_ids, owner, slot_of_row, text_embeds, vit_norm, vit_qkv_w, vit_qkv_b, vit_out_w,
            merge_norm, merge_w1, merge_b1, merge_w2, merge_b2, llm_norm, q_w, q_b, kv_w, kv_b, 2,
        )
    merged = vision_block(
        patches, window_ids, vit_norm, vit_qkv_w, vit_qkv_b, vit_out_w, merge_norm
    )
    rows_all = gather_mp(merged, 0)
    hidden = jax.nn.gelu(
        jnp.dot(rows_all, merge_w1, preferred_element_type=jnp.float32) + merge_b1,
        approximate=False,
    ).astype(jnp.bfloat16)
    own_rows = scatter_mp(
        jnp.dot(hidden, merge_w2, preferred_element_type=jnp.float32).astype(jnp.bfloat16), 1
    )
    embedded = (own_rows + merge_b2).astype(jnp.bfloat16)
    seq_rows = text_embeds.shape[0]
    groups = lax.axis_size("dp")
    capacity = seq_rows // groups
    target_group = owner[:, 0]
    onehot = (target_group[:, None] == jnp.arange(groups, dtype=jnp.int32)[None, :]).astype(
        jnp.int32
    )
    rank_in = jnp.sum((jnp.cumsum(onehot, axis=0) - onehot) * onehot, axis=1)
    send_slot = target_group * capacity + rank_in
    selector = send_slot[None, :] == jnp.arange(seq_rows, dtype=jnp.int32)[:, None]
    query_cols = q_w.shape[1]
    kv_cols = kv_w.shape[2]
    if lax.axis_size("mp") == 8:
        picker = slot_of_row[0][:, None] == jnp.arange(seq_rows, dtype=jnp.int32)[None, :]
        kv_both = jnp.concatenate([kv_w[0], kv_w[1]], axis=1)
        projected, squares = handover(embedded, selector, picker, text_embeds, llm_norm, q_w, kv_both, 2)
        squares = squares[:, 0, :seq_rows].reshape(-1, 1)
        projected = projected * lax.rsqrt(squares / text_embeds.shape[1] + epsilon)
    else:
        buffer = jnp.dot(
            selector.astype(jnp.bfloat16), embedded, preferred_element_type=jnp.float32
        ).astype(jnp.bfloat16)
        buffer = buffer.reshape(groups, capacity, embedded.shape[1])
        counts = jnp.broadcast_to(jnp.sum(onehot, axis=0)[:, None, None], (groups, 8, 128))
        arrived, arrived_counts = exchange((buffer, counts), "dp", lambda target: target, 2)
        arrived = arrived.reshape(seq_rows, embedded.shape[1])
        chosen = slot_of_row[0]
        places = jnp.arange(seq_rows, dtype=jnp.int32)
        filled = places % capacity < jnp.repeat(arrived_counts[:, 0, 0], capacity)
        chooser = (chosen[:, None] == places[None, :]) & filled[None, :]
        picked = jnp.dot(chooser.astype(jnp.bfloat16), arrived, preferred_element_type=jnp.float32)
        image_here = jnp.any(chooser, axis=1)[:, None]
        sequence = jnp.where(image_here, picked, text_embeds.astype(jnp.float32))
        llm_normed = rms_norm(sequence, llm_norm).astype(jnp.bfloat16)
        shard_rows = gather_mp(llm_normed, 3)
        projected = jnp.concatenate(
            [
                jnp.dot(shard_rows, q_w, preferred_element_type=jnp.float32),
                jnp.dot(shard_rows, kv_w[0], preferred_element_type=jnp.float32),
                jnp.dot(shard_rows, kv_w[1], preferred_element_type=jnp.float32),
            ],
            axis=1,
        )
    length = projected.shape[0]
    queries = (projected[:, :query_cols] + q_b).astype(jnp.bfloat16)
    key_rows = (projected[:, query_cols : query_cols + kv_cols] + kv_b[0]).astype(jnp.bfloat16)
    value_rows = (projected[:, query_cols + kv_cols :] + kv_b[1]).astype(jnp.bfloat16)
    heads_here = query_cols // HD
    group_size = QH // KVH
    dims_here = kv_cols // KVH

    def head_major(columns):
        return columns.T.reshape(dims_here, KVH, length).swapaxes(0, 1)

    stacked = jnp.stack([head_major(key_rows), head_major(value_rows)], axis=1)
    (own_head,) = exchange((stacked,), "mp", lambda target: target * heads_here // group_size, 4)
    key_cols = own_head[:, 0].reshape(HD, length)
    value_cols = own_head[:, 1].reshape(HD, length)
    query_heads = queries.reshape(length, heads_here, HD)
    scores = jnp.einsum(
        "qhd,dk->hqk", query_heads, key_cols, preferred_element_type=jnp.float32
    ) * HD ** (-0.5)
    allowed = jnp.arange(length)[:, None] >= jnp.arange(length)[None, :]
    scores = jnp.where(allowed[None], scores, -1e30)
    peak = jnp.max(scores, axis=-1, keepdims=True)
    weights = jnp.exp(scores - peak)
    weights = (weights / jnp.sum(weights, axis=-1, keepdims=True)).astype(jnp.bfloat16)
    mixture = jnp.einsum("hqk,dk->qhd", weights, value_cols, preferred_element_type=jnp.float32)
    return mixture.astype(jnp.bfloat16).reshape(length, query_cols)


def solution(mesh):
    return jax.shard_map(
        shards,
        mesh=mesh,
        in_specs=(
            P(("dp", "mp"), None),
            P(("dp", "mp"), None),
            P(("dp", "mp"), None),
            P(("dp", "mp"), None),
            P(("dp", "mp"), None),
            P(),
            P(),
            P(),
            P(),
            P(),
            P(None, "mp"),
            P("mp"),
            P("mp", None),
            P(),
            P(),
            P(None, "mp"),
            P("mp"),
            P(None, None, "mp"),
            P(None, "mp"),
        ),
        out_specs=P("dp", "mp"),
        check_vma=False,
    )
```
